16 devices in a mesh: fsdp: 16 (over z, y, x, core).
Axes of the slice: x: 2, y: 2, z: 2, core: 2. Of those that a mesh axis runs over, the one named last changes fastest.
Arguments:
- h_saved: bfloat16 [3, 32768, 896], P(None, 'fsdp')
- g_out: bfloat16 [32768, 896], P('fsdp')
- w_gate: bfloat16 [3, 896, 4864], P(None, 'fsdp')
- w_up: bfloat16 [3, 896, 4864], P(None, 'fsdp')
- w_down: bfloat16 [3, 4864, 896], P(None, 'fsdp')
Outputs:
- output 1: float32 [3, 896, 4864], P(None, 'fsdp')
- output 2: float32 [3, 896, 4864], P(None, 'fsdp')
- output 3: float32 [3, 4864, 896], P(None, 'fsdp')
- output 4: bfloat16 [32768, 896], P('fsdp')
All inputs are finite; a program needn't handle non-finite values.
Results may differ from the reference program's by a relative error of at most 0.00587019.
Values are sent between devices in bfloat16 or wider.
A program may use at most 1 GiB of HBM per device.

```python
import jax
import jax.numpy as jnp
from jax import lax

D = 896
FF = 4864
LAYERS = 3
TOKENS = 32768

EPS = 1e-6
ROW_BLOCK = min(TOKENS, 1024)
NUM_BLOCKS = TOKENS // ROW_BLOCK


def setup_inputs(seed: int = 0) -> dict:
    keys = jax.random.split(jax.random.key(seed), 5)
    h_saved = jax.random.normal(keys[0], (LAYERS, TOKENS, D), jnp.float32).astype(jnp.bfloat16)
    g_out = jax.random.normal(keys[1], (TOKENS, D), jnp.float32).astype(jnp.bfloat16)
    w_gate = (jax.random.normal(keys[2], (LAYERS, D, FF), jnp.float32) * (D ** -0.5)).astype(jnp.bfloat16)
    w_up = (jax.random.normal(keys[3], (LAYERS, D, FF), jnp.float32) * (D ** -0.5)).astype(jnp.bfloat16)
    w_down = (jax.random.normal(keys[4], (LAYERS, FF, D), jnp.float32) * (FF ** -0.5)).astype(jnp.bfloat16)
    return {'h_saved': h_saved, 'g_out': g_out, 'w_gate': w_gate, 'w_up': w_up, 'w_down': w_down}


def block_backward(h_rows, g_rows, w_gate, w_up, w_down):
    hid_f32 = h_rows.astype(jnp.float32)
    inv_rms = lax.rsqrt(jnp.mean(hid_f32 * hid_f32, axis=-1, keepdims=True) + EPS)
    norm_f32 = hid_f32 * inv_rms
    normed = norm_f32.astype(jnp.bfloat16)
    gate_pre = jnp.dot(normed, w_gate, preferred_element_type=jnp.float32)
    up_pre = jnp.dot(normed, w_up, preferred_element_type=jnp.float32)
    gate_sig = jax.nn.sigmoid(gate_pre)
    gate_act = gate_pre * gate_sig
    hidden = (gate_act * up_pre).astype(jnp.bfloat16)
    d_hidden = jnp.dot(g_rows, w_down.T, preferred_element_type=jnp.float32)
    grad_down = jnp.dot(hidden.T, g_rows, preferred_element_type=jnp.float32)
    d_gate = (d_hidden * up_pre * gate_sig * (1.0 + gate_pre * (1.0 - gate_sig))).astype(jnp.bfloat16)
    d_up = (d_hidden * gate_act).astype(jnp.bfloat16)
    grad_gate = jnp.dot(normed.T, d_gate, preferred_element_type=jnp.float32)
    grad_up = jnp.dot(normed.T, d_up, preferred_element_type=jnp.float32)
    d_normed = jnp.dot(d_gate, w_gate.T, preferred_element_type=jnp.float32) + jnp.dot(d_up, w_up.T, preferred_element_type=jnp.float32)
    d_resid = inv_rms * (d_normed - norm_f32 * jnp.mean(d_normed * norm_f32, axis=-1, keepdims=True))
    g_next = (g_rows.astype(jnp.float32) + d_resid).astype(jnp.bfloat16)
    return g_next, grad_gate, grad_up, grad_down


def reference(h_saved, g_out, w_gate, w_up, w_down):
    def layer_step(g_rows, layer_in):
        h_layer, gate_w, up_w, down_w = layer_in

        def block_step(grad_sums, block_in):
            h_block, g_block = block_in
            g_next, grad_gate, grad_up, grad_down = block_backward(h_block, g_block, gate_w, up_w, down_w)
            new_sums = (grad_sums[0] + grad_gate, grad_sums[1] + grad_up, grad_sums[2] + grad_down)
            return new_sums, g_next

        zero_sums = (jnp.zeros((D, FF), jnp.float32), jnp.zeros((D, FF), jnp.float32), jnp.zeros((FF, D), jnp.float32))
        blocks_in = (h_layer.reshape(NUM_BLOCKS, ROW_BLOCK, D), g_rows.reshape(NUM_BLOCKS, ROW_BLOCK, D))
        grad_sums, g_blocks = lax.scan(block_step, zero_sums, blocks_in)
        return g_blocks.reshape(TOKENS, D), grad_sums

    g_first, grad_stack = lax.scan(layer_step, g_out, (h_saved, w_gate, w_up, w_down), reverse=True)
    return grad_stack[0], grad_stack[1], grad_stack[2], g_first
```

```python
import jax
import jax.numpy as jnp
from jax import lax
from jax.experimental import pallas as pl
from jax.experimental.pallas import tpu as pltpu
from jax.sharding import PartitionSpec as P

EPS = 1e-6
LAYERS = 3
D = 896
FF = 4864
ROWS = 2048
DEV = 16
DS = D // DEV
FS = FF // DEV
CPD = 16
CH = CPD * DEV
NC = FF // CH
NK = NC * LAYERS
LEAD = 4
TAIL = 5
WS = 6
RB = 1024
BB = 256
HALF = CH // 2
MESH = pl.DeviceIdType.MESH
BF = jnp.bfloat16
F32 = jnp.float32


def dot(a, b, ca, cb):
    return lax.dot_general(a, b, (((ca,), (cb,)), ((), ())), preferred_element_type=F32)


def kernel(h_hbm, g_hbm, w1_hbm, w3_hbm, w2_hbm,
           o1_hbm, o3_hbm, o2_hbm, og_hbm,
           n_v, nt_v, g_v, gt_v, dn_v, h_v, a_v, d_v,
           w1_v, w3_v, w2_v,
           g1_v, g3_v, g2_v,
           rd1, rd3, rd2, ra1, ra3, ra2, rb1, rb3, rb2, rc1, rc3, rc2,
           pa1, pa3, pa2, pb1, pb3, pb2, s1, s3, s2,
           ag_send, ag_recv, rs_send, rs_recv, own_sem, out_sem, h_sem, g_sem):
    me = lax.axis_index('fsdp')
    c = me % 2
    x = (me // 2) % 2
    y = (me // 4) % 2
    z = (me // 8) % 2
    core = me + 1 - 2 * c
    nx = me + 2 - 4 * x
    ny = me + 4 - 8 * y
    nz = me + 8 - 16 * z

    barrier = pltpu.get_barrier_semaphore()
    for peer in (core, nx, ny, nz):
        pl.semaphore_signal(barrier, inc=1, device_id=(peer,), device_id_type=MESH)
    pl.semaphore_wait(barrier, 4)

    weights = (w1_v, w3_v, w2_v)
    grads = (g1_v, g3_v, g2_v)
    rds, ras, rbs, rcs = (rd1, rd3, rd2), (ra1, ra3, ra2), (rb1, rb3, rb2), (rc1, rc3, rc2)
    pas, pbs, outs = (pa1, pa3, pa2), (pb1, pb3, pb2), (s1, s3, s2)
    order = ((nx, ny, nz), (ny, nz, nx), (nz, nx, ny))

    def gather_slice(m, stage, k):
        s = lax.rem(k, WS)
        w = weights[m]
        if m == 0:
            return (w.at[s, c, z, y, x], w.at[s, c, z, y], w.at[s, c, z], w.at[s, c])[stage]
        if m == 1:
            return (w.at[s, c, z, y, x], w.at[s, c, z, :, x], w.at[s, c, :, :, x], w.at[s, c])[stage]
        return (w.at[s, z, y, x, c], w.at[s, :, y, x, c], w.at[s, :, y, :, c], w.at[s, :, :, :, c])[stage]

    def own_block(m, k):
        layer = LAYERS - 1 - k // NC
        i = lax.rem(k, NC)
        if m == 2:
            return w2_hbm.at[layer, pl.ds(pl.multiple_of(i * CPD, CPD), CPD)]
        return (w1_hbm, w3_hbm)[m].at[layer, i]

    def gather_copy(m, stage, k):
        par = lax.rem(k, 2)
        dst = gather_slice(m, stage, k)
        src = own_block(m, k) if stage == 0 else dst
        peer = core if stage == 3 else order[m][stage]
        return pltpu.make_async_remote_copy(
            src_ref=src, dst_ref=dst, send_sem=ag_send.at[m, stage, par], recv_sem=ag_recv.at[m, stage, par],
            device_id=(peer,), device_id_type=MESH)

    def own_copy(m, k):
        return pltpu.make_async_copy(own_block(m, k), gather_slice(m, 0, k), own_sem.at[m])

    def reduce_copy(m, stage, k):
        par = lax.rem(k, 2)
        g, pa, pb = grads[m], pas[m], pbs[m]
        if stage == 0:
            src, dst, peer = g.at[par, :, :, :, 1 - c], rds[m].at[par], core
        elif stage == 1:
            src = (g.at[par, :, :, 1 - x, c], g.at[par, :, 1 - y, :, c], g.at[par, 1 - z, :, :, c])[m]
            dst, peer = ras[m].at[par], order[m][0]
        elif stage == 2:
            src = (pa.at[:, 1 - y], pa.at[1 - z], pa.at[:, 1 - x])[m]
            dst, peer = rbs[m].at[par], order[m][1]
        else:
            src = (pb.at[1 - z], pb.at[1 - x], pb.at[1 - y])[m]
            dst, peer = rcs[m].at[par], order[m][2]
        return pltpu.make_async_remote_copy(
            src_ref=src, dst_ref=dst, send_sem=rs_send.at[m, stage, par], recv_sem=rs_recv.at[m, stage, par],
            device_id=(peer,), device_id_type=MESH)

    def out_copy(m, k):
        layer = LAYERS - 1 - k // NC
        i = lax.rem(k, NC)
        if m == 2:
            dst = o2_hbm.at[layer, pl.ds(pl.multiple_of(i * CPD, CPD), CPD)]
        else:
            dst = (o1_hbm, o3_hbm)[m].at[layer, i]
        return pltpu.make_async_copy(outs[m], dst, out_sem.at[m])

    def h_copy(li):
        return pltpu.make_async_copy(h_hbm.at[LAYERS - 1 - li], h_v.at[lax.rem(li, 2)], h_sem.at[lax.rem(li, 2)])

    def g_copy():
        return pltpu.make_async_copy(g_hbm, g_v, g_sem)

    def finalize_rows(li, r0):
        rows = pl.ds(r0, BB)
        hf = h_v[lax.rem(li, 2), rows, :].astype(F32)
        r = lax.rsqrt(jnp.mean(hf * hf, axis=-1, keepdims=True) + EPS)
        m = hf * r
        dn = dn_v[rows, :]
        dr = r * (dn - m * jnp.mean(dn * m, axis=-1, keepdims=True))
        g_v[rows, :] = (g_v[rows, :].astype(F32) + dr).astype(BF)

    def prepare_rows(li, r0):
        rows = pl.ds(r0, BB)
        hf = h_v[lax.rem(li, 2), rows, :].astype(F32)
        r = lax.rsqrt(jnp.mean(hf * hf, axis=-1, keepdims=True) + EPS)
        nb = (hf * r).astype(BF)
        n_v[rows, :] = nb
        nt_v[:, rows] = nb.T
        gt_v[:, rows] = g_v[rows, :].T
        dn_v[rows, :] = jnp.zeros((BB, D), F32)

    def gather_step(k):
        @pl.when((k >= 0) & (k < NK))
        def _():
            for m in range(3):
                gather_copy(m, 3, k).wait()

        for lag, stage in ((1, 2), (2, 1), (3, 0)):
            @pl.when((k + lag >= 0) & (k + lag < NK))
            def _():
                for m in range(3):
                    gather_copy(m, stage, k + lag).wait()
                    if stage == 0:
                        own_copy(m, k + lag).wait()

        for lag, stage in ((1, 3), (2, 2), (3, 1), (4, 0)):
            @pl.when((k + lag >= 0) & (k + lag < NK))
            def _():
                for m in range(3):
                    gather_copy(m, stage, k + lag).start()
                    if stage == 0:
                        own_copy(m, k + lag).start()

        @pl.when((k >= 1) & (k <= NK))
        def _():
            for m in range(3):
                reduce_copy(m, 0, k - 1).start()

    def reduce_step(k):
        def live(lag):
            return (k - lag >= 0) & (k - lag < NK)

        @pl.when(live(4))
        def _():
            kf = k - 4
            par = lax.rem(kf, 2)

            @pl.when(kf >= 1)
            def _():
                for m in range(3):
                    out_copy(m, kf - 1).wait()
            for m in range(3):
                reduce_copy(m, 3, kf).wait()
                keep = (z, x, y)[m]
                outs[m][...] = rcs[m][par] + pbs[m][keep]
                out_copy(m, kf).start()

        @pl.when(live(3))
        def _():
            kf = k - 3
            par = lax.rem(kf, 2)
            for m in range(3):
                reduce_copy(m, 2, kf).wait()
                for a in range(2):
                    kept = (lambda: pa1[a, y], lambda: pa3[z, a], lambda: pa2[a, x])[m]()
                    pbs[m][a] = rbs[m][par, a] + kept

        @pl.when(live(2))
        def _():
            kf = k - 2
            par = lax.rem(kf, 2)
            for m in range(3):
                reduce_copy(m, 1, kf).wait()
                for a in range(2):
                    for b in range(2):
                        kept = (lambda: g1_v[par, a, b, x, c], lambda: g3_v[par, a, y, b, c], lambda: g2_v[par, z, a, b, c])[m]()
                        pas[m][a, b] = ras[m][par, a, b] + kept

        @pl.when(live(1))
        def _():
            kf = k - 1
            par = lax.rem(kf, 2)
            for m in range(3):
                reduce_copy(m, 0, kf).wait()
                for a in range(2):
                    for b in range(2):
                        for d in range(2):
                            grads[m][par, a, b, d, c] = grads[m][par, a, b, d, c] + rds[m][par, a, b, d]

        for lag, stage in ((3, 3), (2, 2), (1, 1)):
            @pl.when(live(lag))
            def _():
                for m in range(3):
                    reduce_copy(m, stage, k - lag).start()

    def row_phase(k):
        s = lax.rem(k, WS)

        def body(b, carry):
            rows = pl.ds(pl.multiple_of(b * RB, RB), RB)
            w1 = jnp.concatenate([w1_v[s, 0].reshape(D, HALF), w1_v[s, 1].reshape(D, HALF)], axis=1)
            w3 = jnp.concatenate([w3_v[s, 0].reshape(D, HALF), w3_v[s, 1].reshape(D, HALF)], axis=1)
            w2 = w2_v[s].reshape(CH, D)
            nb = n_v[rows, :]
            u = dot(nb, w1, 1, 0)
            v = dot(nb, w3, 1, 0)
            da = jnp.concatenate([dot(g_v[pl.ds(pl.multiple_of(b * RB + q * (RB // 2), RB // 2), RB // 2), :], w2, 1, 1) for q in range(2)], axis=0)
            sig = 1.0 / (1.0 + jnp.exp(-u))
            act = u * sig
            a_v[rows, :] = (act * v).astype(BF)
            du = (da * v * sig * (1.0 + u * (1.0 - sig))).astype(BF)
            dv = (da * act).astype(BF)
            d_v[rows, pl.ds(0, CH)] = du
            d_v[rows, pl.ds(CH, CH)] = dv
            for q in range(2):
                rq = slice(q * (RB // 2), (q + 1) * (RB // 2))
                rr = pl.ds(pl.multiple_of(b * RB + q * (RB // 2), RB // 2), RB // 2)
                dn_v[rr, :] += dot(du[rq], w1, 1, 1) + dot(dv[rq], w3, 1, 1)
            return carry

        lax.fori_loop(0, ROWS // RB, body, 0)

    def grad_phase(k):
        par = lax.rem(k, 2)
        nt = nt_v[...]
        g1_v[par] = dot(nt, d_v[:, pl.ds(0, CH)], 1, 0).reshape(2, 2, 2, 2, DS, CH)
        g3_v[par] = dot(nt, d_v[:, pl.ds(CH, CH)], 1, 0).reshape(2, 2, 2, 2, DS, CH)
        g2_v[par] = dot(gt_v[...], a_v[...], 1, 0).T.reshape(2, 2, 2, 2, CPD, D)

    h_copy(0).start()
    g_copy().start()
    h_copy(1).start()

    def step(t, carry):
        k = t - LEAD

        @pl.when(t == 0)
        def _():
            pass

        @pl.when((k == NC) | (k == 2 * NC) | (k == NK))
        def _():
            li = k // NC

            def rows(b, cc):
                finalize_rows(li - 1, pl.multiple_of(b * BB, BB))
                return cc
            lax.fori_loop(0, ROWS // BB, rows, 0)

            @pl.when(li < LAYERS)
            def _():
                h_copy(li).wait()

                def rows2(b, cc):
                    prepare_rows(li, pl.multiple_of(b * BB, BB))
                    return cc
                lax.fori_loop(0, ROWS // BB, rows2, 0)

            @pl.when(li < LAYERS - 1)
            def _():
                h_copy(li + 1).start()

            @pl.when(li == LAYERS)
            def _():
                pltpu.make_async_copy(g_v, og_hbm, g_sem).start()

        gather_step(k)

        @pl.when(k < 0)
        def _():
            @pl.when(t == 0)
            def _():
                h_copy(0).wait()
                g_copy().wait()
            for j in range(ROWS // BB // LEAD):
                prepare_rows(0, pl.multiple_of((t * (ROWS // BB // LEAD) + j) * BB, BB))

        @pl.when((k >= 0) & (k < NK))
        def _():
            row_phase(k)

        reduce_step(k)

        @pl.when((k >= 0) & (k < NK))
        def _():
            grad_phase(k)
        return carry

    lax.fori_loop(0, LEAD + NK + TAIL, step, 0)
    for m in range(3):
        out_copy(m, NK - 1).wait()
    pltpu.make_async_copy(g_v, og_hbm, g_sem).wait()


def fused(h, g, w1, w3, w2):
    any_spec = pl.BlockSpec(memory_space=pl.ANY)
    V = pltpu.VMEM
    wide, low = (DS, CH), (CPD, D)
    three = lambda *lead: [V(lead + wide, F32), V(lead + wide, F32), V(lead + low, F32)]
    scratch = [
        V((ROWS, D), BF), V((D, ROWS), BF), V((ROWS, D), BF), V((D, ROWS), BF),
        V((ROWS, D), F32), V((2, ROWS, D), BF), V((ROWS, CH), BF), V((ROWS, 2 * CH), BF),
        V((WS, 2, 2, 2, 2, 2 * DS, HALF), BF), V((WS, 2, 2, 2, 2, 2 * DS, HALF), BF), V((WS, 2, 2, 2, 2, CPD, D), BF),
        *three(2, 2, 2, 2, 2),
        *three(2, 2, 2, 2), *three(2, 2, 2), *three(2, 2), *three(2),
        *three(2, 2), *three(2), *three(),
        pltpu.SemaphoreType.DMA((3, 4, 2)), pltpu.SemaphoreType.DMA((3, 4, 2)),
        pltpu.SemaphoreType.DMA((3, 4, 2)), pltpu.SemaphoreType.DMA((3, 4, 2)),
        pltpu.SemaphoreType.DMA((3,)), pltpu.SemaphoreType.DMA((3,)),
        pltpu.SemaphoreType.DMA((2,)), pltpu.SemaphoreType.DMA(()),
    ]
    return pl.pallas_call(
        kernel,
        name='mlp_backward',
        out_shape=(
            jax.ShapeDtypeStruct((LAYERS, NC, DS, CH), F32),
            jax.ShapeDtypeStruct((LAYERS, NC, DS, CH), F32),
            jax.ShapeDtypeStruct((LAYERS, FS, D), F32),
            jax.ShapeDtypeStruct((ROWS, D), BF),
        ),
        in_specs=[any_spec] * 5,
        out_specs=(any_spec,) * 4,
        scratch_shapes=scratch,
        compiler_params=pltpu.CompilerParams(collective_id=0, has_side_effects=True, vmem_limit_bytes=67_043_328),
    )(h, g, w1, w3, w2)


def chunk_columns(w):
    w = w.reshape(LAYERS, DS, DEV, NC, CPD).transpose(0, 3, 1, 2, 4).reshape(LAYERS, NC, DS, CH)
    c = lax.axis_index('fsdp') % 2
    first = c == 0
    mine = jnp.where(first, w[..., :HALF], w[..., HALF:])
    sent = jnp.where(first, w[..., HALF:], w[..., :HALF])
    got = lax.ppermute(sent, 'fsdp', [(p, p ^ 1) for p in range(DEV)])
    return jnp.concatenate([jnp.where(first, mine, got), jnp.where(first, got, mine)], axis=2)


def restore_columns(o):
    return o.reshape(LAYERS, NC, DS, DEV, CPD).transpose(0, 2, 3, 1, 4).reshape(LAYERS, DS, FF)


def solution(mesh):
    weight_spec = P(None, 'fsdp', None)
    row_spec = P('fsdp', None)

    def local(h_saved, g_out, w_gate, w_up, w_down):
        o1, o3, o2, g = fused(h_saved, g_out, chunk_columns(w_gate), chunk_columns(w_up), w_down)
        return restore_columns(o1), restore_columns(o3), o2, g

    return jax.shard_map(local, mesh=mesh, in_specs=(weight_spec, row_spec, weight_spec, weight_spec, weight_spec), out_specs=(weight_spec, weight_spec, weight_spec, row_spec), check_vma=False)
```

```python
import jax
import jax.numpy as jnp
from jax import lax
from jax.experimental import pallas as pl
from jax.experimental.pallas import tpu as pltpu
from jax.sharding import PartitionSpec as P

EPS = 1e-6
LAYERS = 3
D = 896
FF = 4864
ROWS = 2048
DEV = 16
DS = D // DEV
FS = FF // DEV
CPD = 16
CH = CPD * DEV
NC = FF // CH
NK = NC * LAYERS
LEAD = 5
TAIL = 4
WS = 6
RB = 1024
BB = 256
HALF = CH // 2
LANES = 128
NB = ROWS // BB
MESH = pl.DeviceIdType.MESH
BF = jnp.bfloat16
F32 = jnp.float32


def dot(a, b, ca, cb):
    return lax.dot_general(a, b, (((ca,), (cb,)), ((), ())), preferred_element_type=F32)


def kernel(h_hbm, g_hbm, w1_hbm, w3_hbm, w2_hbm,
           o1_hbm, o3_hbm, o2_hbm, og_hbm,
           n_v, nt_v, g_v, gt_v, dn_v, h_v, a_v, d_v,
           c1_v, c3_v, e1_v, e3_v, f1_v, f3_v, t1_v, t3_v,
           w1_v, w3_v, w2_v,
           g1_v, g3_v, g2_v,
           rd1, rd3, rd2, ra1, ra3, ra2, rb1, rb3, rb2, rc1, rc3, rc2,
           pa1, pa3, pa2, pb1, pb3, pb2, s2,
           ag_send, ag_recv, rs_send, rs_recv, ex_send, ex_recv, own_sem, out_sem, cols_sem, h_sem, g_sem):
    me = lax.axis_index('fsdp')
    c = me % 2
    x = (me // 2) % 2
    y = (me // 4) % 2
    z = (me // 8) % 2
    core = me + 1 - 2 * c
    nx = me + 2 - 4 * x
    ny = me + 4 - 8 * y
    nz = me + 8 - 16 * z

    barrier = pltpu.get_barrier_semaphore()
    for peer in (core, nx, ny, nz):
        pl.semaphore_signal(barrier, inc=1, device_id=(peer,), device_id_type=MESH)
    pl.semaphore_wait(barrier, 4)

    weights = (w1_v, w3_v, w2_v)
    grads = (g1_v, g3_v, g2_v)
    rds, ras, rbs, rcs = (rd1, rd3, rd2), (ra1, ra3, ra2), (rb1, rb3, rb2), (rc1, rc3, rc2)
    pas, pbs, outs = (pa1, pa3, pa2), (pb1, pb3, pb2), (t1_v, t3_v, s2)
    cols, halves, theirs = (c1_v, c3_v), (e1_v, e3_v), (f1_v, f3_v)
    order = ((nx, ny, nz), (ny, nz, nx), (nz, nx, ny))

    def gather_slice(m, stage, k):
        s = lax.rem(k, WS)
        w = weights[m]
        if m == 0:
            return (w.at[s, c, z, y, x], w.at[s, c, z, y], w.at[s, c, z], w.at[s, c])[stage]
        if m == 1:
            return (w.at[s, c, z, y, x], w.at[s, c, z, :, x], w.at[s, c, :, :, x], w.at[s, c])[stage]
        return (w.at[s, z, y, x, c], w.at[s, :, y, x, c], w.at[s, :, y, :, c], w.at[s, :, :, :, c])[stage]

    def own_rows(k):
        return w2_hbm.at[LAYERS - 1 - k // NC, pl.ds(pl.multiple_of(lax.rem(k, NC) * CPD, CPD), CPD)]

    def gather_copy(m, stage, k):
        par = lax.rem(k, 2)
        dst = gather_slice(m, stage, k)
        src = own_rows(k) if (stage == 0 and m == 2) else dst
        peer = core if stage == 3 else order[m][stage]
        return pltpu.make_async_remote_copy(
            src_ref=src, dst_ref=dst, send_sem=ag_send.at[m, stage, par], recv_sem=ag_recv.at[m, stage, par],
            device_id=(peer,), device_id_type=MESH)

    def own_copy(k):
        return pltpu.make_async_copy(own_rows(k), gather_slice(2, 0, k), own_sem)

    def cols_copy(m, li):
        slot = lax.rem(li, 2)
        return pltpu.make_async_copy((w1_hbm, w3_hbm)[m].at[LAYERS - 1 - li], cols[m].at[slot], cols_sem.at[m, slot])

    def half_copy(m, k):
        par = lax.rem(k, 2)
        return pltpu.make_async_remote_copy(
            src_ref=halves[m].at[1 - c], dst_ref=theirs[m].at[par], send_sem=ex_send.at[m, par], recv_sem=ex_recv.at[m, par],
            device_id=(core,), device_id_type=MESH)

    lane = lax.broadcasted_iota(jnp.int32, (DS, LANES), 1)

    def place(p, i):
        col = FS * p + CPD * i
        tile = col // LANES
        return pl.ds(pl.multiple_of(tile * LANES, LANES), LANES), col - tile * LANES

    def pick_columns(k):
        li = k // NC
        i = lax.rem(k, NC)
        slot = lax.rem(li, 2)
        for m in range(2):
            for half in range(2):
                acc = jnp.zeros((DS, LANES), F32)
                for q in range(DEV // 2):
                    tile, off = place(half * (DEV // 2) + q, i)
                    part = pltpu.roll(cols[m][slot, :, tile].astype(F32), lax.rem(CPD * q + LANES - off, LANES), 1)
                    acc = jnp.where((lane >= CPD * q) & (lane < CPD * (q + 1)), part, acc)
                halves[m][half] = acc

    def merge_rows(k):
        par = lax.rem(k, 2)
        for m in range(2):
            mine, other = halves[m][c], theirs[m][par]
            low = jnp.where(c == 0, mine, other)
            high = jnp.where(c == 0, other, mine)
            weights[m][lax.rem(k, WS), c, z, y, x] = jnp.concatenate([low, high], axis=0).astype(BF)

    def put_columns(m, i, value):
        for half in range(2):
            src = value[:, half * LANES:(half + 1) * LANES]
            for q in range(DEV // 2):
                tile, off = place(half * (DEV // 2) + q, i)
                part = pltpu.roll(src, lax.rem(off + LANES - CPD * q, LANES), 1)
                outs[m][:, tile] = jnp.where((lane >= off) & (lane < off + CPD), part, outs[m][:, tile])

    def reduce_copy(m, stage, k):
        par = lax.rem(k, 2)
        g, pa, pb = grads[m], pas[m], pbs[m]
        if stage == 0:
            src, dst, peer = g.at[par, :, :, :, 1 - c], rds[m].at[par], core
        elif stage == 1:
            src = (g.at[par, :, :, 1 - x, c], g.at[par, :, 1 - y, :, c], g.at[par, 1 - z, :, :, c])[m]
            dst, peer = ras[m].at[par], order[m][0]
        elif stage == 2:
            src = (pa.at[:, 1 - y], pa.at[1 - z], pa.at[:, 1 - x])[m]
            dst, peer = rbs[m].at[par], order[m][1]
        else:
            src = (pb.at[1 - z], pb.at[1 - x], pb.at[1 - y])[m]
            dst, peer = rcs[m].at[par], order[m][2]
        return pltpu.make_async_remote_copy(
            src_ref=src, dst_ref=dst, send_sem=rs_send.at[m, stage, par], recv_sem=rs_recv.at[m, stage, par],
            device_id=(peer,), device_id_type=MESH)

    def out_copy(m, k):
        layer = LAYERS - 1 - k // NC
        if m == 2:
            dst = o2_hbm.at[layer, pl.ds(pl.multiple_of(lax.rem(k, NC) * CPD, CPD), CPD)]
        else:
            dst = (o1_hbm, o3_hbm)[m].at[layer]
        return pltpu.make_async_copy(outs[m], dst, out_sem.at[m])

    def h_copy(li, b):
        rows = pl.ds(pl.multiple_of(b * BB, BB), BB)
        return pltpu.make_async_copy(h_hbm.at[LAYERS - 1 - li, rows], h_v.at[rows], h_sem.at[b])

    def g_copy():
        return pltpu.make_async_copy(g_hbm, g_v, g_sem)

    def finalize_rows(r0):
        rows = pl.ds(r0, BB)
        hf = h_v[rows, :].astype(F32)
        r = lax.rsqrt(jnp.mean(hf * hf, axis=-1, keepdims=True) + EPS)
        m = hf * r
        dn = dn_v[rows, :]
        dr = r * (dn - m * jnp.mean(dn * m, axis=-1, keepdims=True))
        g_v[rows, :] = (g_v[rows, :].astype(F32) + dr).astype(BF)

    def prepare_rows(r0):
        rows = pl.ds(r0, BB)
        hf = h_v[rows, :].astype(F32)
        r = lax.rsqrt(jnp.mean(hf * hf, axis=-1, keepdims=True) + EPS)
        nb = (hf * r).astype(BF)
        n_v[rows, :] = nb
        nt_v[:, rows] = nb.T
        gt_v[:, rows] = g_v[rows, :].T
        dn_v[rows, :] = jnp.zeros((BB, D), F32)

    def gather_step(k):
        @pl.when((k >= 0) & (k < NK))
        def _():
            for m in range(3):
                gather_copy(m, 3, k).wait()

        for lag, stage in ((1, 2), (2, 1), (3, 0)):
            @pl.when((k + lag >= 0) & (k + lag < NK))
            def _():
                for m in range(3):
                    gather_copy(m, stage, k + lag).wait()
                if stage == 0:
                    own_copy(k + lag).wait()

        for lag, stage in ((1, 3), (2, 2), (3, 1), (4, 0)):
            @pl.when((k + lag >= 0) & (k + lag < NK))
            def _():
                for m in range(3):
                    gather_copy(m, stage, k + lag).start()
                if stage == 0:
                    own_copy(k + lag).start()

        @pl.when((k >= 1) & (k <= NK))
        def _():
            for m in range(3):
                reduce_copy(m, 0, k - 1).start()

        @pl.when(k + 5 < NK)
        def _():
            kn = k + 5
            li = kn // NC

            @pl.when(lax.rem(kn, NC) == 0)
            def _():
                for m in range(2):
                    cols_copy(m, li).wait()
            pick_columns(kn)
            for m in range(2):
                half_copy(m, kn).start()

            @pl.when((lax.rem(kn, NC) == NC - 1) & (li == 0))
            def _():
                for m in range(2):
                    cols_copy(m, 2).start()

    def reduce_step(k):
        def live(lag):
            return (k - lag >= 0) & (k - lag < NK)

        @pl.when(k + 5 < NK)
        def _():
            for m in range(2):
                half_copy(m, k + 5).wait()
            merge_rows(k + 5)

        @pl.when(live(4))
        def _():
            kf = k - 4
            par = lax.rem(kf, 2)

            i = lax.rem(kf, NC)

            @pl.when(kf >= 1)
            def _():
                out_copy(2, kf - 1).wait()

            @pl.when((kf >= 1) & (i == 0))
            def _():
                for m in range(2):
                    out_copy(m, kf - 1).wait()
            for m in range(3):
                reduce_copy(m, 3, kf).wait()
                done = rcs[m][par] + pbs[m][(z, x, y)[m]]
                if m == 2:
                    s2[...] = done
                else:
                    put_columns(m, i, done)
            out_copy(2, kf).start()

            @pl.when(i == NC - 1)
            def _():
                for m in range(2):
                    out_copy(m, kf).start()

        @pl.when(live(3))
        def _():
            kf = k - 3
            par = lax.rem(kf, 2)
            for m in range(3):
                reduce_copy(m, 2, kf).wait()
                for a in range(2):
                    kept = (lambda: pa1[a, y], lambda: pa3[z, a], lambda: pa2[a, x])[m]()
                    pbs[m][a] = rbs[m][par, a] + kept

        @pl.when(live(2))
        def _():
            kf = k - 2
            par = lax.rem(kf, 2)
            for m in range(3):
                reduce_copy(m, 1, kf).wait()
                for a in range(2):
                    for b in range(2):
                        kept = (lambda: g1_v[par, a, b, x, c], lambda: g3_v[par, a, y, b, c], lambda: g2_v[par, z, a, b, c])[m]()
                        pas[m][a, b] = ras[m][par, a, b] + kept

        @pl.when(live(1))
        def _():
            kf = k - 1
            par = lax.rem(kf, 2)
            for m in range(3):
                reduce_copy(m, 0, kf).wait()
                for a in range(2):
                    for b in range(2):
                        for d in range(2):
                            grads[m][par, a, b, d, c] = grads[m][par, a, b, d, c] + rds[m][par, a, b, d]

        for lag, stage in ((3, 3), (2, 2), (1, 1)):
            @pl.when(live(lag))
            def _():
                for m in range(3):
                    reduce_copy(m, stage, k - lag).start()

    def row_phase(k):
        s = lax.rem(k, WS)

        def body(b, carry):
            rows = pl.ds(pl.multiple_of(b * RB, RB), RB)
            w1 = jnp.concatenate([w1_v[s, 0].reshape(D, HALF), w1_v[s, 1].reshape(D, HALF)], axis=1)
            w3 = jnp.concatenate([w3_v[s, 0].reshape(D, HALF), w3_v[s, 1].reshape(D, HALF)], axis=1)
            w2 = w2_v[s].reshape(CH, D)
            nb = n_v[rows, :]
            u = dot(nb, w1, 1, 0)
            v = dot(nb, w3, 1, 0)
            da = jnp.concatenate([dot(g_v[pl.ds(pl.multiple_of(b * RB + q * (RB // 2), RB // 2), RB // 2), :], w2, 1, 1) for q in range(2)], axis=0)
            sig = 1.0 / (1.0 + jnp.exp(-u))
            act = u * sig
            a_v[rows, :] = (act * v).astype(BF)
            du = (da * v * sig * (1.0 + u * (1.0 - sig))).astype(BF)
            dv = (da * act).astype(BF)
            d_v[rows, pl.ds(0, CH)] = du
            d_v[rows, pl.ds(CH, CH)] = dv
            for q in range(2):
                rq = slice(q * (RB // 2), (q + 1) * (RB // 2))
                rr = pl.ds(pl.multiple_of(b * RB + q * (RB // 2), RB // 2), RB // 2)
                dn_v[rr, :] += dot(du[rq], w1, 1, 1) + dot(dv[rq], w3, 1, 1)
            return carry

        lax.fori_loop(0, ROWS // RB, body, 0)

    def grad_phase(k):
        par = lax.rem(k, 2)
        nt = nt_v[...]
        g1_v[par] = dot(nt, d_v[:, pl.ds(0, CH)], 1, 0).reshape(2, 2, 2, 2, DS, CH)
        g3_v[par] = dot(nt, d_v[:, pl.ds(CH, CH)], 1, 0).reshape(2, 2, 2, 2, DS, CH)
        g2_v[par] = dot(gt_v[...], a_v[...], 1, 0).T.reshape(2, 2, 2, 2, CPD, D)

    for m in range(2):
        cols_copy(m, 0).start()
    for b in range(NB):
        h_copy(0, b).start()
    g_copy().start()
    for m in range(2):
        cols_copy(m, 1).start()

    def step(t, carry):
        k = t - LEAD
        inside = (k >= 0) & (k < NK)
        last = inside & (lax.rem(k + NC, NC) == NC - 1)
        gather_step(k)

        @pl.when((t >= 1) & (t < LEAD))
        def _():
            @pl.when(t == 1)
            def _():
                for b in range(NB):
                    h_copy(0, b).wait()
                g_copy().wait()
            per = NB // (LEAD - 1)
            for j in range(per):
                prepare_rows(pl.multiple_of(((t - 1) * per + j) * BB, BB))

        @pl.when(inside)
        def _():
            row_phase(k)

        @pl.when(last)
        def _():
            li = k // NC

            def rows(b, cc):
                finalize_rows(pl.multiple_of(b * BB, BB))

                @pl.when(li < LAYERS - 1)
                def _():
                    h_copy(li + 1, b).start()
                return cc
            lax.fori_loop(0, NB, rows, 0)

            @pl.when(li == LAYERS - 1)
            def _():
                pltpu.make_async_copy(g_v, og_hbm, g_sem).start()

        reduce_step(k)

        @pl.when(inside)
        def _():
            grad_phase(k)

        @pl.when(last & (k < NK - 1))
        def _():
            li = k // NC

            def rows(b, cc):
                h_copy(li + 1, b).wait()
                prepare_rows(pl.multiple_of(b * BB, BB))
                return cc
            lax.fori_loop(0, NB, rows, 0)
        return carry

    lax.fori_loop(0, LEAD + NK + TAIL, step, 0)
    for m in range(3):
        out_copy(m, NK - 1).wait()
    pltpu.make_async_copy(g_v, og_hbm, g_sem).wait()


def fused(h, g, w1, w3, w2):
    any_spec = pl.BlockSpec(memory_space=pl.ANY)
    V = pltpu.VMEM
    wide, low = (DS, CH), (CPD, D)
    three = lambda *lead: [V(lead + wide, F32), V(lead + wide, F32), V(lead + low, F32)]
    scratch = [
        V((ROWS, D), BF), V((D, ROWS), BF), V((ROWS, D), BF), V((D, ROWS), BF),
        V((ROWS, D), F32), V((ROWS, D), BF), V((ROWS, CH), BF), V((ROWS, 2 * CH), BF),
        V((2, DS, FF), BF), V((2, DS, FF), BF), V((2, DS, LANES), F32), V((2, DS, LANES), F32),
        V((2, DS, LANES), F32), V((2, DS, LANES), F32), V((DS, FF), F32), V((DS, FF), F32),
        V((WS, 2, 2, 2, 2, 2 * DS, HALF), BF), V((WS, 2, 2, 2, 2, 2 * DS, HALF), BF), V((WS, 2, 2, 2, 2, CPD, D), BF),
        *three(2, 2, 2, 2, 2),
        *three(2, 2, 2, 2), *three(2, 2, 2), *three(2, 2), *three(2),
        *three(2, 2), *three(2), V(low, F32),
        pltpu.SemaphoreType.DMA((3, 4, 2)), pltpu.SemaphoreType.DMA((3, 4, 2)),
        pltpu.SemaphoreType.DMA((3, 4, 2)), pltpu.SemaphoreType.DMA((3, 4, 2)),
        pltpu.SemaphoreType.DMA((2, 2)), pltpu.SemaphoreType.DMA((2, 2)),
        pltpu.SemaphoreType.DMA(()), pltpu.SemaphoreType.DMA((3,)), pltpu.SemaphoreType.DMA((2, 2)),
        pltpu.SemaphoreType.DMA((NB,)), pltpu.SemaphoreType.DMA(()),
    ]
    return pl.pallas_call(
        kernel,
        name='mlp_backward',
        out_shape=(
            jax.ShapeDtypeStruct((LAYERS, DS, FF), F32),
            jax.ShapeDtypeStruct((LAYERS, DS, FF), F32),
            jax.ShapeDtypeStruct((LAYERS, FS, D), F32),
            jax.ShapeDtypeStruct((ROWS, D), BF),
        ),
        in_specs=[any_spec] * 5,
        out_specs=(any_spec,) * 4,
        scratch_shapes=scratch,
        compiler_params=pltpu.CompilerParams(collective_id=0, has_side_effects=True, vmem_limit_bytes=67_043_328),
    )(h, g, w1, w3, w2)


def solution(mesh):
    weight_spec = P(None, 'fsdp', None)
    row_spec = P('fsdp', None)

    return jax.shard_map(fused, mesh=mesh, in_specs=(weight_spec, row_spec, weight_spec, weight_spec, weight_spec), out_specs=(weight_spec, weight_spec, weight_spec, row_spec), check_vma=False)
```

```python
import jax
import jax.numpy as jnp
from jax import lax
from jax.experimental import pallas as pl
from jax.experimental.pallas import tpu as pltpu
from jax.sharding import PartitionSpec as P

EPS = 1e-6
LAYERS = 3
D = 896
FF = 4864
ROWS = 2048
DEV = 16
DS = D // DEV
FS = FF // DEV
CPD = 16
CH = CPD * DEV
NC = FF // CH
NK = NC * LAYERS
LEAD = 5
TAIL = 4
WS = 6
RB = 1024
BB = 256
HALF = CH // 2
LANES = 128
NB = ROWS // BB
MESH = pl.DeviceIdType.MESH
BF = jnp.bfloat16
F32 = jnp.float32


def dot(a, b, ca, cb):
    return lax.dot_general(a, b, (((ca,), (cb,)), ((), ())), preferred_element_type=F32)


def kernel(h_hbm, g_hbm, w1_hbm, w3_hbm, w2_hbm,
           o1_hbm, o3_hbm, o2_hbm, og_hbm,
           n_v, nt_v, g_v, gt_v, dn_v, h_v, a_v, d_v,
           c1_v, c3_v, e1_v, e3_v, f1_v, f3_v, t1_v, t3_v,
           w1_v, w3_v, w2_v,
           g1_v, g3_v, g2_v,
           rd1, rd3, rd2, ra1, ra3, ra2, rb1, rb3, rb2, rc1, rc3, rc2,
           pa1, pa3, pa2, pb1, pb3, pb2, s1, s3, s2,
           ag_send, ag_recv, rs_send, rs_recv, ex_send, ex_recv, own_sem, out_sem, cols_sem, h_sem, g_sem):
    me = lax.axis_index('fsdp')
    c = me % 2
    x = (me // 2) % 2
    y = (me // 4) % 2
    z = (me // 8) % 2
    core = me + 1 - 2 * c
    nx = me + 2 - 4 * x
    ny = me + 4 - 8 * y
    nz = me + 8 - 16 * z

    barrier = pltpu.get_barrier_semaphore()
    for peer in (core, nx, ny, nz):
        pl.semaphore_signal(barrier, inc=1, device_id=(peer,), device_id_type=MESH)
    weights = (w1_v, w3_v, w2_v)
    grads = (g1_v, g3_v, g2_v)
    rds, ras, rbs, rcs = (rd1, rd3, rd2), (ra1, ra3, ra2), (rb1, rb3, rb2), (rc1, rc3, rc2)
    pas, pbs, outs = (pa1, pa3, pa2), (pb1, pb3, pb2), (t1_v, t3_v, s2)
    dones = (s1, s3, s2)
    cols, halves, theirs = (c1_v, c3_v), (e1_v, e3_v), (f1_v, f3_v)
    order = ((nx, ny, nz), (ny, nz, nx), (nz, nx, ny))

    def gather_slice(m, stage, k):
        s = lax.rem(k, WS)
        w = weights[m]
        if m == 0:
            return (w.at[s, c, z, y, x], w.at[s, c, z, y], w.at[s, c, z], w.at[s, c])[stage]
        if m == 1:
            return (w.at[s, c, z, y, x], w.at[s, c, z, :, x], w.at[s, c, :, :, x], w.at[s, c])[stage]
        return (w.at[s, z, y, x, c], w.at[s, :, y, x, c], w.at[s, :, y, :, c], w.at[s, :, :, :, c])[stage]

    def own_rows(k):
        return w2_hbm.at[LAYERS - 1 - k // NC, pl.ds(pl.multiple_of(lax.rem(k, NC) * CPD, CPD), CPD)]

    def gather_copy(m, stage, k):
        par = lax.rem(k, 2)
        dst = gather_slice(m, stage, k)
        src = own_rows(k) if (stage == 0 and m == 2) else dst
        peer = core if stage == 3 else order[m][stage]
        return pltpu.make_async_remote_copy(
            src_ref=src, dst_ref=dst, send_sem=ag_send.at[m, stage, par], recv_sem=ag_recv.at[m, stage, par],
            device_id=(peer,), device_id_type=MESH)

    def own_copy(k):
        return pltpu.make_async_copy(own_rows(k), gather_slice(2, 0, k), own_sem)

    def cols_copy(m, li):
        slot = lax.rem(li, 2)
        return pltpu.make_async_copy((w1_hbm, w3_hbm)[m].at[LAYERS - 1 - li], cols[m].at[slot], cols_sem.at[m, slot])

    def half_copy(m, k):
        par = lax.rem(k, 2)
        return pltpu.make_async_remote_copy(
            src_ref=halves[m].at[1 - c], dst_ref=theirs[m].at[par], send_sem=ex_send.at[m, par], recv_sem=ex_recv.at[m, par],
            device_id=(core,), device_id_type=MESH)

    lane = lax.broadcasted_iota(jnp.int32, (DS, LANES), 1)

    def place(p, i):
        col = FS * p + CPD * i
        tile = col // LANES
        return pl.ds(pl.multiple_of(tile * LANES, LANES), LANES), col - tile * LANES

    def pick_columns(k):
        li = k // NC
        i = lax.rem(k, NC)
        slot = lax.rem(li, 2)
        for m in range(2):
            for half in range(2):
                acc = jnp.zeros((DS, LANES), F32)
                for q in range(DEV // 2):
                    tile, off = place(half * (DEV // 2) + q, i)
                    part = pltpu.roll(cols[m][slot, :, tile].astype(F32), lax.rem(CPD * q + LANES - off, LANES), 1)
                    acc = jnp.where((lane >= CPD * q) & (lane < CPD * (q + 1)), part, acc)
                halves[m][half] = acc

    def merge_rows(k):
        par = lax.rem(k, 2)
        for m in range(2):
            mine, other = halves[m][c], theirs[m][par]
            low = jnp.where(c == 0, mine, other)
            high = jnp.where(c == 0, other, mine)
            weights[m][lax.rem(k, WS), c, z, y, x] = jnp.concatenate([low, high], axis=0).astype(BF)

    def put_columns(i):
        for m in range(2):
            put_matrix(m, i)

    def put_matrix(m, i):
        for half in range(2):
            src = dones[m][:, half * LANES:(half + 1) * LANES]
            for q in range(DEV // 2):
                tile, off = place(half * (DEV // 2) + q, i)
                part = pltpu.roll(src, lax.rem(off + LANES - CPD * q, LANES), 1)
                outs[m][:, tile] = jnp.where((lane >= off) & (lane < off + CPD), part, outs[m][:, tile])

    def reduce_copy(m, stage, k):
        par = lax.rem(k, 2)
        slot = lax.rem(k, 3) if stage == 3 else par
        g, pa, pb = grads[m], pas[m].at[par], pbs[m].at[par]
        if stage == 0:
            src, dst, peer = g.at[par, :, :, :, 1 - c], rds[m].at[par], core
        elif stage == 1:
            src = (g.at[par, :, :, 1 - x, c], g.at[par, :, 1 - y, :, c], g.at[par, 1 - z, :, :, c])[m]
            dst, peer = ras[m].at[par], order[m][0]
        elif stage == 2:
            src = (pa.at[:, 1 - y], pa.at[1 - z], pa.at[:, 1 - x])[m]
            dst, peer = rbs[m].at[par], order[m][1]
        else:
            src = (pb.at[1 - z], pb.at[1 - x], pb.at[1 - y])[m]
            dst, peer = rcs[m].at[lax.rem(k, 3)], order[m][2]
        return pltpu.make_async_remote_copy(
            src_ref=src, dst_ref=dst, send_sem=rs_send.at[m, stage, slot], recv_sem=rs_recv.at[m, stage, slot],
            device_id=(peer,), device_id_type=MESH)

    def out_copy(m, k):
        layer = LAYERS - 1 - k // NC
        if m == 2:
            dst = o2_hbm.at[layer, pl.ds(pl.multiple_of(lax.rem(k, NC) * CPD, CPD), CPD)]
        else:
            dst = (o1_hbm, o3_hbm)[m].at[layer]
        return pltpu.make_async_copy(outs[m], dst, out_sem.at[m])

    def h_copy(li, b):
        rows = pl.ds(pl.multiple_of(b * BB, BB), BB)
        return pltpu.make_async_copy(h_hbm.at[LAYERS - 1 - li, rows], h_v.at[rows], h_sem.at[b])

    def g_copy():
        return pltpu.make_async_copy(g_hbm, g_v, g_sem)

    def finalize_rows(r0):
        rows = pl.ds(r0, BB)
        hf = h_v[rows, :].astype(F32)
        r = lax.rsqrt(jnp.mean(hf * hf, axis=-1, keepdims=True) + EPS)
        m = hf * r
        dn = dn_v[rows, :]
        dr = r * (dn - m * jnp.mean(dn * m, axis=-1, keepdims=True))
        g_v[rows, :] = (g_v[rows, :].astype(F32) + dr).astype(BF)

    def prepare_rows(r0):
        rows = pl.ds(r0, BB)
        hf = h_v[rows, :].astype(F32)
        r = lax.rsqrt(jnp.mean(hf * hf, axis=-1, keepdims=True) + EPS)
        nb = (hf * r).astype(BF)
        n_v[rows, :] = nb
        nt_v[:, rows] = nb.T
        gt_v[:, rows] = g_v[rows, :].T
        dn_v[rows, :] = jnp.zeros((BB, D), F32)

    def gather_step(k):
        @pl.when((k >= 1) & (k <= NK))
        def _():
            for m in range(3):
                reduce_copy(m, 0, k - 1).start()

        @pl.when((k >= 0) & (k < NK))
        def _():
            for m in range(3):
                gather_copy(m, 3, k).wait()

        for lag, stage in ((1, 2), (2, 1), (3, 0)):
            @pl.when((k + lag >= 0) & (k + lag < NK))
            def _():
                for m in range(3):
                    gather_copy(m, stage, k + lag).wait()
                if stage == 0:
                    own_copy(k + lag).wait()

        for lag, stage in ((1, 3), (2, 2), (3, 1), (4, 0)):
            @pl.when((k + lag >= 0) & (k + lag < NK))
            def _():
                for m in range(3):
                    gather_copy(m, stage, k + lag).start()
                if stage == 0:
                    own_copy(k + lag).start()

        @pl.when((k <= 0) & (k > -LEAD))
        def _():
            pick_columns(k + 5)

        @pl.when(k + 5 < NK)
        def _():
            for m in range(2):
                half_copy(m, k + 5).start()

        @pl.when(k + 5 == NC - 1)
        def _():
            for m in range(2):
                cols_copy(m, 2).start()

        @pl.when((k + 6 == NC) | (k + 6 == 2 * NC))
        def _():
            for m in range(2):
                cols_copy(m, (k + 6) // NC).wait()

    def reduce_step(k):
        def live(lag):
            return (k - lag >= 0) & (k - lag < NK)

        def finish():
            kf = k - 4
            i = lax.rem(kf, NC)

            @pl.when(kf >= 1)
            def _():
                out_copy(2, kf - 1).wait()

            @pl.when((kf >= 1) & (i == 0))
            def _():
                for m in range(2):
                    out_copy(m, kf - 1).wait()
            for m in range(3):
                reduce_copy(m, 3, kf).wait()
            for m in range(3):
                dones[m][...] = rcs[m][lax.rem(kf, 3)] + pbs[m][lax.rem(kf, 2), (z, x, y)[m]]
            out_copy(2, kf).start()

        def third():
            kf = k - 3
            par = lax.rem(kf, 2)
            for m in range(3):
                reduce_copy(m, 2, kf).wait()
            for m in range(3):
                for a in range(2):
                    kept = (lambda: pa1[par, a, y], lambda: pa3[par, z, a], lambda: pa2[par, a, x])[m]()
                    pbs[m][par, a] = rbs[m][par, a] + kept
            for m in range(3):
                reduce_copy(m, 3, kf).start()

        def second():
            kf = k - 2
            par = lax.rem(kf, 2)
            for m in range(3):
                reduce_copy(m, 1, kf).wait()
            for m in range(3):
                for a in range(2):
                    for b in range(2):
                        kept = (lambda: g1_v[par, a, b, x, c], lambda: g3_v[par, a, y, b, c], lambda: g2_v[par, z, a, b, c])[m]()
                        pas[m][par, a, b] = ras[m][par, a, b] + kept
            for m in range(3):
                reduce_copy(m, 2, kf).start()

        def first():
            kf = k - 1
            par = lax.rem(kf, 2)
            for m in range(3):
                reduce_copy(m, 0, kf).wait()
            for m in range(3):
                for a in range(2):
                    for b in range(2):
                        for d in range(2):
                            grads[m][par, a, b, d, c] = grads[m][par, a, b, d, c] + rds[m][par, a, b, d]
            for m in range(3):
                reduce_copy(m, 1, kf).start()

        @pl.when(k + 5 < NK)
        def _():
            for m in range(2):
                half_copy(m, k + 5).wait()
            merge_rows(k + 5)

        @pl.when(k <= NK)
        def _():
            pl.when(live(4))(finish)
            pl.when(live(3))(third)
            pl.when(live(2))(second)
            pl.when(live(1))(first)

        @pl.when(k > NK)
        def _():
            pl.when(live(2))(second)
            pl.when(live(3))(third)
            pl.when(live(4))(finish)

    def row_phase(k):
        s = lax.rem(k, WS)

        def body(b, carry):
            rows = pl.ds(pl.multiple_of(b * RB, RB), RB)
            w1 = jnp.concatenate([w1_v[s, 0].reshape(D, HALF), w1_v[s, 1].reshape(D, HALF)], axis=1)
            w3 = jnp.concatenate([w3_v[s, 0].reshape(D, HALF), w3_v[s, 1].reshape(D, HALF)], axis=1)
            w2 = w2_v[s].reshape(CH, D)
            nb = n_v[rows, :]
            u = dot(nb, w1, 1, 0)
            v = dot(nb, w3, 1, 0)
            da = jnp.concatenate([dot(g_v[pl.ds(pl.multiple_of(b * RB + q * (RB // 2), RB // 2), RB // 2), :], w2, 1, 1) for q in range(2)], axis=0)
            sig = 1.0 / (1.0 + jnp.exp(-u))
            act = u * sig
            a_v[rows, :] = (act * v).astype(BF)
            du = (da * v * sig * (1.0 + u * (1.0 - sig))).astype(BF)
            dv = (da * act).astype(BF)
            d_v[rows, pl.ds(0, CH)] = du
            d_v[rows, pl.ds(CH, CH)] = dv
            for q in range(2):
                rq = slice(q * (RB // 2), (q + 1) * (RB // 2))
                rr = pl.ds(pl.multiple_of(b * RB + q * (RB // 2), RB // 2), RB // 2)
                dn_v[rr, :] += dot(du[rq], w1, 1, 1) + dot(dv[rq], w3, 1, 1)
            return carry

        lax.fori_loop(0, ROWS // RB, body, 0)

    def grad_phase(k):
        par = lax.rem(k, 2)
        pick_columns(k + 6)
        put_columns(lax.rem(k - 4 + NC, NC))
        nt = nt_v[...]
        g1_v[par] = dot(nt, d_v[:, pl.ds(0, CH)], 1, 0).reshape(2, 2, 2, 2, DS, CH)
        g3_v[par] = dot(nt, d_v[:, pl.ds(CH, CH)], 1, 0).reshape(2, 2, 2, 2, DS, CH)
        g2_v[par] = dot(gt_v[...], a_v[...], 1, 0).T.reshape(2, 2, 2, 2, CPD, D)

    for m in range(2):
        cols_copy(m, 0).start()
    for b in range(NB):
        h_copy(0, b).start()
    g_copy().start()
    for m in range(2):
        cols_copy(m, 1).start()
    for m in range(2):
        cols_copy(m, 0).wait()
    pick_columns(0)
    pl.semaphore_wait(barrier, 4)

    def step(t, carry):
        k = t - LEAD
        inside = (k >= 0) & (k < NK)
        last = inside & (lax.rem(k + NC, NC) == NC - 1)
        gather_step(k)

        @pl.when((t >= 1) & (t < LEAD))
        def _():
            @pl.when(t == 1)
            def _():
                for b in range(NB):
                    h_copy(0, b).wait()
                g_copy().wait()
            per = NB // (LEAD - 1)
            for j in range(per):
                prepare_rows(pl.multiple_of(((t - 1) * per + j) * BB, BB))

        @pl.when(inside)
        def _():
            row_phase(k)

        @pl.when((last & (k < NK - 1)) | (k == NK))
        def _():
            li = k // NC

            def rows(b, cc):
                finalize_rows(pl.multiple_of(b * BB, BB))

                @pl.when(k < NK)
                def _():
                    h_copy(li + 1, b).start()
                return cc
            lax.fori_loop(0, NB, rows, 0)

            @pl.when(k == NK)
            def _():
                pltpu.make_async_copy(g_v, og_hbm, g_sem).start()

        reduce_step(k)

        @pl.when(inside)
        def _():
            grad_phase(k)

        @pl.when(k >= NK)
        def _():
            put_columns(lax.rem(k - 4, NC))

        @pl.when((k >= 4) & (lax.rem(k - 4 + NC, NC) == NC - 1))
        def _():
            for m in range(2):
                out_copy(m, k - 4).start()

        @pl.when(last & (k < NK - 1))
        def _():
            li = k // NC

            def rows(b, cc):
                h_copy(li + 1, b).wait()
                prepare_rows(pl.multiple_of(b * BB, BB))
                return cc
            lax.fori_loop(0, NB, rows, 0)
        return carry

    lax.fori_loop(0, LEAD + NK + TAIL, step, 0)
    for m in range(3):
        out_copy(m, NK - 1).wait()
    pltpu.make_async_copy(g_v, og_hbm, g_sem).wait()


def hand_out(*refs):
    srcs, dsts, bufs, sem_in, sem_out = refs[:4], refs[4:8], refs[8:12], refs[12], refs[13]
    pieces = []
    for j in range(4):
        if j < 3:
            pieces += [(j, layer) for layer in range(LAYERS)]
        else:
            pieces += [(j, pl.ds(q * (ROWS // 4), ROWS // 4)) for q in range(4)]
    ins = [pltpu.make_async_copy(srcs[j].at[w], bufs[j].at[w], sem_in.at[n]) for n, (j, w) in enumerate(pieces)]
    outs = [pltpu.make_async_copy(bufs[j].at[w], dsts[j].at[w], sem_out.at[n]) for n, (j, w) in enumerate(pieces)]
    for copy in ins:
        copy.start()
    for copy, out in zip(ins, outs):
        copy.wait()
        out.start()
    for out in outs:
        out.wait()


def fused(h, g, w1, w3, w2):
    any_spec = pl.BlockSpec(memory_space=pl.ANY)
    V = pltpu.VMEM
    wide, low = (DS, CH), (CPD, D)
    three = lambda *lead: [V(lead + wide, F32), V(lead + wide, F32), V(lead + low, F32)]
    scratch = [
        V((ROWS, D), BF), V((D, ROWS), BF), V((ROWS, D), BF), V((D, ROWS), BF),
        V((ROWS, D), F32), V((ROWS, D), BF), V((ROWS, CH), BF), V((ROWS, 2 * CH), BF),
        V((2, DS, FF), BF), V((2, DS, FF), BF), V((2, DS, LANES), F32), V((2, DS, LANES), F32),
        V((2, DS, LANES), F32), V((2, DS, LANES), F32), V((DS, FF), F32), V((DS, FF), F32),
        V((WS, 2, 2, 2, 2, 2 * DS, HALF), BF), V((WS, 2, 2, 2, 2, 2 * DS, HALF), BF), V((WS, 2, 2, 2, 2, CPD, D), BF),
        *three(2, 2, 2, 2, 2),
        *three(2, 2, 2, 2), *three(2, 2, 2), *three(2, 2), *three(3),
        *three(2, 2, 2), *three(2, 2), *three(),
        pltpu.SemaphoreType.DMA((3, 4, 2)), pltpu.SemaphoreType.DMA((3, 4, 2)),
        pltpu.SemaphoreType.DMA((3, 4, 3)), pltpu.SemaphoreType.DMA((3, 4, 3)),
        pltpu.SemaphoreType.DMA((2, 2)), pltpu.SemaphoreType.DMA((2, 2)),
        pltpu.SemaphoreType.DMA(()), pltpu.SemaphoreType.DMA((3,)), pltpu.SemaphoreType.DMA((2, 2)),
        pltpu.SemaphoreType.DMA((NB,)), pltpu.SemaphoreType.DMA(()),
    ]
    results = (
        jax.ShapeDtypeStruct((LAYERS, DS, FF), F32),
        jax.ShapeDtypeStruct((LAYERS, DS, FF), F32),
        jax.ShapeDtypeStruct((LAYERS, FS, D), F32),
        jax.ShapeDtypeStruct((ROWS, D), BF),
    )
    parts = pl.pallas_call(
        kernel,
        name='mlp_backward',
        out_shape=results,
        in_specs=[any_spec] * 5,
        out_specs=(any_spec,) * 4,
        scratch_shapes=scratch,
        compiler_params=pltpu.CompilerParams(collective_id=0, has_side_effects=True, vmem_limit_bytes=67_043_328),
    )(h, g, w1, w3, w2)
    return pl.pallas_call(
        hand_out,
        name='hand_out',
        out_shape=results,
        in_specs=[any_spec] * 4,
        out_specs=(any_spec,) * 4,
        scratch_shapes=[V(r.shape, r.dtype) for r in results] + [pltpu.SemaphoreType.DMA((13,)), pltpu.SemaphoreType.DMA((13,))],
        compiler_params=pltpu.CompilerParams(vmem_limit_bytes=67_043_328),
        cost_estimate=pl.CostEstimate(flops=0, bytes_accessed=27_000_000, transcendentals=0),
    )(*parts)


def solution(mesh):
    weight_spec = P(None, 'fsdp', None)
    row_spec = P('fsdp', None)

    return jax.shard_map(fused, mesh=mesh, in_specs=(weight_spec, row_spec, weight_spec, weight_spec, weight_spec), out_specs=(weight_spec, weight_spec, weight_spec, row_spec), check_vma=False)
```

```python
import jax
import jax.numpy as jnp
from jax import lax
from jax.experimental import pallas as pl
from jax.experimental.pallas import tpu as pltpu
from jax.sharding import PartitionSpec as P

EPS = 1e-6
LAYERS = 3
D = 896
FF = 4864
ROWS = 2048
DEV = 16
DS = D // DEV
FS = FF // DEV
CPD = 16
CH = CPD * DEV
NC = FF // CH
NK = NC * LAYERS
LEAD = 5
TAIL = 4
WS = 6
RB = 1024
BB = 256
HALF = CH // 2
LANES = 128
NB = ROWS // BB
MESH = pl.DeviceIdType.MESH
BF = jnp.bfloat16
F32 = jnp.float32


def dot(a, b, ca, cb):
    return lax.dot_general(a, b, (((ca,), (cb,)), ((), ())), preferred_element_type=F32)


def kernel(h_hbm, g_hbm, w1_hbm, w3_hbm, w2_hbm,
           o1_v, o3_v, o2_v, g_v,
           n_v, nt_v, gt_v, dn_v, h_v, a_v, d_v,
           c1_v, c3_v, e1_v, e3_v, f1_v, f3_v,
           w1_v, w3_v, w2_v,
           g1_v, g3_v, g2_v,
           rd1, rd3, rd2, ra1, ra3, ra2, rb1, rb3, rb2, rc1, rc3, rc2,
           pa1, pa3, pa2, pb1, pb3, pb2, s1, s3,
           ag_send, ag_recv, rs_send, rs_recv, ex_send, ex_recv, own_sem, cols_sem, h_sem, g_sem):
    me = lax.axis_index('fsdp')
    c = me % 2
    x = (me // 2) % 2
    y = (me // 4) % 2
    z = (me // 8) % 2
    core = me + 1 - 2 * c
    nx = me + 2 - 4 * x
    ny = me + 4 - 8 * y
    nz = me + 8 - 16 * z

    barrier = pltpu.get_barrier_semaphore()
    for peer in (core, nx, ny, nz):
        pl.semaphore_signal(barrier, inc=1, device_id=(peer,), device_id_type=MESH)
    weights = (w1_v, w3_v, w2_v)
    grads = (g1_v, g3_v, g2_v)
    rds, ras, rbs, rcs = (rd1, rd3, rd2), (ra1, ra3, ra2), (rb1, rb3, rb2), (rc1, rc3, rc2)
    pas, pbs, outs, dones = (pa1, pa3, pa2), (pb1, pb3, pb2), (o1_v, o3_v), (s1, s3)
    cols, halves, theirs = (c1_v, c3_v), (e1_v, e3_v), (f1_v, f3_v)
    order = ((nx, ny, nz), (ny, nz, nx), (nz, nx, ny))

    def gather_slice(m, stage, k):
        s = lax.rem(k, WS)
        w = weights[m]
        if m == 0:
            return (w.at[s, c, z, y, x], w.at[s, c, z, y], w.at[s, c, z], w.at[s, c])[stage]
        if m == 1:
            return (w.at[s, c, z, y, x], w.at[s, c, z, :, x], w.at[s, c, :, :, x], w.at[s, c])[stage]
        return (w.at[s, z, y, x, c], w.at[s, :, y, x, c], w.at[s, :, y, :, c], w.at[s, :, :, :, c])[stage]

    def own_rows(k):
        return w2_hbm.at[LAYERS - 1 - k // NC, pl.ds(pl.multiple_of(lax.rem(k, NC) * CPD, CPD), CPD)]

    def gather_copy(m, stage, k):
        par = lax.rem(k, 2)
        dst = gather_slice(m, stage, k)
        src = own_rows(k) if (stage == 0 and m == 2) else dst
        peer = core if stage == 3 else order[m][stage]
        return pltpu.make_async_remote_copy(
            src_ref=src, dst_ref=dst, send_sem=ag_send.at[m, stage, par], recv_sem=ag_recv.at[m, stage, par],
            device_id=(peer,), device_id_type=MESH)

    def own_copy(k):
        return pltpu.make_async_copy(own_rows(k), gather_slice(2, 0, k), own_sem)

    def cols_copy(m, li):
        return pltpu.make_async_copy((w1_hbm, w3_hbm)[m].at[LAYERS - 1 - li], cols[m], cols_sem.at[m])

    def half_copy(m, k):
        par = lax.rem(k, 2)
        return pltpu.make_async_remote_copy(
            src_ref=halves[m].at[1 - c], dst_ref=theirs[m].at[par], send_sem=ex_send.at[m, par], recv_sem=ex_recv.at[m, par],
            device_id=(core,), device_id_type=MESH)

    lane = lax.broadcasted_iota(jnp.int32, (DS, LANES), 1)

    def place(p, i):
        col = FS * p + CPD * i
        tile = col // LANES
        return pl.ds(pl.multiple_of(tile * LANES, LANES), LANES), col - tile * LANES

    def pick_columns(k):
        i = lax.rem(k, NC)
        for m in range(2):
            for half in range(2):
                acc = jnp.zeros((DS, LANES), F32)
                for q in range(DEV // 2):
                    tile, off = place(half * (DEV // 2) + q, i)
                    part = pltpu.roll(cols[m][:, tile].astype(F32), lax.rem(CPD * q + LANES - off, LANES), 1)
                    acc = jnp.where((lane >= CPD * q) & (lane < CPD * (q + 1)), part, acc)
                halves[m][half] = acc

    def merge_rows(k):
        par = lax.rem(k, 2)
        for m in range(2):
            mine, other = halves[m][c], theirs[m][par]
            low = jnp.where(c == 0, mine, other)
            high = jnp.where(c == 0, other, mine)
            weights[m][lax.rem(k, WS), c, z, y, x] = jnp.concatenate([low, high], axis=0).astype(BF)

    def put_columns(k):
        layer = lax.rem(LAYERS - (k + NC) // NC, LAYERS)
        i = lax.rem(k + NC, NC)
        for m in range(2):
            for half in range(2):
                src = dones[m][:, half * LANES:(half + 1) * LANES]
                for q in range(DEV // 2):
                    tile, off = place(half * (DEV // 2) + q, i)
                    part = pltpu.roll(src, lax.rem(off + LANES - CPD * q, LANES), 1)
                    outs[m][layer, :, tile] = jnp.where((lane >= off) & (lane < off + CPD), part, outs[m][layer, :, tile])

    def reduce_copy(m, stage, k):
        par = lax.rem(k, 2)
        slot = lax.rem(k, 3) if stage == 3 else par
        g, pa, pb = grads[m], pas[m].at[par], pbs[m].at[par]
        if stage == 0:
            src, dst, peer = g.at[par, :, :, :, 1 - c], rds[m].at[par], core
        elif stage == 1:
            src = (g.at[par, :, :, 1 - x, c], g.at[par, :, 1 - y, :, c], g.at[par, 1 - z, :, :, c])[m]
            dst, peer = ras[m].at[par], order[m][0]
        elif stage == 2:
            src = (pa.at[:, 1 - y], pa.at[1 - z], pa.at[:, 1 - x])[m]
            dst, peer = rbs[m].at[par], order[m][1]
        else:
            src = (pb.at[1 - z], pb.at[1 - x], pb.at[1 - y])[m]
            dst, peer = rcs[m].at[lax.rem(k, 3)], order[m][2]
        return pltpu.make_async_remote_copy(
            src_ref=src, dst_ref=dst, send_sem=rs_send.at[m, stage, slot], recv_sem=rs_recv.at[m, stage, slot],
            device_id=(peer,), device_id_type=MESH)

    def h_copy(li, b):
        rows = pl.ds(pl.multiple_of(b * BB, BB), BB)
        return pltpu.make_async_copy(h_hbm.at[LAYERS - 1 - li, rows], h_v.at[rows], h_sem.at[b])

    def g_copy():
        return pltpu.make_async_copy(g_hbm, g_v, g_sem)

    def finalize_rows(r0):
        rows = pl.ds(r0, BB)
        hf = h_v[rows, :].astype(F32)
        r = lax.rsqrt(jnp.mean(hf * hf, axis=-1, keepdims=True) + EPS)
        m = hf * r
        dn = dn_v[rows, :]
        dr = r * (dn - m * jnp.mean(dn * m, axis=-1, keepdims=True))
        g_v[rows, :] = (g_v[rows, :].astype(F32) + dr).astype(BF)

    def prepare_rows(r0):
        rows = pl.ds(r0, BB)
        hf = h_v[rows, :].astype(F32)
        r = lax.rsqrt(jnp.mean(hf * hf, axis=-1, keepdims=True) + EPS)
        nb = (hf * r).astype(BF)
        n_v[rows, :] = nb
        nt_v[:, rows] = nb.T
        gt_v[:, rows] = g_v[rows, :].T
        dn_v[rows, :] = jnp.zeros((BB, D), F32)

    def gather_first(k):
        @pl.when((k >= 1) & (k <= NK))
        def _():
            for m in range(3):
                reduce_copy(m, 0, k - 1).start()

        @pl.when((k >= 0) & (k < NK))
        def _():
            for m in range(3):
                gather_copy(m, 3, k).wait()

    def gather_rest(k):
        for lag, stage in ((1, 2), (2, 1), (3, 0)):
            @pl.when((k + lag >= 0) & (k + lag < NK))
            def _():
                for m in range(3):
                    gather_copy(m, stage, k + lag).wait()
                if stage == 0:
                    own_copy(k + lag).wait()
                for m in range(3):
                    gather_copy(m, stage + 1, k + lag).start()

        @pl.when((k + 4 >= 0) & (k + 4 < NK))
        def _():
            for m in range(3):
                gather_copy(m, 0, k + 4).start()
            own_copy(k + 4).start()

        @pl.when((k <= 0) & (k > -LEAD))
        def _():
            pick_columns(k + 5)

        @pl.when(k + 5 < NK)
        def _():
            for m in range(2):
                half_copy(m, k + 5).start()

        @pl.when((k + 6 == NC) | (k + 6 == 2 * NC))
        def _():
            for m in range(2):
                cols_copy(m, (k + 6) // NC).start()

    def reduce_step(k):
        def live(lag):
            return (k - lag >= 0) & (k - lag < NK)

        def finish():
            kf = k - 4
            for m in range(3):
                reduce_copy(m, 3, kf).wait()
            for m in range(3):
                done = rcs[m][lax.rem(kf, 3)] + pbs[m][lax.rem(kf, 2), (z, x, y)[m]]
                if m == 2:
                    o2_v[LAYERS - 1 - kf // NC, pl.ds(pl.multiple_of(lax.rem(kf, NC) * CPD, CPD), CPD), :] = done
                else:
                    dones[m][...] = done

        def third():
            kf = k - 3
            par = lax.rem(kf, 2)
            for m in range(3):
                reduce_copy(m, 2, kf).wait()
            for m in range(3):
                for a in range(2):
                    kept = (lambda: pa1[par, a, y], lambda: pa3[par, z, a], lambda: pa2[par, a, x])[m]()
                    pbs[m][par, a] = rbs[m][par, a] + kept
            for m in range(3):
                reduce_copy(m, 3, kf).start()

        def second():
            kf = k - 2
            par = lax.rem(kf, 2)
            for m in range(3):
                reduce_copy(m, 1, kf).wait()
            for m in range(3):
                for a in range(2):
                    for b in range(2):
                        kept = (lambda: g1_v[par, a, b, x, c], lambda: g3_v[par, a, y, b, c], lambda: g2_v[par, z, a, b, c])[m]()
                        pas[m][par, a, b] = ras[m][par, a, b] + kept
            for m in range(3):
                reduce_copy(m, 2, kf).start()

        def first():
            kf = k - 1
            par = lax.rem(kf, 2)
            for m in range(3):
                reduce_copy(m, 0, kf).wait()
            for m in range(3):
                for a in range(2):
                    for b in range(2):
                        for d in range(2):
                            grads[m][par, a, b, d, c] = grads[m][par, a, b, d, c] + rds[m][par, a, b, d]
            for m in range(3):
                reduce_copy(m, 1, kf).start()

        @pl.when(k + 5 < NK)
        def _():
            for m in range(2):
                half_copy(m, k + 5).wait()
            merge_rows(k + 5)

        @pl.when((k + 6 == NC) | (k + 6 == 2 * NC))
        def _():
            for m in range(2):
                cols_copy(m, (k + 6) // NC).wait()

        @pl.when(k <= NK)
        def _():
            pl.when(live(4))(finish)
            pl.when(live(3))(third)
            pl.when(live(2))(second)
            pl.when(live(1))(first)

        @pl.when(k > NK)
        def _():
            pl.when(live(2))(second)
            pl.when(live(3))(third)
            pl.when(live(4))(finish)

    def row_phase(k):
        s = lax.rem(k, WS)

        def body(b, carry):
            rows = pl.ds(pl.multiple_of(b * RB, RB), RB)
            w1 = jnp.concatenate([w1_v[s, 0].reshape(D, HALF), w1_v[s, 1].reshape(D, HALF)], axis=1)
            w3 = jnp.concatenate([w3_v[s, 0].reshape(D, HALF), w3_v[s, 1].reshape(D, HALF)], axis=1)
            w2 = w2_v[s].reshape(CH, D)
            nb = n_v[rows, :]
            u = dot(nb, w1, 1, 0)
            v = dot(nb, w3, 1, 0)
            da = jnp.concatenate([dot(g_v[pl.ds(pl.multiple_of(b * RB + q * (RB // 2), RB // 2), RB // 2), :], w2, 1, 1) for q in range(2)], axis=0)
            sig = 1.0 / (1.0 + jnp.exp(-u))
            act = u * sig
            a_v[rows, :] = (act * v).astype(BF)
            du = (da * v * sig * (1.0 + u * (1.0 - sig))).astype(BF)
            dv = (da * act).astype(BF)
            d_v[rows, pl.ds(0, CH)] = du
            d_v[rows, pl.ds(CH, CH)] = dv
            for q in range(2):
                rq = slice(q * (RB // 2), (q + 1) * (RB // 2))
                rr = pl.ds(pl.multiple_of(b * RB + q * (RB // 2), RB // 2), RB // 2)
                dn_v[rr, :] += dot(du[rq], w1, 1, 1) + dot(dv[rq], w3, 1, 1)
            return carry

        lax.fori_loop(0, ROWS // RB, body, 0)

    def grad_phase(k):
        par = lax.rem(k, 2)
        pick_columns(k + 6)
        put_columns(k - 4)
        nt = nt_v[...]
        g1_v[par] = dot(nt, d_v[:, pl.ds(0, CH)], 1, 0).reshape(2, 2, 2, 2, DS, CH)
        g3_v[par] = dot(nt, d_v[:, pl.ds(CH, CH)], 1, 0).reshape(2, 2, 2, 2, DS, CH)
        g2_v[par] = dot(gt_v[...], a_v[...], 1, 0).T.reshape(2, 2, 2, 2, CPD, D)

    for m in range(2):
        cols_copy(m, 0).start()
    for b in range(NB):
        h_copy(0, b).start()
    g_copy().start()
    for m in range(2):
        cols_copy(m, 0).wait()
    pick_columns(0)
    pl.semaphore_wait(barrier, 4)

    def step(t, carry):
        k = t - LEAD
        inside = (k >= 0) & (k < NK)
        last = inside & (lax.rem(k + NC, NC) == NC - 1)
        gather_first(k)

        @pl.when(k != 0)
        def _():
            gather_rest(k)

        @pl.when((t >= 1) & (t < LEAD))
        def _():
            @pl.when(t == 1)
            def _():
                for b in range(NB):
                    h_copy(0, b).wait()
                g_copy().wait()
            per = NB // (LEAD - 1)
            for j in range(per):
                prepare_rows(pl.multiple_of(((t - 1) * per + j) * BB, BB))

        @pl.when(inside)
        def _():
            row_phase(k)

        @pl.when(k == 0)
        def _():
            gather_rest(k)

        @pl.when((last & (k < NK - 1)) | (k == NK))
        def _():
            li = k // NC

            def rows(b, cc):
                finalize_rows(pl.multiple_of(b * BB, BB))

                @pl.when(k < NK)
                def _():
                    h_copy(li + 1, b).start()
                return cc
            lax.fori_loop(0, NB, rows, 0)

        reduce_step(k)

        @pl.when(inside)
        def _():
            grad_phase(k)

        @pl.when(k >= NK)
        def _():
            put_columns(k - 4)

        @pl.when(last & (k < NK - 1))
        def _():
            li = k // NC

            def rows(b, cc):
                h_copy(li + 1, b).wait()
                prepare_rows(pl.multiple_of(b * BB, BB))
                return cc
            lax.fori_loop(0, NB, rows, 0)
        return carry

    lax.fori_loop(0, LEAD + NK + TAIL, step, 0)


def hand_out(*refs):
    srcs, dsts, sem = refs[:4], refs[4:8], refs[8]
    copies = [pltpu.make_async_copy(srcs[j], dsts[j], sem.at[j]) for j in range(4)]
    for copy in copies:
        copy.start()
    for copy in copies:
        copy.wait()


def fused(h, g, w1, w3, w2):
    any_spec = pl.BlockSpec(memory_space=pl.ANY)
    V = pltpu.VMEM
    wide, low = (DS, CH), (CPD, D)
    three = lambda *lead: [V(lead + wide, F32), V(lead + wide, F32), V(lead + low, F32)]
    scratch = [
        V((ROWS, D), BF), V((D, ROWS), BF), V((D, ROWS), BF),
        V((ROWS, D), F32), V((ROWS, D), BF), V((ROWS, CH), BF), V((ROWS, 2 * CH), BF),
        V((DS, FF), BF), V((DS, FF), BF), V((2, DS, LANES), F32), V((2, DS, LANES), F32),
        V((2, DS, LANES), F32), V((2, DS, LANES), F32),
        V((WS, 2, 2, 2, 2, 2 * DS, HALF), BF), V((WS, 2, 2, 2, 2, 2 * DS, HALF), BF), V((WS, 2, 2, 2, 2, CPD, D), BF),
        *three(2, 2, 2, 2, 2),
        *three(2, 2, 2, 2), *three(2, 2, 2), *three(2, 2), *three(3),
        *three(2, 2, 2), *three(2, 2), V(wide, F32), V(wide, F32),
        pltpu.SemaphoreType.DMA((3, 4, 2)), pltpu.SemaphoreType.DMA((3, 4, 2)),
        pltpu.SemaphoreType.DMA((3, 4, 3)), pltpu.SemaphoreType.DMA((3, 4, 3)),
        pltpu.SemaphoreType.DMA((2, 2)), pltpu.SemaphoreType.DMA((2, 2)),
        pltpu.SemaphoreType.DMA(()), pltpu.SemaphoreType.DMA((2,)),
        pltpu.SemaphoreType.DMA((NB,)), pltpu.SemaphoreType.DMA(()),
    ]
    results = (
        jax.ShapeDtypeStruct((LAYERS, DS, FF), F32),
        jax.ShapeDtypeStruct((LAYERS, DS, FF), F32),
        jax.ShapeDtypeStruct((LAYERS, FS, D), F32),
        jax.ShapeDtypeStruct((ROWS, D), BF),
    )
    vmem_spec = pl.BlockSpec(memory_space=pltpu.VMEM)
    parts = pl.pallas_call(
        kernel,
        name='mlp_backward',
        out_shape=tuple(V(r.shape, r.dtype) for r in results),
        in_specs=[any_spec] * 5,
        out_specs=(vmem_spec,) * 4,
        scratch_shapes=scratch,
        compiler_params=pltpu.CompilerParams(collective_id=0, has_side_effects=True, vmem_limit_bytes=51 * 1024 * 1024),
    )(h, g, w1, w3, w2)
    return pl.pallas_call(
        hand_out,
        name='hand_out',
        out_shape=results,
        in_specs=[vmem_spec] * 4,
        out_specs=(any_spec,) * 4,
        scratch_shapes=[pltpu.SemaphoreType.DMA((4,))],
        compiler_params=pltpu.CompilerParams(vmem_limit_bytes=1024 * 1024),
    )(*[pltpu.with_memory_space_constraint(part, pltpu.VMEM) for part in parts])


def solution(mesh):
    weight_spec = P(None, 'fsdp', None)
    row_spec = P('fsdp', None)

    return jax.shard_map(fused, mesh=mesh, in_specs=(weight_spec, row_spec, weight_spec, weight_spec, weight_spec), out_specs=(weight_spec, weight_spec, weight_spec, row_spec), check_vma=False)
```

```python
import jax
import jax.numpy as jnp
from jax import lax
from jax.experimental import pallas as pl
from jax.experimental.pallas import tpu as pltpu
from jax.sharding import PartitionSpec as P

EPS = 1e-6
LAYERS = 3
D = 896
FF = 4864
ROWS = 2048
DEV = 16
DS = D // DEV
FS = FF // DEV
CPD = 16
CH = CPD * DEV
NC = FF // CH
NK = NC * LAYERS
LEAD = 5
TAIL = 4
WS = 6
RB = 1024
BB = 256
HALF = CH // 2
LANES = 128
NB = ROWS // BB
HR = 4
MESH = pl.DeviceIdType.MESH
BF = jnp.bfloat16
F32 = jnp.float32


def dot(a, b, ca, cb):
    return lax.dot_general(a, b, (((ca,), (cb,)), ((), ())), preferred_element_type=F32)


def kernel(h_hbm, g_hbm, w1_hbm, w3_hbm, w2_hbm,
           o1_v, o3_v, o2_v, g_v,
           n_v, nt_v, gt_v, dn_v, h_v, a_v, d_v,
           c1_v, c3_v, e1_v, e3_v, f1_v, f3_v,
           w1_v, w3_v, w2_v,
           g1_v, g3_v, g2_v,
           rd1, rd3, rd2, ra1, ra3, ra2, rb1, rb3, rb2, rc1, rc3, rc2,
           pa1, pa3, pa2, pb1, pb3, pb2, s1, s3,
           ag_send, ag_recv, rs_send, rs_recv, ex_send, ex_recv, own_sem, cols_sem, h_sem, g_sem):
    me = lax.axis_index('fsdp')
    c = me % 2
    x = (me // 2) % 2
    y = (me // 4) % 2
    z = (me // 8) % 2
    core = me + 1 - 2 * c
    nx = me + 2 - 4 * x
    ny = me + 4 - 8 * y
    nz = me + 8 - 16 * z

    barrier = pltpu.get_barrier_semaphore()
    for peer in (core, nx, ny, nz):
        pl.semaphore_signal(barrier, inc=1, device_id=(peer,), device_id_type=MESH)
    weights = (w1_v, w3_v, w2_v)
    grads = (g1_v, g3_v, g2_v)
    rds, ras, rbs, rcs = (rd1, rd3, rd2), (ra1, ra3, ra2), (rb1, rb3, rb2), (rc1, rc3, rc2)
    pas, pbs, outs, dones = (pa1, pa3, pa2), (pb1, pb3, pb2), (o1_v, o3_v), (s1, s3)
    cols, halves, theirs = (c1_v, c3_v), (e1_v, e3_v), (f1_v, f3_v)
    order = ((nx, ny, nz), (ny, nz, nx), (nz, nx, ny))

    def gather_slice(m, stage, k):
        s = lax.rem(k, WS)
        w = weights[m]
        if m == 0:
            return (w.at[s, c, z, y, x], w.at[s, c, z, y], w.at[s, c, z], w.at[s, c])[stage]
        if m == 1:
            return (w.at[s, c, z, y, x], w.at[s, c, z, :, x], w.at[s, c, :, :, x], w.at[s, c])[stage]
        return (w.at[s, z, y, x, c], w.at[s, :, y, x, c], w.at[s, :, y, :, c], w.at[s, :, :, :, c])[stage]

    def own_rows(k):
        return w2_hbm.at[LAYERS - 1 - k // NC, pl.ds(pl.multiple_of(lax.rem(k, NC) * CPD, CPD), CPD)]

    def gather_copy(m, stage, k):
        par = lax.rem(k, 2)
        dst = gather_slice(m, stage, k)
        src = own_rows(k) if (stage == 0 and m == 2) else dst
        peer = core if stage == 3 else order[m][stage]
        return pltpu.make_async_remote_copy(
            src_ref=src, dst_ref=dst, send_sem=ag_send.at[m, stage, par], recv_sem=ag_recv.at[m, stage, par],
            device_id=(peer,), device_id_type=MESH)

    def own_copy(k):
        return pltpu.make_async_copy(own_rows(k), gather_slice(2, 0, k), own_sem)

    def cols_copy(m, li):
        return pltpu.make_async_copy((w1_hbm, w3_hbm)[m].at[LAYERS - 1 - li], cols[m], cols_sem.at[m])

    def half_copy(m, k):
        par = lax.rem(k, 2)
        return pltpu.make_async_remote_copy(
            src_ref=halves[m].at[par, 1 - c], dst_ref=theirs[m].at[par], send_sem=ex_send.at[m, par], recv_sem=ex_recv.at[m, par],
            device_id=(core,), device_id_type=MESH)

    lane = lax.broadcasted_iota(jnp.int32, (DS, LANES), 1)

    def place(p, i):
        col = FS * p + CPD * i
        tile = col // LANES
        return pl.ds(pl.multiple_of(tile * LANES, LANES), LANES), col - tile * LANES

    def pick_columns(k):
        i = lax.rem(k, NC)
        for m in range(2):
            for half in range(2):
                acc = jnp.zeros((DS, LANES), F32)
                for q in range(DEV // 2):
                    tile, off = place(half * (DEV // 2) + q, i)
                    part = pltpu.roll(cols[m][:, tile].astype(F32), lax.rem(CPD * q + LANES - off, LANES), 1)
                    acc = jnp.where((lane >= CPD * q) & (lane < CPD * (q + 1)), part, acc)
                halves[m][lax.rem(k, 2), half] = acc

    def merge_rows(k):
        par = lax.rem(k, 2)
        for m in range(2):
            mine, other = halves[m][par, c], theirs[m][par]
            low = jnp.where(c == 0, mine, other)
            high = jnp.where(c == 0, other, mine)
            weights[m][lax.rem(k, WS), c, z, y, x] = jnp.concatenate([low, high], axis=0).astype(BF)

    def put_columns(k):
        layer = lax.rem(LAYERS - (k + NC) // NC, LAYERS)
        i = lax.rem(k + NC, NC)
        for m in range(2):
            for half in range(2):
                src = dones[m][:, half * LANES:(half + 1) * LANES]
                for q in range(DEV // 2):
                    tile, off = place(half * (DEV // 2) + q, i)
                    part = pltpu.roll(src, lax.rem(off + LANES - CPD * q, LANES), 1)
                    outs[m][layer, :, tile] = jnp.where((lane >= off) & (lane < off + CPD), part, outs[m][layer, :, tile])

    def reduce_copy(m, stage, k):
        par = lax.rem(k, 2)
        slot = par if stage == 0 else lax.rem(k, 3)
        g, pa, pb = grads[m], pas[m].at[par], pbs[m].at[par]
        if stage == 0:
            src, dst, peer = g.at[par, :, :, :, 1 - c], rds[m].at[par], core
        elif stage == 1:
            src = (g.at[par, :, :, 1 - x, c], g.at[par, :, 1 - y, :, c], g.at[par, 1 - z, :, :, c])[m]
            dst, peer = ras[m].at[slot], order[m][0]
        elif stage == 2:
            src = (pa.at[:, 1 - y], pa.at[1 - z], pa.at[:, 1 - x])[m]
            dst, peer = rbs[m].at[slot], order[m][1]
        else:
            src = (pb.at[1 - z], pb.at[1 - x], pb.at[1 - y])[m]
            dst, peer = rcs[m].at[slot], order[m][2]
        return pltpu.make_async_remote_copy(
            src_ref=src, dst_ref=dst, send_sem=rs_send.at[m, stage, slot], recv_sem=rs_recv.at[m, stage, slot],
            device_id=(peer,), device_id_type=MESH)

    def h_copy(li, b):
        rows = pl.ds(pl.multiple_of(b * BB, BB), BB)
        slot = lax.rem(b, HR)
        return pltpu.make_async_copy(h_hbm.at[LAYERS - 1 - li, rows], h_v.at[slot], h_sem.at[slot])

    def g_copy():
        return pltpu.make_async_copy(g_hbm, g_v, g_sem)

    def finalize_rows(b):
        rows = pl.ds(pl.multiple_of(b * BB, BB), BB)
        hf = h_v[lax.rem(b, HR)].astype(F32)
        r = lax.rsqrt(jnp.mean(hf * hf, axis=-1, keepdims=True) + EPS)
        m = hf * r
        dn = dn_v[rows, :]
        dr = r * (dn - m * jnp.mean(dn * m, axis=-1, keepdims=True))
        g_v[rows, :] = (g_v[rows, :].astype(F32) + dr).astype(BF)

    def prepare_rows(li, b):
        rows = pl.ds(pl.multiple_of(b * BB, BB), BB)
        h_copy(li, b).wait()
        hf = h_v[lax.rem(b, HR)].astype(F32)
        r = lax.rsqrt(jnp.mean(hf * hf, axis=-1, keepdims=True) + EPS)
        nb = (hf * r).astype(BF)
        n_v[rows, :] = nb
        nt_v[:, rows] = nb.T
        gt_v[:, rows] = g_v[rows, :].T
        dn_v[rows, :] = jnp.zeros((BB, D), F32)
        h_copy(li, lax.rem(b + HR, NB)).start()

    def gather_first(k):
        @pl.when((k >= 1) & (k <= NK))
        def _():
            for m in range(3):
                reduce_copy(m, 0, k - 1).start()

        @pl.when((k >= 0) & (k < NK))
        def _():
            for m in range(3):
                gather_copy(m, 3, k).wait()

    def gather_rest(k):
        @pl.when((k + 4 >= 0) & (k + 4 < NK))
        def _():
            for m in range(2):
                half_copy(m, k + 4).wait()
            merge_rows(k + 4)

        for lag, stage in ((1, 2), (2, 1), (3, 0)):
            @pl.when((k + lag >= 0) & (k + lag < NK))
            def _():
                for m in range(3):
                    gather_copy(m, stage, k + lag).wait()
                if stage == 0:
                    own_copy(k + lag).wait()
                for m in range(3):
                    gather_copy(m, stage + 1, k + lag).start()

        @pl.when((k + 4 >= 0) & (k + 4 < NK))
        def _():
            for m in range(3):
                gather_copy(m, 0, k + 4).start()
            own_copy(k + 4).start()

        @pl.when((k <= 0) & (k > -LEAD))
        def _():
            pick_columns(k + 5)

        @pl.when(k + 5 < NK)
        def _():
            for m in range(2):
                half_copy(m, k + 5).start()

        @pl.when((k + 6 == NC) | (k + 6 == 2 * NC))
        def _():
            for m in range(2):
                cols_copy(m, (k + 6) // NC).start()

    def reduce_step(k):
        def live(lag):
            return (k - lag >= 0) & (k - lag < NK)

        def finish():
            kf = k - 4
            for m in range(3):
                reduce_copy(m, 3, kf).wait()
            for m in range(3):
                done = rcs[m][lax.rem(kf, 3)] + pbs[m][lax.rem(kf, 2), (z, x, y)[m]]
                if m == 2:
                    o2_v[LAYERS - 1 - kf // NC, pl.ds(pl.multiple_of(lax.rem(kf, NC) * CPD, CPD), CPD), :] = done
                else:
                    dones[m][...] = done

        def third():
            kf = k - 3
            par = lax.rem(kf, 2)
            for m in range(3):
                reduce_copy(m, 2, kf).wait()
            for m in range(3):
                for a in range(2):
                    kept = (lambda: pa1[par, a, y], lambda: pa3[par, z, a], lambda: pa2[par, a, x])[m]()
                    pbs[m][par, a] = rbs[m][lax.rem(kf, 3), a] + kept
            for m in range(3):
                reduce_copy(m, 3, kf).start()

        def second():
            kf = k - 2
            par = lax.rem(kf, 2)
            for m in range(3):
                reduce_copy(m, 1, kf).wait()
            for m in range(3):
                for a in range(2):
                    for b in range(2):
                        kept = (lambda: g1_v[par, a, b, x, c], lambda: g3_v[par, a, y, b, c], lambda: g2_v[par, z, a, b, c])[m]()
                        pas[m][par, a, b] = ras[m][lax.rem(kf, 3), a, b] + kept
            for m in range(3):
                reduce_copy(m, 2, kf).start()

        def first():
            kf = k - 1
            par = lax.rem(kf, 2)
            for m in range(3):
                reduce_copy(m, 0, kf).wait()
            for m in range(3):
                for a in range(2):
                    for b in range(2):
                        for d in range(2):
                            grads[m][par, a, b, d, c] = grads[m][par, a, b, d, c] + rds[m][par, a, b, d]
            for m in range(3):
                reduce_copy(m, 1, kf).start()

        @pl.when((k + 6 == NC) | (k + 6 == 2 * NC))
        def _():
            for m in range(2):
                cols_copy(m, (k + 6) // NC).wait()

        @pl.when(k < NK)
        def _():
            pl.when(live(4))(finish)
            pl.when(live(3))(third)
            pl.when(live(2))(second)
            pl.when(live(1))(first)

        @pl.when(k >= NK)
        def _():
            pl.when(live(1))(first)
            pl.when(live(2))(second)
            pl.when(live(3))(third)
            pl.when(live(4))(finish)

    def row_phase(k):
        s = lax.rem(k, WS)

        def body(b, carry):
            @pl.when((k == 0) & (b == 1))
            def _():
                gather_rest(k)

            rows = pl.ds(pl.multiple_of(b * RB, RB), RB)
            w1 = jnp.concatenate([w1_v[s, 0].reshape(D, HALF), w1_v[s, 1].reshape(D, HALF)], axis=1)
            w3 = jnp.concatenate([w3_v[s, 0].reshape(D, HALF), w3_v[s, 1].reshape(D, HALF)], axis=1)
            w2 = w2_v[s].reshape(CH, D)
            nb = n_v[rows, :]
            u = dot(nb, w1, 1, 0)
            v = dot(nb, w3, 1, 0)
            da = jnp.concatenate([dot(g_v[pl.ds(pl.multiple_of(b * RB + q * (RB // 2), RB // 2), RB // 2), :], w2, 1, 1) for q in range(2)], axis=0)
            sig = 1.0 / (1.0 + jnp.exp(-u))
            act = u * sig
            a_v[rows, :] = (act * v).astype(BF)
            du = (da * v * sig * (1.0 + u * (1.0 - sig))).astype(BF)
            dv = (da * act).astype(BF)
            d_v[rows, pl.ds(0, CH)] = du
            d_v[rows, pl.ds(CH, CH)] = dv
            for q in range(2):
                rq = slice(q * (RB // 2), (q + 1) * (RB // 2))
                rr = pl.ds(pl.multiple_of(b * RB + q * (RB // 2), RB // 2), RB // 2)
                dn_v[rr, :] += dot(du[rq], w1, 1, 1) + dot(dv[rq], w3, 1, 1)
            return carry

        lax.fori_loop(0, ROWS // RB, body, 0)

    def grad_phase(k):
        par = lax.rem(k, 2)
        pick_columns(k + 6)
        put_columns(k - 4)
        nt = nt_v[...]
        g1_v[par] = dot(nt, d_v[:, pl.ds(0, CH)], 1, 0).reshape(2, 2, 2, 2, DS, CH)
        g3_v[par] = dot(nt, d_v[:, pl.ds(CH, CH)], 1, 0).reshape(2, 2, 2, 2, DS, CH)
        g2_v[par] = dot(gt_v[...], a_v[...], 1, 0).T.reshape(2, 2, 2, 2, CPD, D)

    for m in range(2):
        cols_copy(m, 0).start()
    for b in range(HR):
        h_copy(0, b).start()
    g_copy().start()
    for m in range(2):
        cols_copy(m, 0).wait()
    pick_columns(0)
    pl.semaphore_wait(barrier, 4)

    def step(t, carry):
        k = t - LEAD
        inside = (k >= 0) & (k < NK)
        last = inside & (lax.rem(k + NC, NC) == NC - 1)
        gather_first(k)

        @pl.when(k != 0)
        def _():
            gather_rest(k)

        @pl.when((t >= 1) & (t < LEAD))
        def _():
            @pl.when(t == 1)
            def _():
                g_copy().wait()
            per = NB // (LEAD - 1)
            for j in range(per):
                prepare_rows(0, (t - 1) * per + j)

        @pl.when(inside)
        def _():
            row_phase(k)

        @pl.when((last & (k < NK - 1)) | (k == NK))
        def _():
            li = (k - 1) // NC

            def rows(b, cc):
                h_copy(li, b).wait()
                finalize_rows(b)

                @pl.when(b < NB - HR)
                def _():
                    h_copy(li, b + HR).start()

                @pl.when((b >= NB - HR) & (k < NK))
                def _():
                    h_copy(li + 1, b + HR - NB).start()
                return cc
            lax.fori_loop(0, NB, rows, 0)

        reduce_step(k)

        @pl.when(inside)
        def _():
            grad_phase(k)

        @pl.when(k >= NK)
        def _():
            put_columns(k - 4)

        @pl.when(last & (k < NK - 1))
        def _():
            li = k // NC

            def rows(b, cc):
                prepare_rows(li + 1, b)
                return cc
            lax.fori_loop(0, NB, rows, 0)
        return carry

    lax.fori_loop(0, LEAD + NK + TAIL, step, 0)


def hand_out(*refs):
    srcs, dsts, sem = refs[:4], refs[4:8], refs[8]
    pieces = [(j, layer) for j in range(3) for layer in range(LAYERS)]
    pieces += [(3, pl.ds(q * (ROWS // 4), ROWS // 4)) for q in range(4)]
    copies = [pltpu.make_async_copy(srcs[j].at[w], dsts[j].at[w], sem.at[n]) for n, (j, w) in enumerate(pieces)]
    for copy in copies:
        copy.start()
    for copy in copies:
        copy.wait()


def fused(h, g, w1, w3, w2):
    any_spec = pl.BlockSpec(memory_space=pl.ANY)
    V = pltpu.VMEM
    wide, low = (DS, CH), (CPD, D)
    three = lambda *lead: [V(lead + wide, F32), V(lead + wide, F32), V(lead + low, F32)]
    scratch = [
        V((ROWS, D), BF), V((D, ROWS), BF), V((D, ROWS), BF),
        V((ROWS, D), F32), V((HR, BB, D), BF), V((ROWS, CH), BF), V((ROWS, 2 * CH), BF),
        V((DS, FF), BF), V((DS, FF), BF), V((2, 2, DS, LANES), F32), V((2, 2, DS, LANES), F32),
        V((2, DS, LANES), F32), V((2, DS, LANES), F32),
        V((WS, 2, 2, 2, 2, 2 * DS, HALF), BF), V((WS, 2, 2, 2, 2, 2 * DS, HALF), BF), V((WS, 2, 2, 2, 2, CPD, D), BF),
        *three(2, 2, 2, 2, 2),
        *three(2, 2, 2, 2), *three(3, 2, 2), *three(3, 2), *three(3),
        *three(2, 2, 2), *three(2, 2), V(wide, F32), V(wide, F32),
        pltpu.SemaphoreType.DMA((3, 4, 2)), pltpu.SemaphoreType.DMA((3, 4, 2)),
        pltpu.SemaphoreType.DMA((3, 4, 3)), pltpu.SemaphoreType.DMA((3, 4, 3)),
        pltpu.SemaphoreType.DMA((2, 2)), pltpu.SemaphoreType.DMA((2, 2)),
        pltpu.SemaphoreType.DMA(()), pltpu.SemaphoreType.DMA((2,)),
        pltpu.SemaphoreType.DMA((HR,)), pltpu.SemaphoreType.DMA(()),
    ]
    results = (
        jax.ShapeDtypeStruct((LAYERS, DS, FF), F32),
        jax.ShapeDtypeStruct((LAYERS, DS, FF), F32),
        jax.ShapeDtypeStruct((LAYERS, FS, D), F32),
        jax.ShapeDtypeStruct((ROWS, D), BF),
    )
    vmem_spec = pl.BlockSpec(memory_space=pltpu.VMEM)
    parts = pl.pallas_call(
        kernel,
        name='mlp_backward',
        out_shape=tuple(V(r.shape, r.dtype) for r in results),
        in_specs=[any_spec] * 5,
        out_specs=(vmem_spec,) * 4,
        scratch_shapes=scratch,
        compiler_params=pltpu.CompilerParams(collective_id=0, has_side_effects=True, vmem_limit_bytes=51 * 1024 * 1024),
    )(h, g, w1, w3, w2)
    return pl.pallas_call(
        hand_out,
        name='hand_out',
        out_shape=results,
        in_specs=[vmem_spec] * 4,
        out_specs=(any_spec,) * 4,
        scratch_shapes=[pltpu.SemaphoreType.DMA((13,))],
        compiler_params=pltpu.CompilerParams(vmem_limit_bytes=1024 * 1024),
    )(*[pltpu.with_memory_space_constraint(part, pltpu.VMEM) for part in parts])


def solution(mesh):
    weight_spec = P(None, 'fsdp', None)
    row_spec = P('fsdp', None)

    return jax.shard_map(fused, mesh=mesh, in_specs=(weight_spec, row_spec, weight_spec, weight_spec, weight_spec), out_specs=(weight_spec, weight_spec, weight_spec, row_spec), check_vma=False)
```

```python
import jax
import jax.numpy as jnp
from jax import lax
from jax.experimental import pallas as pl
from jax.experimental.pallas import tpu as pltpu
from jax.sharding import PartitionSpec as P

EPS = 1e-6
LAYERS = 3
D = 896
FF = 4864
ROWS = 2048
DEV = 16
DS = D // DEV
FS = FF // DEV
CPD = 16
CH = CPD * DEV
NC = FF // CH
NK = NC * LAYERS
LEAD = 5
TAIL = 4
WS = 6
RB = 1024
BB = 256
HALF = CH // 2
LANES = 128
NB = ROWS // BB
HR = 4
MESH = pl.DeviceIdType.MESH
BF = jnp.bfloat16
F32 = jnp.float32


def dot(a, b, ca, cb):
    return lax.dot_general(a, b, (((ca,), (cb,)), ((), ())), preferred_element_type=F32)


def kernel(h_hbm, g_hbm, w1_hbm, w3_hbm, w2_hbm,
           o1_v, o3_v, o2_v, g_v,
           n_v, nt_v, gt_v, dn_v, h_v, a_v, d_v,
           c1_v, c3_v, e1_v, e3_v, f1_v, f3_v,
           w1_v, w3_v, w2_v,
           g1_v, g3_v, g2_v,
           rd1, rd3, rd2, ra1, ra3, ra2, rb1, rb3, rb2, rc1, rc3, rc2,
           pa1, pa3, pa2, pb1, pb3, pb2, s1, s3,
           ag_send, ag_recv, rs_send, rs_recv, ex_send, ex_recv, own_sem, cols_sem, h_sem, g_sem):
    me = lax.axis_index('fsdp')
    c = me % 2
    x = (me // 2) % 2
    y = (me // 4) % 2
    z = (me // 8) % 2
    core = me + 1 - 2 * c
    nx = me + 2 - 4 * x
    ny = me + 4 - 8 * y
    nz = me + 8 - 16 * z

    barrier = pltpu.get_barrier_semaphore()
    for peer in (core, nx, ny, nz):
        pl.semaphore_signal(barrier, inc=1, device_id=(peer,), device_id_type=MESH)
    weights = (w1_v, w3_v, w2_v)
    grads = (g1_v, g3_v, g2_v)
    rds, ras, rbs, rcs = (rd1, rd3, rd2), (ra1, ra3, ra2), (rb1, rb3, rb2), (rc1, rc3, rc2)
    pas, pbs, outs, dones = (pa1, pa3, pa2), (pb1, pb3, pb2), (o1_v, o3_v), (s1, s3)
    cols, halves, theirs = (c1_v, c3_v), (e1_v, e3_v), (f1_v, f3_v)
    order = ((nx, ny, nz), (ny, nz, nx), (nz, nx, ny))

    def gather_slice(m, stage, k):
        s = lax.rem(k, WS)
        w = weights[m]
        if m == 0:
            return (w.at[s, c, z, y, x], w.at[s, c, z, y], w.at[s, c, z], w.at[s, c])[stage]
        if m == 1:
            return (w.at[s, c, z, y, x], w.at[s, c, z, :, x], w.at[s, c, :, :, x], w.at[s, c])[stage]
        return (w.at[s, z, y, x, c], w.at[s, :, y, x, c], w.at[s, :, y, :, c], w.at[s, :, :, :, c])[stage]

    def own_rows(k):
        return w2_hbm.at[LAYERS - 1 - k // NC, pl.ds(pl.multiple_of(lax.rem(k, NC) * CPD, CPD), CPD)]

    def gather_copy(m, stage, k):
        par = lax.rem(k, 2)
        dst = gather_slice(m, stage, k)
        src = own_rows(k) if (stage == 0 and m == 2) else dst
        peer = core if stage == 3 else order[m][stage]
        return pltpu.make_async_remote_copy(
            src_ref=src, dst_ref=dst, send_sem=ag_send.at[m, stage, par], recv_sem=ag_recv.at[m, stage, par],
            device_id=(peer,), device_id_type=MESH)

    def own_copy(k):
        return pltpu.make_async_copy(own_rows(k), gather_slice(2, 0, k), own_sem)

    def cols_copy(m, li):
        return pltpu.make_async_copy((w1_hbm, w3_hbm)[m].at[LAYERS - 1 - li], cols[m], cols_sem.at[m])

    def half_copy(m, k):
        par = lax.rem(k, 2)
        return pltpu.make_async_remote_copy(
            src_ref=halves[m].at[par, 1 - c], dst_ref=theirs[m].at[par], send_sem=ex_send.at[m, par], recv_sem=ex_recv.at[m, par],
            device_id=(core,), device_id_type=MESH)

    lane = lax.broadcasted_iota(jnp.int32, (DS, LANES), 1)

    def place(p, i):
        col = FS * p + CPD * i
        tile = col // LANES
        return pl.ds(pl.multiple_of(tile * LANES, LANES), LANES), col - tile * LANES

    def pick_columns(k):
        i = lax.rem(k, NC)
        for m in range(2):
            for half in range(2):
                acc = jnp.zeros((DS, LANES), F32)
                for q in range(DEV // 2):
                    tile, off = place(half * (DEV // 2) + q, i)
                    part = pltpu.roll(cols[m][:, tile].astype(F32), lax.rem(CPD * q + LANES - off, LANES), 1)
                    acc = jnp.where((lane >= CPD * q) & (lane < CPD * (q + 1)), part, acc)
                halves[m][lax.rem(k, 2), half] = acc

    def merge_rows(k):
        par = lax.rem(k, 2)
        for m in range(2):
            mine, other = halves[m][par, c], theirs[m][par]
            low = jnp.where(c == 0, mine, other)
            high = jnp.where(c == 0, other, mine)
            weights[m][lax.rem(k, WS), c, z, y, x] = jnp.concatenate([low, high], axis=0).astype(BF)

    def put_columns(k):
        layer = lax.rem(LAYERS - (k + NC) // NC, LAYERS)
        i = lax.rem(k + NC, NC)
        for m in range(2):
            for half in range(2):
                src = dones[m][:, half * LANES:(half + 1) * LANES]
                for q in range(DEV // 2):
                    tile, off = place(half * (DEV // 2) + q, i)
                    part = pltpu.roll(src, lax.rem(off + LANES - CPD * q, LANES), 1)
                    outs[m][layer, :, tile] = jnp.where((lane >= off) & (lane < off + CPD), part, outs[m][layer, :, tile])

    def reduce_copy(m, stage, k):
        par = lax.rem(k, 2)
        slot = par if stage == 0 else lax.rem(k, 3)
        g, pa, pb = grads[m], pas[m].at[par], pbs[m].at[par]
        if stage == 0:
            src, dst, peer = g.at[par, :, :, :, 1 - c], rds[m].at[par], core
        elif stage == 1:
            src = (g.at[par, :, :, 1 - x, c], g.at[par, :, 1 - y, :, c], g.at[par, 1 - z, :, :, c])[m]
            dst, peer = ras[m].at[slot], order[m][0]
        elif stage == 2:
            src = (pa.at[:, 1 - y], pa.at[1 - z], pa.at[:, 1 - x])[m]
            dst, peer = rbs[m].at[slot], order[m][1]
        else:
            src = (pb.at[1 - z], pb.at[1 - x], pb.at[1 - y])[m]
            dst, peer = rcs[m].at[slot], order[m][2]
        return pltpu.make_async_remote_copy(
            src_ref=src, dst_ref=dst, send_sem=rs_send.at[m, stage, slot], recv_sem=rs_recv.at[m, stage, slot],
            device_id=(peer,), device_id_type=MESH)

    def h_copy(li, b):
        rows = pl.ds(pl.multiple_of(b * BB, BB), BB)
        slot = lax.rem(b, HR)
        return pltpu.make_async_copy(h_hbm.at[LAYERS - 1 - li, rows], h_v.at[slot], h_sem.at[slot])

    def g_copy():
        return pltpu.make_async_copy(g_hbm, g_v, g_sem)

    def finalize_rows(b):
        rows = pl.ds(pl.multiple_of(b * BB, BB), BB)
        hf = h_v[lax.rem(b, HR)].astype(F32)
        r = lax.rsqrt(jnp.mean(hf * hf, axis=-1, keepdims=True) + EPS)
        m = hf * r
        dn = dn_v[rows, :]
        dr = r * (dn - m * jnp.mean(dn * m, axis=-1, keepdims=True))
        g_v[rows, :] = (g_v[rows, :].astype(F32) + dr).astype(BF)

    def finalize_layer(li):
        def rows(b, cc):
            h_copy(li, b).wait()
            finalize_rows(b)

            @pl.when(b < NB - HR)
            def _():
                h_copy(li, b + HR).start()

            @pl.when((b >= NB - HR) & (li < LAYERS - 1))
            def _():
                h_copy(li + 1, b + HR - NB).start()
            return cc
        with jax.named_scope('fin'):
            lax.fori_loop(0, NB, rows, 0)

    def prepare_rows(li, b):
        rows = pl.ds(pl.multiple_of(b * BB, BB), BB)
        h_copy(li, b).wait()
        hf = h_v[lax.rem(b, HR)].astype(F32)
        r = lax.rsqrt(jnp.mean(hf * hf, axis=-1, keepdims=True) + EPS)
        nb = (hf * r).astype(BF)
        n_v[rows, :] = nb
        nt_v[:, rows] = nb.T
        gt_v[:, rows] = g_v[rows, :].T
        dn_v[rows, :] = jnp.zeros((BB, D), F32)
        h_copy(li, lax.rem(b + HR, NB)).start()

    def gather_first(k):
        @pl.when((k >= 1) & (k < NK))
        def _():
            for m in range(3):
                reduce_copy(m, 0, k - 1).start()

        @pl.when((k >= 0) & (k < NK))
        def _():
            with jax.named_scope('wag3'):
                for m in range(3):
                    gather_copy(m, 3, k).wait()

    def gather_rest(k):
        @pl.when((k + 4 >= 0) & (k + 4 < NK))
        def _():
            for m in range(2):
                half_copy(m, k + 4).wait()
            merge_rows(k + 4)

        for lag, stage in ((1, 2), (2, 1), (3, 0)):
            @pl.when((k + lag >= 0) & (k + lag < NK))
            def _():
                with jax.named_scope(f'wag{stage}'):
                    for m in range(3):
                        gather_copy(m, stage, k + lag).wait()
                if stage == 0:
                    own_copy(k + lag).wait()
                for m in range(3):
                    gather_copy(m, stage + 1, k + lag).start()

        @pl.when((k + 4 >= 0) & (k + 4 < NK))
        def _():
            for m in range(3):
                gather_copy(m, 0, k + 4).start()
            own_copy(k + 4).start()

        @pl.when((k <= 0) & (k > -LEAD))
        def _():
            pick_columns(k + 5)

        @pl.when(k + 5 < NK)
        def _():
            for m in range(2):
                half_copy(m, k + 5).start()

        @pl.when((k + 6 == NC) | (k + 6 == 2 * NC))
        def _():
            for m in range(2):
                cols_copy(m, (k + 6) // NC).start()

    def reduce_step(k):
        def live(lag):
            return (k - lag >= 0) & (k - lag < NK)

        def finish():
            kf = k - 4
            with jax.named_scope('wrs3'):
                for m in range(3):
                    reduce_copy(m, 3, kf).wait()
            for m in range(3):
                done = rcs[m][lax.rem(kf, 3)] + pbs[m][lax.rem(kf, 2), (z, x, y)[m]]
                if m == 2:
                    o2_v[LAYERS - 1 - kf // NC, pl.ds(pl.multiple_of(lax.rem(kf, NC) * CPD, CPD), CPD), :] = done
                else:
                    dones[m][...] = done

        def third():
            kf = k - 3
            par = lax.rem(kf, 2)
            for m in range(3):
                with jax.named_scope('wrs2'):
                    reduce_copy(m, 2, kf).wait()
                for a in range(2):
                    kept = (lambda: pa1[par, a, y], lambda: pa3[par, z, a], lambda: pa2[par, a, x])[m]()
                    pbs[m][par, a] = rbs[m][lax.rem(kf, 3), a] + kept
                reduce_copy(m, 3, kf).start()

        def second():
            kf = k - 2
            par = lax.rem(kf, 2)
            for m in range(3):
                with jax.named_scope('wrs1'):
                    reduce_copy(m, 1, kf).wait()
                for a in range(2):
                    for b in range(2):
                        kept = (lambda: g1_v[par, a, b, x, c], lambda: g3_v[par, a, y, b, c], lambda: g2_v[par, z, a, b, c])[m]()
                        pas[m][par, a, b] = ras[m][lax.rem(kf, 3), a, b] + kept
                reduce_copy(m, 2, kf).start()

        def first():
            kf = k - 1
            par = lax.rem(kf, 2)
            for m in range(3):
                with jax.named_scope('wrs0'):
                    reduce_copy(m, 0, kf).wait()
                for a in range(2):
                    for b in range(2):
                        for d in range(2):
                            grads[m][par, a, b, d, c] = grads[m][par, a, b, d, c] + rds[m][par, a, b, d]
                reduce_copy(m, 1, kf).start()

        @pl.when((k + 6 == NC) | (k + 6 == 2 * NC))
        def _():
            for m in range(2):
                cols_copy(m, (k + 6) // NC).wait()

        @pl.when(k <= NK)
        def _():
            pl.when(live(4))(finish)

        @pl.when(k < NK)
        def _():
            pl.when(live(3))(third)
            pl.when(live(2))(second)
            pl.when(live(1))(first)

        @pl.when(k >= NK)
        def _():
            pl.when(live(1))(first)
            pl.when(k == NK)(lambda: finalize_layer(LAYERS - 1))
            pl.when(live(2))(second)
            pl.when(live(3))(third)

        @pl.when(k > NK)
        def _():
            finish()

    def row_phase(k):
        s = lax.rem(k, WS)

        def body(b, carry):
            @pl.when((k == 0) & (b == 1))
            def _():
                gather_rest(k)

            rows = pl.ds(pl.multiple_of(b * RB, RB), RB)
            w1 = jnp.concatenate([w1_v[s, 0].reshape(D, HALF), w1_v[s, 1].reshape(D, HALF)], axis=1)
            w3 = jnp.concatenate([w3_v[s, 0].reshape(D, HALF), w3_v[s, 1].reshape(D, HALF)], axis=1)
            w2 = w2_v[s].reshape(CH, D)
            nb = n_v[rows, :]
            u = dot(nb, w1, 1, 0)
            v = dot(nb, w3, 1, 0)
            da = jnp.concatenate([dot(g_v[pl.ds(pl.multiple_of(b * RB + q * (RB // 2), RB // 2), RB // 2), :], w2, 1, 1) for q in range(2)], axis=0)
            sig = 1.0 / (1.0 + jnp.exp(-u))
            act = u * sig
            a_v[rows, :] = (act * v).astype(BF)
            du = (da * v * sig * (1.0 + u * (1.0 - sig))).astype(BF)
            dv = (da * act).astype(BF)
            d_v[rows, pl.ds(0, CH)] = du
            d_v[rows, pl.ds(CH, CH)] = dv
            for q in range(2):
                rq = slice(q * (RB // 2), (q + 1) * (RB // 2))
                rr = pl.ds(pl.multiple_of(b * RB + q * (RB // 2), RB // 2), RB // 2)
                dn_v[rr, :] += dot(du[rq], w1, 1, 1) + dot(dv[rq], w3, 1, 1)
            return carry

        lax.fori_loop(0, ROWS // RB, body, 0)

    def grad_phase(k, early):
        par = lax.rem(k, 2)
        if not early:
            pick_columns(k + 6)
        put_columns(k - 4)
        nt = nt_v[...]
        g1_v[par] = dot(nt, d_v[:, pl.ds(0, CH)], 1, 0).reshape(2, 2, 2, 2, DS, CH)
        if early:
            reduce_copy(0, 0, k).start()
        g3_v[par] = dot(nt, d_v[:, pl.ds(CH, CH)], 1, 0).reshape(2, 2, 2, 2, DS, CH)
        if early:
            reduce_copy(1, 0, k).start()
        g2_v[par] = dot(gt_v[...], a_v[...], 1, 0).T.reshape(2, 2, 2, 2, CPD, D)
        if early:
            reduce_copy(2, 0, k).start()

    for m in range(2):
        cols_copy(m, 0).start()
    for b in range(HR):
        h_copy(0, b).start()
    g_copy().start()
    for m in range(2):
        cols_copy(m, 0).wait()
    pick_columns(0)
    pl.semaphore_wait(barrier, 4)

    def step(t, carry):
        k = t - LEAD
        inside = (k >= 0) & (k < NK)
        last = inside & (lax.rem(k + NC, NC) == NC - 1)
        gather_first(k)

        @pl.when(k != 0)
        def _():
            gather_rest(k)

        @pl.when((t >= 1) & (t < LEAD))
        def _():
            @pl.when(t == 1)
            def _():
                g_copy().wait()

            def rows(b, cc):
                prepare_rows(0, b)
                return cc
            lax.fori_loop(3 * (t - 1), 3 * t - t // 3 - t // 4 * 3, rows, 0)

        @pl.when(inside)
        def _():
            with jax.named_scope('row'):
                row_phase(k)

        @pl.when(last & (k < NK - 1))
        def _():
            finalize_layer(k // NC)

        reduce_step(k)

        @pl.when((k >= 0) & (k < NK - 1))
        def _():
            with jax.named_scope('grad'):
                grad_phase(k, False)

        @pl.when(k == NK - 1)
        def _():
            with jax.named_scope('grad'):
                grad_phase(k, True)

        @pl.when(k >= NK)
        def _():
            put_columns(k - 4)

        @pl.when(last & (k < NK - 1))
        def _():
            li = k // NC

            def rows(b, cc):
                prepare_rows(li + 1, b)
                return cc
            lax.fori_loop(0, NB, rows, 0)
        return carry

    lax.fori_loop(0, LEAD + NK + TAIL, step, 0)


def hand_out(*refs):
    srcs, dsts, sem = refs[:4], refs[4:8], refs[8]
    pieces = [(j, layer) for j in range(3) for layer in range(LAYERS)]
    pieces += [(3, pl.ds(q * (ROWS // 4), ROWS // 4)) for q in range(4)]
    copies = [pltpu.make_async_copy(srcs[j].at[w], dsts[j].at[w], sem.at[n]) for n, (j, w) in enumerate(pieces)]
    for copy in copies:
        copy.start()
    for copy in copies:
        copy.wait()


def fused(h, g, w1, w3, w2):
    any_spec = pl.BlockSpec(memory_space=pl.ANY)
    V = pltpu.VMEM
    wide, low = (DS, CH), (CPD, D)
    three = lambda *lead: [V(lead + wide, F32), V(lead + wide, F32), V(lead + low, F32)]
    scratch = [
        V((ROWS, D), BF), V((D, ROWS), BF), V((D, ROWS), BF),
        V((ROWS, D), F32), V((HR, BB, D), BF), V((ROWS, CH), BF), V((ROWS, 2 * CH), BF),
        V((DS, FF), BF), V((DS, FF), BF), V((2, 2, DS, LANES), F32), V((2, 2, DS, LANES), F32),
        V((2, DS, LANES), F32), V((2, DS, LANES), F32),
        V((WS, 2, 2, 2, 2, 2 * DS, HALF), BF), V((WS, 2, 2, 2, 2, 2 * DS, HALF), BF), V((WS, 2, 2, 2, 2, CPD, D), BF),
        *three(2, 2, 2, 2, 2),
        *three(2, 2, 2, 2), *three(3, 2, 2), *three(3, 2), *three(3),
        *three(2, 2, 2), *three(2, 2), V(wide, F32), V(wide, F32),
        pltpu.SemaphoreType.DMA((3, 4, 2)), pltpu.SemaphoreType.DMA((3, 4, 2)),
        pltpu.SemaphoreType.DMA((3, 4, 3)), pltpu.SemaphoreType.DMA((3, 4, 3)),
        pltpu.SemaphoreType.DMA((2, 2)), pltpu.SemaphoreType.DMA((2, 2)),
        pltpu.SemaphoreType.DMA(()), pltpu.SemaphoreType.DMA((2,)),
        pltpu.SemaphoreType.DMA((HR,)), pltpu.SemaphoreType.DMA(()),
    ]
    results = (
        jax.ShapeDtypeStruct((LAYERS, DS, FF), F32),
        jax.ShapeDtypeStruct((LAYERS, DS, FF), F32),
        jax.ShapeDtypeStruct((LAYERS, FS, D), F32),
        jax.ShapeDtypeStruct((ROWS, D), BF),
    )
    vmem_spec = pl.BlockSpec(memory_space=pltpu.VMEM)
    parts = pl.pallas_call(
        kernel,
        name='mlp_backward',
        out_shape=tuple(V(r.shape, r.dtype) for r in results),
        in_specs=[any_spec] * 5,
        out_specs=(vmem_spec,) * 4,
        scratch_shapes=scratch,
        compiler_params=pltpu.CompilerParams(collective_id=0, has_side_effects=True, vmem_limit_bytes=51 * 1024 * 1024),
    )(h, g, w1, w3, w2)
    return pl.pallas_call(
        hand_out,
        name='hand_out',
        out_shape=results,
        in_specs=[vmem_spec] * 4,
        out_specs=(any_spec,) * 4,
        scratch_shapes=[pltpu.SemaphoreType.DMA((13,))],
        compiler_params=pltpu.CompilerParams(vmem_limit_bytes=1024 * 1024),
    )(*[pltpu.with_memory_space_constraint(part, pltpu.VMEM) for part in parts])


def solution(mesh):
    weight_spec = P(None, 'fsdp', None)
    row_spec = P('fsdp', None)

    return jax.shard_map(fused, mesh=mesh, in_specs=(weight_spec, row_spec, weight_spec, weight_spec, weight_spec), out_specs=(weight_spec, weight_spec, weight_spec, row_spec), check_vma=False)
```

```python
import jax
import jax.numpy as jnp
from jax import lax
from jax.experimental import pallas as pl
from jax.experimental.pallas import tpu as pltpu
from jax.sharding import PartitionSpec as P

EPS = 1e-6
LAYERS = 3
D = 896
FF = 4864
ROWS = 2048
DEV = 16
DS = D // DEV
FS = FF // DEV
CPD = 16
CH = CPD * DEV
NC = FF // CH
NK = NC * LAYERS
LEAD = 5
TAIL = 4
WS = 6
RB = 1024
BB = 256
HALF = CH // 2
LANES = 128
NB = ROWS // BB
HR = 4
MESH = pl.DeviceIdType.MESH
BF = jnp.bfloat16
F32 = jnp.float32


def dot(a, b, ca, cb):
    return lax.dot_general(a, b, (((ca,), (cb,)), ((), ())), preferred_element_type=F32)


def kernel(h_hbm, g_hbm, w1_hbm, w3_hbm, w2_hbm,
           o1_v, o3_v, o2_v, g_v,
           n_v, nt_v, gt_v, dn_v, h_v, a_v, d_v,
           c1_v, c3_v, e1_v, e3_v, f1_v, f3_v,
           w1_v, w3_v, w2_v,
           g1_v, g3_v, g2_v,
           rd1, rd3, rd2, ra1, ra3, ra2, rb1, rb3, rb2, rc1, rc3, rc2,
           pa1, pa3, pa2, pb1, pb3, pb2, s1, s3,
           ag_send, ag_recv, rs_send, rs_recv, ex_send, ex_recv, own_sem, cols_sem, h_sem, g_sem):
    me = lax.axis_index('fsdp')
    c = me % 2
    x = (me // 2) % 2
    y = (me // 4) % 2
    z = (me // 8) % 2
    core = me + 1 - 2 * c
    nx = me + 2 - 4 * x
    ny = me + 4 - 8 * y
    nz = me + 8 - 16 * z

    barrier = pltpu.get_barrier_semaphore()
    for peer in (core, nx, ny, nz):
        pl.semaphore_signal(barrier, inc=1, device_id=(peer,), device_id_type=MESH)
    weights = (w1_v, w3_v, w2_v)
    grads = (g1_v, g3_v, g2_v)
    rds, ras, rbs, rcs = (rd1, rd3, rd2), (ra1, ra3, ra2), (rb1, rb3, rb2), (rc1, rc3, rc2)
    pas, pbs, outs, dones = (pa1, pa3, pa2), (pb1, pb3, pb2), (o1_v, o3_v), (s1, s3)
    cols, halves, theirs = (c1_v, c3_v), (e1_v, e3_v), (f1_v, f3_v)
    order = ((nx, ny, nz), (ny, nz, nx), (nz, nx, ny))

    def gather_slice(m, stage, k):
        s = lax.rem(k, WS)
        w = weights[m]
        if m == 0:
            return (lambda: w.at[s, c, z, y, x], lambda: w.at[s, c, z, y], lambda: w.at[s, c, z],
                    lambda: w.at[s, c, z, y], lambda: w.at[s, c, z, 1 - y], lambda: w.at[s, c, 1 - z])[stage]()
        if m == 1:
            return (lambda: w.at[s, c, z, y, x], lambda: w.at[s, c, z, :, x], lambda: w.at[s, c, :, :, x],
                    lambda: w.at[s, c, z, :, x], lambda: w.at[s, c, 1 - z, :, x], lambda: w.at[s, c, :, :, 1 - x])[stage]()
        return (lambda: w.at[s, z, y, x, c], lambda: w.at[s, :, y, x, c], lambda: w.at[s, :, y, :, c],
                lambda: w.at[s, :, y, x, c], lambda: w.at[s, :, y, 1 - x, c], lambda: w.at[s, :, 1 - y, :, c])[stage]()

    def own_rows(k):
        return w2_hbm.at[LAYERS - 1 - k // NC, pl.ds(pl.multiple_of(lax.rem(k, NC) * CPD, CPD), CPD)]

    def gather_copy(m, stage, k):
        par = lax.rem(k, 2)
        dst = gather_slice(m, stage, k)
        src = own_rows(k) if (stage == 0 and m == 2) else dst
        peer = core if stage >= 3 else order[m][stage]
        return pltpu.make_async_remote_copy(
            src_ref=src, dst_ref=dst, send_sem=ag_send.at[m, stage, par], recv_sem=ag_recv.at[m, stage, par],
            device_id=(peer,), device_id_type=MESH)

    def own_copy(k):
        return pltpu.make_async_copy(own_rows(k), gather_slice(2, 0, k), own_sem)

    def cols_copy(m, li):
        return pltpu.make_async_copy((w1_hbm, w3_hbm)[m].at[LAYERS - 1 - li], cols[m], cols_sem.at[m])

    def half_copy(m, k):
        par = lax.rem(k, 2)
        return pltpu.make_async_remote_copy(
            src_ref=halves[m].at[par, 1 - c], dst_ref=theirs[m].at[par], send_sem=ex_send.at[m, par], recv_sem=ex_recv.at[m, par],
            device_id=(core,), device_id_type=MESH)

    lane = lax.broadcasted_iota(jnp.int32, (DS, LANES), 1)

    def place(p, i):
        col = FS * p + CPD * i
        tile = col // LANES
        return pl.ds(pl.multiple_of(tile * LANES, LANES), LANES), col - tile * LANES

    def pick_columns(k):
        i = lax.rem(k, NC)
        for m in range(2):
            for half in range(2):
                acc = jnp.zeros((DS, LANES), F32)
                for q in range(DEV // 2):
                    tile, off = place(half * (DEV // 2) + q, i)
                    part = pltpu.roll(cols[m][:, tile].astype(F32), lax.rem(CPD * q + LANES - off, LANES), 1)
                    acc = jnp.where((lane >= CPD * q) & (lane < CPD * (q + 1)), part, acc)
                halves[m][lax.rem(k, 2), half] = acc

    def merge_rows(k):
        par = lax.rem(k, 2)
        for m in range(2):
            mine, other = halves[m][par, c], theirs[m][par]
            low = jnp.where(c == 0, mine, other)
            high = jnp.where(c == 0, other, mine)
            weights[m][lax.rem(k, WS), c, z, y, x] = jnp.concatenate([low, high], axis=0).astype(BF)

    def put_columns(k):
        layer = lax.rem(LAYERS - (k + NC) // NC, LAYERS)
        i = lax.rem(k + NC, NC)
        for m in range(2):
            for half in range(2):
                src = dones[m][:, half * LANES:(half + 1) * LANES]
                for q in range(DEV // 2):
                    tile, off = place(half * (DEV // 2) + q, i)
                    part = pltpu.roll(src, lax.rem(off + LANES - CPD * q, LANES), 1)
                    outs[m][layer, :, tile] = jnp.where((lane >= off) & (lane < off + CPD), part, outs[m][layer, :, tile])

    def reduce_copy(m, stage, k):
        par = lax.rem(k, 2)
        slot = par if stage == 0 else lax.rem(k, 3)
        g, pa, pb = grads[m], pas[m].at[par], pbs[m].at[par]
        if stage == 0:
            src, dst, peer = g.at[par, :, :, :, 1 - c], rds[m].at[par], core
        elif stage == 1:
            src = (g.at[par, :, :, 1 - x, c], g.at[par, :, 1 - y, :, c], g.at[par, 1 - z, :, :, c])[m]
            dst, peer = ras[m].at[slot], order[m][0]
        elif stage == 2:
            src = (pa.at[:, 1 - y], pa.at[1 - z], pa.at[:, 1 - x])[m]
            dst, peer = rbs[m].at[slot], order[m][1]
        else:
            src = (pb.at[1 - z], pb.at[1 - x], pb.at[1 - y])[m]
            dst, peer = rcs[m].at[slot], order[m][2]
        return pltpu.make_async_remote_copy(
            src_ref=src, dst_ref=dst, send_sem=rs_send.at[m, stage, slot], recv_sem=rs_recv.at[m, stage, slot],
            device_id=(peer,), device_id_type=MESH)

    def h_copy(li, b):
        rows = pl.ds(pl.multiple_of(b * BB, BB), BB)
        slot = lax.rem(b, HR)
        return pltpu.make_async_copy(h_hbm.at[LAYERS - 1 - li, rows], h_v.at[slot], h_sem.at[slot])

    def g_copy():
        return pltpu.make_async_copy(g_hbm, g_v, g_sem)

    def finalize_rows(b):
        rows = pl.ds(pl.multiple_of(b * BB, BB), BB)
        hf = h_v[lax.rem(b, HR)].astype(F32)
        r = lax.rsqrt(jnp.mean(hf * hf, axis=-1, keepdims=True) + EPS)
        m = hf * r
        dn = dn_v[rows, :]
        dr = r * (dn - m * jnp.mean(dn * m, axis=-1, keepdims=True))
        g_v[rows, :] = (g_v[rows, :].astype(F32) + dr).astype(BF)

    def finalize_layer(li):
        def rows(b, cc):
            h_copy(li, b).wait()
            finalize_rows(b)

            @pl.when(b < NB - HR)
            def _():
                h_copy(li, b + HR).start()

            @pl.when((b >= NB - HR) & (li < LAYERS - 1))
            def _():
                h_copy(li + 1, b + HR - NB).start()
            return cc
        with jax.named_scope('fin'):
            lax.fori_loop(0, NB, rows, 0)

    def prepare_rows(li, b):
        rows = pl.ds(pl.multiple_of(b * BB, BB), BB)
        h_copy(li, b).wait()
        hf = h_v[lax.rem(b, HR)].astype(F32)
        r = lax.rsqrt(jnp.mean(hf * hf, axis=-1, keepdims=True) + EPS)
        nb = (hf * r).astype(BF)
        n_v[rows, :] = nb
        nt_v[:, rows] = nb.T
        gt_v[:, rows] = g_v[rows, :].T
        dn_v[rows, :] = jnp.zeros((BB, D), F32)
        h_copy(li, lax.rem(b + HR, NB)).start()

    def gather_first(k):
        @pl.when((k >= 1) & (k < NK))
        def _():
            for m in range(3):
                reduce_copy(m, 0, k - 1).start()

        @pl.when((k >= 0) & (k < NK))
        def _():
            with jax.named_scope('wag3'):
                for m in range(3):
                    gather_copy(m, 5, k).wait()

    def gather_rest(k):
        def live(lag):
            return (k + lag >= 0) & (k + lag < NK)

        for lag, stage in ((1, 2), (2, 1), (3, 0)):
            @pl.when(live(lag))
            def _():
                with jax.named_scope(f'wag{stage}'):
                    for m in range(3):
                        gather_copy(m, stage, k + lag).wait()
                        if stage > 0:
                            gather_copy(m, stage + 2, k + lag).wait()
                if stage == 0:
                    own_copy(k + lag).wait()
                for m in range(3):
                    gather_copy(m, stage + 3, k + lag).start()
                    if stage < 2:
                        gather_copy(m, stage + 1, k + lag).start()

        @pl.when(live(4))
        def _():
            with jax.named_scope('wex'):
                for m in range(2):
                    half_copy(m, k + 4).wait()
            merge_rows(k + 4)
            for m in range(3):
                gather_copy(m, 0, k + 4).start()
            own_copy(k + 4).start()

        @pl.when((k <= 0) & (k > -LEAD))
        def _():
            pick_columns(k + 5)

        @pl.when(k + 5 < NK)
        def _():
            for m in range(2):
                half_copy(m, k + 5).start()

        @pl.when((k + 6 == NC) | (k + 6 == 2 * NC))
        def _():
            for m in range(2):
                cols_copy(m, (k + 6) // NC).start()

    def reduce_step(k):
        def live(lag):
            return (k - lag >= 0) & (k - lag < NK)

        def finish():
            kf = k - 4
            with jax.named_scope('wrs3'):
                for m in range(3):
                    reduce_copy(m, 3, kf).wait()
            for m in range(3):
                done = rcs[m][lax.rem(kf, 3)] + pbs[m][lax.rem(kf, 2), (z, x, y)[m]]
                if m == 2:
                    o2_v[LAYERS - 1 - kf // NC, pl.ds(pl.multiple_of(lax.rem(kf, NC) * CPD, CPD), CPD), :] = done
                else:
                    dones[m][...] = done

        def third():
            kf = k - 3
            par = lax.rem(kf, 2)
            for m in range(3):
                with jax.named_scope('wrs2'):
                    reduce_copy(m, 2, kf).wait()
                for a in range(2):
                    kept = (lambda: pa1[par, a, y], lambda: pa3[par, z, a], lambda: pa2[par, a, x])[m]()
                    pbs[m][par, a] = rbs[m][lax.rem(kf, 3), a] + kept
                reduce_copy(m, 3, kf).start()

        def second():
            kf = k - 2
            par = lax.rem(kf, 2)
            for m in range(3):
                with jax.named_scope('wrs1'):
                    reduce_copy(m, 1, kf).wait()
                for a in range(2):
                    for b in range(2):
                        kept = (lambda: g1_v[par, a, b, x, c], lambda: g3_v[par, a, y, b, c], lambda: g2_v[par, z, a, b, c])[m]()
                        pas[m][par, a, b] = ras[m][lax.rem(kf, 3), a, b] + kept
                reduce_copy(m, 2, kf).start()

        def first():
            kf = k - 1
            par = lax.rem(kf, 2)
            for m in range(3):
                with jax.named_scope('wrs0'):
                    reduce_copy(m, 0, kf).wait()
                for a in range(2):
                    for b in range(2):
                        for d in range(2):
                            grads[m][par, a, b, d, c] = grads[m][par, a, b, d, c] + rds[m][par, a, b, d]
                reduce_copy(m, 1, kf).start()

        @pl.when((k + 6 == NC) | (k + 6 == 2 * NC))
        def _():
            for m in range(2):
                cols_copy(m, (k + 6) // NC).wait()

        @pl.when(k <= NK)
        def _():
            pl.when(live(4))(finish)

        @pl.when(k < NK)
        def _():
            pl.when(live(3))(third)
            pl.when(live(2))(second)
            pl.when(live(1))(first)

        @pl.when(k >= NK)
        def _():
            pl.when(live(1))(first)
            pl.when(k == NK)(lambda: finalize_layer(LAYERS - 1))
            pl.when(live(2))(second)
            pl.when(live(3))(third)

        @pl.when(k > NK)
        def _():
            finish()

    def row_phase(k):
        s = lax.rem(k, WS)

        def body(b, carry):
            @pl.when((k == 0) & (b == 1))
            def _():
                gather_rest(k)

            rows = pl.ds(pl.multiple_of(b * RB, RB), RB)
            w1 = jnp.concatenate([w1_v[s, 0].reshape(D, HALF), w1_v[s, 1].reshape(D, HALF)], axis=1)
            w3 = jnp.concatenate([w3_v[s, 0].reshape(D, HALF), w3_v[s, 1].reshape(D, HALF)], axis=1)
            w2 = w2_v[s].reshape(CH, D)
            nb = n_v[rows, :]
            u = dot(nb, w1, 1, 0)
            v = dot(nb, w3, 1, 0)
            da = jnp.concatenate([dot(g_v[pl.ds(pl.multiple_of(b * RB + q * (RB // 2), RB // 2), RB // 2), :], w2, 1, 1) for q in range(2)], axis=0)
            sig = 1.0 / (1.0 + jnp.exp(-u))
            act = u * sig
            a_v[rows, :] = (act * v).astype(BF)
            du = (da * v * sig * (1.0 + u * (1.0 - sig))).astype(BF)
            dv = (da * act).astype(BF)
            d_v[rows, pl.ds(0, CH)] = du
            d_v[rows, pl.ds(CH, CH)] = dv
            for q in range(2):
                rq = slice(q * (RB // 2), (q + 1) * (RB // 2))
                rr = pl.ds(pl.multiple_of(b * RB + q * (RB // 2), RB // 2), RB // 2)
                dn_v[rr, :] += dot(du[rq], w1, 1, 1) + dot(dv[rq], w3, 1, 1)
            return carry

        lax.fori_loop(0, ROWS // RB, body, 0)

    def grad_phase(k, early):
        par = lax.rem(k, 2)
        if not early:
            pick_columns(k + 6)
        put_columns(k - 4)
        nt = nt_v[...]
        g1_v[par] = dot(nt, d_v[:, pl.ds(0, CH)], 1, 0).reshape(2, 2, 2, 2, DS, CH)
        g3_v[par] = dot(nt, d_v[:, pl.ds(CH, CH)], 1, 0).reshape(2, 2, 2, 2, DS, CH)
        if early:
            reduce_copy(0, 0, k).start()
            reduce_copy(1, 0, k).start()
        g2_v[par] = dot(gt_v[...], a_v[...], 1, 0).T.reshape(2, 2, 2, 2, CPD, D)
        if early:
            reduce_copy(2, 0, k).start()

    for m in range(2):
        cols_copy(m, 0).start()
    for b in range(HR):
        h_copy(0, b).start()
    g_copy().start()
    for m in range(2):
        cols_copy(m, 0).wait()
    pick_columns(0)
    pl.semaphore_wait(barrier, 4)

    def step(t, carry):
        k = t - LEAD
        inside = (k >= 0) & (k < NK)
        last = inside & (lax.rem(k + NC, NC) == NC - 1)
        gather_first(k)

        @pl.when(k != 0)
        def _():
            gather_rest(k)

        @pl.when((t >= 1) & (t < LEAD))
        def _():
            @pl.when(t == 1)
            def _():
                g_copy().wait()

            def rows(b, cc):
                prepare_rows(0, b)
                return cc
            lax.fori_loop(3 * (t - 1), 3 * t - t // 3 - t // 4 * 3, rows, 0)

        @pl.when(inside)
        def _():
            with jax.named_scope('row'):
                row_phase(k)

        @pl.when(last & (k < NK - 1))
        def _():
            finalize_layer(k // NC)

        reduce_step(k)

        @pl.when((k >= 0) & (k < NK - 1))
        def _():
            with jax.named_scope('grad'):
                grad_phase(k, False)

        @pl.when(k == NK - 1)
        def _():
            with jax.named_scope('grad'):
                grad_phase(k, True)

        @pl.when(k >= NK)
        def _():
            put_columns(k - 4)

        @pl.when(last & (k < NK - 1))
        def _():
            li = k // NC

            def rows(b, cc):
                prepare_rows(li + 1, b)
                return cc
            lax.fori_loop(0, NB, rows, 0)
        return carry

    lax.fori_loop(0, LEAD + NK + TAIL, step, 0)


def hand_out(*refs):
    srcs, dsts, sem = refs[:4], refs[4:8], refs[8]
    pieces = [(j, layer) for j in range(3) for layer in range(LAYERS)]
    pieces += [(3, pl.ds(q * (ROWS // 4), ROWS // 4)) for q in range(4)]
    copies = [pltpu.make_async_copy(srcs[j].at[w], dsts[j].at[w], sem.at[n]) for n, (j, w) in enumerate(pieces)]
    for copy in copies:
        copy.start()
    for copy in copies:
        copy.wait()


def fused(h, g, w1, w3, w2):
    any_spec = pl.BlockSpec(memory_space=pl.ANY)
    V = pltpu.VMEM
    wide, low = (DS, CH), (CPD, D)
    three = lambda *lead: [V(lead + wide, F32), V(lead + wide, F32), V(lead + low, F32)]
    scratch = [
        V((ROWS, D), BF), V((D, ROWS), BF), V((D, ROWS), BF),
        V((ROWS, D), F32), V((HR, BB, D), BF), V((ROWS, CH), BF), V((ROWS, 2 * CH), BF),
        V((DS, FF), BF), V((DS, FF), BF), V((2, 2, DS, LANES), F32), V((2, 2, DS, LANES), F32),
        V((2, DS, LANES), F32), V((2, DS, LANES), F32),
        V((WS, 2, 2, 2, 2, 2 * DS, HALF), BF), V((WS, 2, 2, 2, 2, 2 * DS, HALF), BF), V((WS, 2, 2, 2, 2, CPD, D), BF),
        *three(2, 2, 2, 2, 2),
        *three(2, 2, 2, 2), *three(3, 2, 2), *three(3, 2), *three(3),
        *three(2, 2, 2), *three(2, 2), V(wide, F32), V(wide, F32),
        pltpu.SemaphoreType.DMA((3, 6, 2)), pltpu.SemaphoreType.DMA((3, 6, 2)),
        pltpu.SemaphoreType.DMA((3, 4, 3)), pltpu.SemaphoreType.DMA((3, 4, 3)),
        pltpu.SemaphoreType.DMA((2, 2)), pltpu.SemaphoreType.DMA((2, 2)),
        pltpu.SemaphoreType.DMA(()), pltpu.SemaphoreType.DMA((2,)),
        pltpu.SemaphoreType.DMA((HR,)), pltpu.SemaphoreType.DMA(()),
    ]
    results = (
        jax.ShapeDtypeStruct((LAYERS, DS, FF), F32),
        jax.ShapeDtypeStruct((LAYERS, DS, FF), F32),
        jax.ShapeDtypeStruct((LAYERS, FS, D), F32),
        jax.ShapeDtypeStruct((ROWS, D), BF),
    )
    vmem_spec = pl.BlockSpec(memory_space=pltpu.VMEM)
    parts = pl.pallas_call(
        kernel,
        name='mlp_backward',
        out_shape=tuple(V(r.shape, r.dtype) for r in results),
        in_specs=[any_spec] * 5,
        out_specs=(vmem_spec,) * 4,
        scratch_shapes=scratch,
        compiler_params=pltpu.CompilerParams(collective_id=0, has_side_effects=True, vmem_limit_bytes=51 * 1024 * 1024),
    )(h, g, w1, w3, w2)
    return pl.pallas_call(
        hand_out,
        name='hand_out',
        out_shape=results,
        in_specs=[vmem_spec] * 4,
        out_specs=(any_spec,) * 4,
        scratch_shapes=[pltpu.SemaphoreType.DMA((13,))],
        compiler_params=pltpu.CompilerParams(vmem_limit_bytes=1024 * 1024),
    )(*[pltpu.with_memory_space_constraint(part, pltpu.VMEM) for part in parts])


def solution(mesh):
    weight_spec = P(None, 'fsdp', None)
    row_spec = P('fsdp', None)

    return jax.shard_map(fused, mesh=mesh, in_specs=(weight_spec, row_spec, weight_spec, weight_spec, weight_spec), out_specs=(weight_spec, weight_spec, weight_spec, row_spec), check_vma=False)
```

```python
import jax
import jax.numpy as jnp
from jax import lax
from jax.experimental import pallas as pl
from jax.experimental.pallas import tpu as pltpu
from jax.sharding import PartitionSpec as P

EPS = 1e-6
LAYERS = 3
D = 896
FF = 4864
ROWS = 2048
DEV = 16
DS = D // DEV
FS = FF // DEV
CPD = 16
CH = CPD * DEV
NC = FF // CH
NK = NC * LAYERS
LEAD = 5
TAIL = 4
WS = 6
RB = 1024
BB = 256
HALF = CH // 2
LANES = 128
NB = ROWS // BB
HR = 4
MESH = pl.DeviceIdType.MESH
BF = jnp.bfloat16
F32 = jnp.float32


def dot(a, b, ca, cb):
    return lax.dot_general(a, b, (((ca,), (cb,)), ((), ())), preferred_element_type=F32)


def kernel(h_hbm, g_hbm, w1_hbm, w3_hbm, w2_hbm,
           o1_v, o3_v, o2_v, g_v,
           n_v, nt_v, gt_v, dn_v, h_v, a_v, d_v,
           c1_v, c3_v, e1_v, e3_v, f1_v, f3_v,
           w1_v, w3_v, w2_v,
           g1_v, g3_v, g2_v,
           rd1, rd3, rd2, ra1, ra3, ra2, rb1, rb3, rb2, rc1, rc3, rc2,
           pa1, pa3, pa2, pb1, pb3, pb2, s1, s3,
           ag_send, ag_recv, rs_send, rs_recv, ex_send, ex_recv, own_sem, cols_sem, h_sem, g_sem):
    me = lax.axis_index('fsdp')
    c = me % 2
    x = (me // 2) % 2
    y = (me // 4) % 2
    z = (me // 8) % 2
    core = me + 1 - 2 * c
    nx = me + 2 - 4 * x
    ny = me + 4 - 8 * y
    nz = me + 8 - 16 * z

    weights = (w1_v, w3_v, w2_v)
    grads = (g1_v, g3_v, g2_v)
    rds, ras, rbs, rcs = (rd1, rd3, rd2), (ra1, ra3, ra2), (rb1, rb3, rb2), (rc1, rc3, rc2)
    pas, pbs, outs, dones = (pa1, pa3, pa2), (pb1, pb3, pb2), (o1_v, o3_v), (s1, s3)
    cols, halves, theirs = (c1_v, c3_v), (e1_v, e3_v), (f1_v, f3_v)
    order = ((nx, ny, nz), (ny, nz, nx), (nz, nx, ny))

    def gather_slice(m, stage, k):
        s = lax.rem(k, WS)
        w = weights[m]
        if m == 0:
            return (lambda: w.at[s, c, z, y, x], lambda: w.at[s, c, z, y], lambda: w.at[s, c, z],
                    lambda: w.at[s, c, z, y], lambda: w.at[s, c, z, 1 - y], lambda: w.at[s, c, 1 - z])[stage]()
        if m == 1:
            return (lambda: w.at[s, c, z, y, x], lambda: w.at[s, c, z, :, x], lambda: w.at[s, c, :, :, x],
                    lambda: w.at[s, c, z, :, x], lambda: w.at[s, c, 1 - z, :, x], lambda: w.at[s, c, :, :, 1 - x])[stage]()
        return (lambda: w.at[s, z, y, x, c], lambda: w.at[s, :, y, x, c], lambda: w.at[s, :, y, :, c],
                lambda: w.at[s, :, y, x, c], lambda: w.at[s, :, y, 1 - x, c], lambda: w.at[s, :, 1 - y, :, c])[stage]()

    def own_rows(k):
        return w2_hbm.at[LAYERS - 1 - k // NC, pl.ds(pl.multiple_of(lax.rem(k, NC) * CPD, CPD), CPD)]

    def gather_copy(m, stage, k):
        par = lax.rem(k, 2)
        dst = gather_slice(m, stage, k)
        src = own_rows(k) if (stage == 0 and m == 2) else dst
        peer = core if stage >= 3 else order[m][stage]
        return pltpu.make_async_remote_copy(
            src_ref=src, dst_ref=dst, send_sem=ag_send.at[m, stage, par], recv_sem=ag_recv.at[m, stage, par],
            device_id=(peer,), device_id_type=MESH)

    def own_copy(k):
        return pltpu.make_async_copy(own_rows(k), gather_slice(2, 0, k), own_sem)

    def cols_copy(m, li):
        return pltpu.make_async_copy((w1_hbm, w3_hbm)[m].at[LAYERS - 1 - li], cols[m], cols_sem.at[m])

    def half_copy(m, k):
        par = lax.rem(k, 2)
        return pltpu.make_async_remote_copy(
            src_ref=halves[m].at[par, 1 - c], dst_ref=theirs[m].at[par], send_sem=ex_send.at[m, par], recv_sem=ex_recv.at[m, par],
            device_id=(core,), device_id_type=MESH)

    lane = lax.broadcasted_iota(jnp.int32, (DS, LANES), 1)

    def place(p, i):
        col = FS * p + CPD * i
        tile = col // LANES
        return pl.ds(pl.multiple_of(tile * LANES, LANES), LANES), col - tile * LANES

    def pick_columns(k):
        i = lax.rem(k, NC)
        for m in range(2):
            for half in range(2):
                acc = jnp.zeros((DS, LANES), F32)
                for q in range(DEV // 2):
                    tile, off = place(half * (DEV // 2) + q, i)
                    part = pltpu.roll(cols[m][:, tile].astype(F32), lax.rem(CPD * q + LANES - off, LANES), 1)
                    acc = jnp.where((lane >= CPD * q) & (lane < CPD * (q + 1)), part, acc)
                halves[m][lax.rem(k, 2), half] = acc

    def merge_rows(k):
        par = lax.rem(k, 2)
        for m in range(2):
            mine, other = halves[m][par, c], theirs[m][par]
            low = jnp.where(c == 0, mine, other)
            high = jnp.where(c == 0, other, mine)
            weights[m][lax.rem(k, WS), c, z, y, x] = jnp.concatenate([low, high], axis=0).astype(BF)

    def put_columns(k):
        layer = lax.rem(LAYERS - (k + NC) // NC, LAYERS)
        i = lax.rem(k + NC, NC)
        for m in range(2):
            for half in range(2):
                src = dones[m][:, half * LANES:(half + 1) * LANES]
                for q in range(DEV // 2):
                    tile, off = place(half * (DEV // 2) + q, i)
                    part = pltpu.roll(src, lax.rem(off + LANES - CPD * q, LANES), 1)
                    outs[m][layer, :, tile] = jnp.where((lane >= off) & (lane < off + CPD), part, outs[m][layer, :, tile])

    def reduce_copy(m, stage, k):
        par = lax.rem(k, 2)
        slot = par if stage == 0 else lax.rem(k, 3)
        g, pa, pb = grads[m], pas[m].at[par], pbs[m].at[par]
        if stage == 0:
            src, dst, peer = g.at[par, :, :, :, 1 - c], rds[m].at[par], core
        elif stage == 1:
            src = (g.at[par, :, :, 1 - x, c], g.at[par, :, 1 - y, :, c], g.at[par, 1 - z, :, :, c])[m]
            dst, peer = ras[m].at[slot], order[m][0]
        elif stage == 2:
            src = (pa.at[:, 1 - y], pa.at[1 - z], pa.at[:, 1 - x])[m]
            dst, peer = rbs[m].at[slot], order[m][1]
        else:
            src = (pb.at[1 - z], pb.at[1 - x], pb.at[1 - y])[m]
            dst, peer = rcs[m].at[slot], order[m][2]
        return pltpu.make_async_remote_copy(
            src_ref=src, dst_ref=dst, send_sem=rs_send.at[m, stage, slot], recv_sem=rs_recv.at[m, stage, slot],
            device_id=(peer,), device_id_type=MESH)

    def h_copy(li, b):
        rows = pl.ds(pl.multiple_of(b * BB, BB), BB)
        slot = lax.rem(b, HR)
        return pltpu.make_async_copy(h_hbm.at[LAYERS - 1 - li, rows], h_v.at[slot], h_sem.at[slot])

    def g_copy():
        return pltpu.make_async_copy(g_hbm, g_v, g_sem)

    def finalize_rows(b):
        rows = pl.ds(pl.multiple_of(b * BB, BB), BB)
        hf = h_v[lax.rem(b, HR)].astype(F32)
        r = lax.rsqrt(jnp.mean(hf * hf, axis=-1, keepdims=True) + EPS)
        m = hf * r
        dn = dn_v[rows, :]
        dr = r * (dn - m * jnp.mean(dn * m, axis=-1, keepdims=True))
        g_v[rows, :] = (g_v[rows, :].astype(F32) + dr).astype(BF)

    def finalize_layer(li):
        def rows(b, cc):
            h_copy(li, b).wait()
            finalize_rows(b)

            @pl.when(b < NB - HR)
            def _():
                h_copy(li, b + HR).start()

            @pl.when((b >= NB - HR) & (li < LAYERS - 1))
            def _():
                h_copy(li + 1, b + HR - NB).start()
            return cc
        lax.fori_loop(0, NB, rows, 0)

    def prepare_rows(li, b):
        rows = pl.ds(pl.multiple_of(b * BB, BB), BB)
        h_copy(li, b).wait()
        hf = h_v[lax.rem(b, HR)].astype(F32)
        r = lax.rsqrt(jnp.mean(hf * hf, axis=-1, keepdims=True) + EPS)
        nb = (hf * r).astype(BF)
        n_v[rows, :] = nb
        nt_v[:, rows] = nb.T
        gt_v[:, rows] = g_v[rows, :].T
        dn_v[rows, :] = jnp.zeros((BB, D), F32)
        h_copy(li, lax.rem(b + HR, NB)).start()

    def gather_first(k):
        @pl.when((k >= 0) & (k < NK))
        def _():
            for m in range(3):
                gather_copy(m, 5, k).wait()

    def gather_rest(k):
        def live(lag):
            return (k + lag >= 0) & (k + lag < NK)

        for lag, stage in ((1, 2), (2, 1), (3, 0)):
            @pl.when(live(lag))
            def _():
                for m in range(3):
                    gather_copy(m, stage, k + lag).wait()
                    if stage > 0:
                        gather_copy(m, stage + 2, k + lag).wait()
                if stage == 0:
                    own_copy(k + lag).wait()
                for m in range(3):
                    gather_copy(m, stage + 3, k + lag).start()
                    if stage < 2:
                        gather_copy(m, stage + 1, k + lag).start()

        @pl.when(live(4))
        def _():
            for m in range(2):
                half_copy(m, k + 4).wait()
            merge_rows(k + 4)
            for m in range(3):
                gather_copy(m, 0, k + 4).start()
            own_copy(k + 4).start()

        @pl.when((k <= 0) & (k > -LEAD))
        def _():
            pick_columns(k + 5)

        @pl.when(k + 5 < NK)
        def _():
            for m in range(2):
                half_copy(m, k + 5).start()

        @pl.when((k + 6 == NC) | (k + 6 == 2 * NC))
        def _():
            for m in range(2):
                cols_copy(m, (k + 6) // NC).start()

    def reduce_step(k):
        def live(lag):
            return (k - lag >= 0) & (k - lag < NK)

        def finish():
            kf = k - 4
            for m in range(3):
                reduce_copy(m, 3, kf).wait()
            for m in range(3):
                done = rcs[m][lax.rem(kf, 3)] + pbs[m][lax.rem(kf, 2), (z, x, y)[m]]
                if m == 2:
                    o2_v[LAYERS - 1 - kf // NC, pl.ds(pl.multiple_of(lax.rem(kf, NC) * CPD, CPD), CPD), :] = done
                else:
                    dones[m][...] = done

        def third():
            kf = k - 3
            par = lax.rem(kf, 2)
            for m in range(3):
                reduce_copy(m, 2, kf).wait()
                for a in range(2):
                    kept = (lambda: pa1[par, a, y], lambda: pa3[par, z, a], lambda: pa2[par, a, x])[m]()
                    pbs[m][par, a] = rbs[m][lax.rem(kf, 3), a] + kept
                reduce_copy(m, 3, kf).start()

        def second():
            kf = k - 2
            par = lax.rem(kf, 2)
            for m in range(3):
                reduce_copy(m, 1, kf).wait()
                for a in range(2):
                    for b in range(2):
                        kept = (lambda: g1_v[par, a, b, x, c], lambda: g3_v[par, a, y, b, c], lambda: g2_v[par, z, a, b, c])[m]()
                        pas[m][par, a, b] = ras[m][lax.rem(kf, 3), a, b] + kept
                reduce_copy(m, 2, kf).start()

        def first():
            kf = k - 1
            par = lax.rem(kf, 2)
            for m in range(3):
                reduce_copy(m, 0, kf).wait()
                for a in range(2):
                    for b in range(2):
                        for d in range(2):
                            grads[m][par, a, b, d, c] = grads[m][par, a, b, d, c] + rds[m][par, a, b, d]
                reduce_copy(m, 1, kf).start()

        @pl.when((k + 6 == NC) | (k + 6 == 2 * NC))
        def _():
            for m in range(2):
                cols_copy(m, (k + 6) // NC).wait()

        @pl.when(k <= NK)
        def _():
            pl.when(live(4))(finish)

        @pl.when(k < NK)
        def _():
            pl.when(live(3))(third)
            pl.when(live(2))(second)
            pl.when(live(1))(first)

        @pl.when(k >= NK)
        def _():
            pl.when(live(1))(first)
            pl.when(k == NK)(lambda: finalize_layer(LAYERS - 1))
            pl.when(live(2))(second)
            pl.when(live(3))(third)

        @pl.when(k > NK)
        def _():
            finish()

    def row_phase(k):
        s = lax.rem(k, WS)

        def body(b, carry):
            @pl.when((k == 0) & (b == 1))
            def _():
                gather_rest(k)

            rows = pl.ds(pl.multiple_of(b * RB, RB), RB)
            w1 = jnp.concatenate([w1_v[s, 0].reshape(D, HALF), w1_v[s, 1].reshape(D, HALF)], axis=1)
            w3 = jnp.concatenate([w3_v[s, 0].reshape(D, HALF), w3_v[s, 1].reshape(D, HALF)], axis=1)
            w2 = w2_v[s].reshape(CH, D)
            nb = n_v[rows, :]
            u = dot(nb, w1, 1, 0)
            v = dot(nb, w3, 1, 0)
            da = jnp.concatenate([dot(g_v[pl.ds(pl.multiple_of(b * RB + q * (RB // 2), RB // 2), RB // 2), :], w2, 1, 1) for q in range(2)], axis=0)
            sig = 1.0 / (1.0 + jnp.exp(-u))
            act = u * sig
            a_v[rows, :] = (act * v).astype(BF)
            du = (da * v * sig * (1.0 + u * (1.0 - sig))).astype(BF)
            dv = (da * act).astype(BF)
            d_v[rows, pl.ds(0, CH)] = du
            d_v[rows, pl.ds(CH, CH)] = dv
            for q in range(2):
                rq = slice(q * (RB // 2), (q + 1) * (RB // 2))
                rr = pl.ds(pl.multiple_of(b * RB + q * (RB // 2), RB // 2), RB // 2)
                dn_v[rr, :] += dot(du[rq], w1, 1, 1) + dot(dv[rq], w3, 1, 1)
            return carry

        lax.fori_loop(0, ROWS // RB, body, 0)

    def grad_phase(k):
        par = lax.rem(k, 2)
        pick_columns(k + 6)
        put_columns(k - 4)
        nt = nt_v[...]
        g1_v[par] = dot(nt, d_v[:, pl.ds(0, CH)], 1, 0).reshape(2, 2, 2, 2, DS, CH)
        g3_v[par] = dot(nt, d_v[:, pl.ds(CH, CH)], 1, 0).reshape(2, 2, 2, 2, DS, CH)
        g2_v[par] = dot(gt_v[...], a_v[...], 1, 0).T.reshape(2, 2, 2, 2, CPD, D)

    for m in range(2):
        cols_copy(m, 0).start()
    barrier = pltpu.get_barrier_semaphore()
    for peer in (core, nx, ny, nz):
        pl.semaphore_signal(barrier, inc=1, device_id=(peer,), device_id_type=MESH)
    for b in range(HR):
        h_copy(0, b).start()
    g_copy().start()
    for m in range(2):
        cols_copy(m, 0).wait()
    pick_columns(0)
    pl.semaphore_wait(barrier, 4)

    def step(t, carry):
        k = t - LEAD
        inside = (k >= 0) & (k < NK)
        last = inside & (lax.rem(k + NC, NC) == NC - 1)
        gather_first(k)

        @pl.when(k != 0)
        def _():
            gather_rest(k)

        @pl.when((t >= 1) & (t < LEAD))
        def _():
            @pl.when(t == 1)
            def _():
                g_copy().wait()

            def rows(b, cc):
                prepare_rows(0, b)
                return cc
            lax.fori_loop(3 * (t - 1), 3 * t - t // 3 - t // 4 * 3, rows, 0)

        @pl.when(inside)
        def _():
            row_phase(k)

        @pl.when(last & (k < NK - 1))
        def _():
            finalize_layer(k // NC)

        reduce_step(k)

        @pl.when(inside)
        def _():
            grad_phase(k)
            for m in range(3):
                reduce_copy(m, 0, k).start()

        @pl.when(k >= NK)
        def _():
            put_columns(k - 4)

        @pl.when(last & (k < NK - 1))
        def _():
            li = k // NC

            def rows(b, cc):
                prepare_rows(li + 1, b)
                return cc
            lax.fori_loop(0, NB, rows, 0)
        return carry

    lax.fori_loop(0, LEAD + NK + TAIL, step, 0)


def hand_out(*refs):
    srcs, dsts, sem = refs[:4], refs[4:8], refs[8]
    pieces = [(j, layer) for j in range(3) for layer in range(LAYERS)]
    pieces += [(3, pl.ds(q * (ROWS // 4), ROWS // 4)) for q in range(4)]
    copies = [pltpu.make_async_copy(srcs[j].at[w], dsts[j].at[w], sem.at[n]) for n, (j, w) in enumerate(pieces)]
    for copy in copies:
        copy.start()
    for copy in copies:
        copy.wait()


def fused(h, g, w1, w3, w2):
    any_spec = pl.BlockSpec(memory_space=pl.ANY)
    V = pltpu.VMEM
    wide, low = (DS, CH), (CPD, D)
    three = lambda *lead: [V(lead + wide, F32), V(lead + wide, F32), V(lead + low, F32)]
    scratch = [
        V((ROWS, D), BF), V((D, ROWS), BF), V((D, ROWS), BF),
        V((ROWS, D), F32), V((HR, BB, D), BF), V((ROWS, CH), BF), V((ROWS, 2 * CH), BF),
        V((DS, FF), BF), V((DS, FF), BF), V((2, 2, DS, LANES), F32), V((2, 2, DS, LANES), F32),
        V((2, DS, LANES), F32), V((2, DS, LANES), F32),
        V((WS, 2, 2, 2, 2, 2 * DS, HALF), BF), V((WS, 2, 2, 2, 2, 2 * DS, HALF), BF), V((WS, 2, 2, 2, 2, CPD, D), BF),
        *three(2, 2, 2, 2, 2),
        *three(2, 2, 2, 2), *three(3, 2, 2), *three(3, 2), *three(3),
        *three(2, 2, 2), *three(2, 2), V(wide, F32), V(wide, F32),
        pltpu.SemaphoreType.DMA((3, 6, 2)), pltpu.SemaphoreType.DMA((3, 6, 2)),
        pltpu.SemaphoreType.DMA((3, 4, 3)), pltpu.SemaphoreType.DMA((3, 4, 3)),
        pltpu.SemaphoreType.DMA((2, 2)), pltpu.SemaphoreType.DMA((2, 2)),
        pltpu.SemaphoreType.DMA(()), pltpu.SemaphoreType.DMA((2,)),
        pltpu.SemaphoreType.DMA((HR,)), pltpu.SemaphoreType.DMA(()),
    ]
    results = (
        jax.ShapeDtypeStruct((LAYERS, DS, FF), F32),
        jax.ShapeDtypeStruct((LAYERS, DS, FF), F32),
        jax.ShapeDtypeStruct((LAYERS, FS, D), F32),
        jax.ShapeDtypeStruct((ROWS, D), BF),
    )
    vmem_spec = pl.BlockSpec(memory_space=pltpu.VMEM)
    parts = pl.pallas_call(
        kernel,
        name='mlp_backward',
        out_shape=tuple(V(r.shape, r.dtype) for r in results),
        in_specs=[any_spec] * 5,
        out_specs=(vmem_spec,) * 4,
        scratch_shapes=scratch,
        compiler_params=pltpu.CompilerParams(collective_id=0, has_side_effects=True, vmem_limit_bytes=51 * 1024 * 1024),
    )(h, g, w1, w3, w2)
    return pl.pallas_call(
        hand_out,
        name='hand_out',
        out_shape=results,
        in_specs=[vmem_spec] * 4,
        out_specs=(any_spec,) * 4,
        scratch_shapes=[pltpu.SemaphoreType.DMA((13,))],
        compiler_params=pltpu.CompilerParams(vmem_limit_bytes=1024 * 1024),
    )(*[pltpu.with_memory_space_constraint(part, pltpu.VMEM) for part in parts])


def solution(mesh):
    weight_spec = P(None, 'fsdp', None)
    row_spec = P('fsdp', None)

    return jax.shard_map(fused, mesh=mesh, in_specs=(weight_spec, row_spec, weight_spec, weight_spec, weight_spec), out_specs=(weight_spec, weight_spec, weight_spec, row_spec), check_vma=False)
```

```python
import jax
import jax.numpy as jnp
from jax import lax
from jax.experimental import pallas as pl
from jax.experimental.pallas import tpu as pltpu
from jax.sharding import PartitionSpec as P

EPS = 1e-6
LAYERS = 3
D = 896
FF = 4864
ROWS = 2048
DEV = 16
DS = D // DEV
FS = FF // DEV
CPD = 16
CH = CPD * DEV
NC = FF // CH
NK = NC * LAYERS
LEAD = 5
TAIL = 4
WS = 6
RB = 1024
BB = 256
HALF = CH // 2
LANES = 128
NB = ROWS // BB
HR = 4
MESH = pl.DeviceIdType.MESH
BF = jnp.bfloat16
F32 = jnp.float32


def dot(a, b, ca, cb):
    return lax.dot_general(a, b, (((ca,), (cb,)), ((), ())), preferred_element_type=F32)


def kernel(h_hbm, g_hbm, w1_hbm, w3_hbm, w2_hbm,
           o1_v, o3_v, o2_v, g_v,
           n_v, nt_v, gt_v, dn_v, h_v, a_v, d_v,
           c1_v, c3_v, e1_v, e3_v, f1_v, f3_v,
           w1_v, w3_v, w2_v,
           g1_v, g3_v, g2_v,
           rd1, rd3, rd2, ra1, ra3, ra2, rb1, rb3, rb2, rc1, rc3, rc2,
           pa1, pa3, pa2, pb1, pb3, pb2, s1, s3,
           ag_send, ag_recv, rs_send, rs_recv, ex_send, ex_recv, own_sem, cols_sem, h_sem, g_sem):
    me = lax.axis_index('fsdp')
    c = me % 2
    x = (me // 2) % 2
    y = (me // 4) % 2
    z = (me // 8) % 2
    core = me + 1 - 2 * c
    nx = me + 2 - 4 * x
    ny = me + 4 - 8 * y
    nz = me + 8 - 16 * z

    weights = (w1_v, w3_v, w2_v)
    grads = (g1_v, g3_v, g2_v)
    rds, ras, rbs, rcs = (rd1, rd3, rd2), (ra1, ra3, ra2), (rb1, rb3, rb2), (rc1, rc3, rc2)
    pas, pbs, outs, dones = (pa1, pa3, pa2), (pb1, pb3, pb2), (o1_v, o3_v), (s1, s3)
    cols, halves, theirs = (c1_v, c3_v), (e1_v, e3_v), (f1_v, f3_v)
    order = ((nx, ny, nz), (ny, nz, nx), (nz, nx, ny))

    def gather_slice(m, stage, k):
        s = lax.rem(k, WS)
        w = weights[m]
        if m == 0:
            return (lambda: w.at[s, c, z, y, x], lambda: w.at[s, c, z, y], lambda: w.at[s, c, z],
                    lambda: w.at[s, c, z, y], lambda: w.at[s, c, z, 1 - y], lambda: w.at[s, c, 1 - z])[stage]()
        if m == 1:
            return (lambda: w.at[s, c, z, y, x], lambda: w.at[s, c, z, :, x], lambda: w.at[s, c, :, :, x],
                    lambda: w.at[s, c, z, :, x], lambda: w.at[s, c, 1 - z, :, x], lambda: w.at[s, c, :, :, 1 - x])[stage]()
        return (lambda: w.at[s, z, y, x, c], lambda: w.at[s, :, y, x, c], lambda: w.at[s, :, y, :, c],
                lambda: w.at[s, :, y, x, c], lambda: w.at[s, :, y, 1 - x, c], lambda: w.at[s, :, 1 - y, :, c])[stage]()

    def own_rows(k):
        return w2_hbm.at[LAYERS - 1 - k // NC, pl.ds(pl.multiple_of(lax.rem(k, NC) * CPD, CPD), CPD)]

    def gather_copy(m, stage, k):
        par = lax.rem(k, 2)
        dst = gather_slice(m, stage, k)
        peer = core if stage >= 3 else order[m][stage]
        return pltpu.make_async_remote_copy(
            src_ref=dst, dst_ref=dst, send_sem=ag_send.at[m, stage, par], recv_sem=ag_recv.at[m, stage, par],
            device_id=(peer,), device_id_type=MESH)

    def own_copy(k):
        return pltpu.make_async_copy(own_rows(k), gather_slice(2, 0, k), own_sem)

    def cols_copy(m, li):
        return pltpu.make_async_copy((w1_hbm, w3_hbm)[m].at[LAYERS - 1 - li], cols[m], cols_sem.at[m])

    def half_copy(m, k):
        par = lax.rem(k, 2)
        return pltpu.make_async_remote_copy(
            src_ref=halves[m].at[par, 1 - c], dst_ref=theirs[m].at[par], send_sem=ex_send.at[m, par], recv_sem=ex_recv.at[m, par],
            device_id=(core,), device_id_type=MESH)

    lane = lax.broadcasted_iota(jnp.int32, (DS, LANES), 1)

    def place(p, i):
        col = FS * p + CPD * i
        tile = col // LANES
        return pl.ds(pl.multiple_of(tile * LANES, LANES), LANES), col - tile * LANES

    def pick_columns(k):
        i = lax.rem(k, NC)
        for m in range(2):
            for half in range(2):
                acc = jnp.zeros((DS, LANES), F32)
                for q in range(DEV // 2):
                    tile, off = place(half * (DEV // 2) + q, i)
                    part = pltpu.roll(cols[m][:, tile].astype(F32), lax.rem(CPD * q + LANES - off, LANES), 1)
                    acc = jnp.where((lane >= CPD * q) & (lane < CPD * (q + 1)), part, acc)
                halves[m][lax.rem(k, 2), half] = acc

    def merge_rows(k):
        par = lax.rem(k, 2)
        for m in range(2):
            mine, other = halves[m][par, c], theirs[m][par]
            low = jnp.where(c == 0, mine, other)
            high = jnp.where(c == 0, other, mine)
            weights[m][lax.rem(k, WS), c, z, y, x] = jnp.concatenate([low, high], axis=0).astype(BF)

    def put_columns(k):
        layer = lax.rem(LAYERS - (k + NC) // NC, LAYERS)
        i = lax.rem(k + NC, NC)
        for m in range(2):
            for half in range(2):
                src = dones[m][:, half * LANES:(half + 1) * LANES]
                for q in range(DEV // 2):
                    tile, off = place(half * (DEV // 2) + q, i)
                    part = pltpu.roll(src, lax.rem(off + LANES - CPD * q, LANES), 1)
                    outs[m][layer, :, tile] = jnp.where((lane >= off) & (lane < off + CPD), part, outs[m][layer, :, tile])

    def reduce_copy(m, stage, k):
        par = lax.rem(k, 2)
        slot = par if stage == 0 else lax.rem(k, 3)
        g, pa, pb = grads[m], pas[m].at[par], pbs[m].at[par]
        if stage == 0:
            src, dst, peer = g.at[par, :, :, :, 1 - c], rds[m].at[par], core
        elif stage == 1:
            src = (g.at[par, :, :, 1 - x, c], g.at[par, :, 1 - y, :, c], g.at[par, 1 - z, :, :, c])[m]
            dst, peer = ras[m].at[slot], order[m][0]
        elif stage == 2:
            src = (pa.at[:, 1 - y], pa.at[1 - z], pa.at[:, 1 - x])[m]
            dst, peer = rbs[m].at[slot], order[m][1]
        else:
            src = (pb.at[1 - z], pb.at[1 - x], pb.at[1 - y])[m]
            dst, peer = rcs[m].at[slot], order[m][2]
        return pltpu.make_async_remote_copy(
            src_ref=src, dst_ref=dst, send_sem=rs_send.at[m, stage, slot], recv_sem=rs_recv.at[m, stage, slot],
            device_id=(peer,), device_id_type=MESH)

    def h_copy(li, b):
        rows = pl.ds(pl.multiple_of(b * BB, BB), BB)
        slot = lax.rem(b, HR)
        return pltpu.make_async_copy(h_hbm.at[LAYERS - 1 - li, rows], h_v.at[slot], h_sem.at[slot])

    def g_copy():
        return pltpu.make_async_copy(g_hbm, g_v, g_sem)

    def finalize_rows(b):
        rows = pl.ds(pl.multiple_of(b * BB, BB), BB)
        hf = h_v[lax.rem(b, HR)].astype(F32)
        r = lax.rsqrt(jnp.mean(hf * hf, axis=-1, keepdims=True) + EPS)
        m = hf * r
        dn = dn_v[rows, :]
        dr = r * (dn - m * jnp.mean(dn * m, axis=-1, keepdims=True))
        g_v[rows, :] = (g_v[rows, :].astype(F32) + dr).astype(BF)

    def finalize_layer(li):
        def rows(b, cc):
            h_copy(li, b).wait()
            finalize_rows(b)

            @pl.when(b < NB - HR)
            def _():
                h_copy(li, b + HR).start()

            @pl.when((b >= NB - HR) & (li < LAYERS - 1))
            def _():
                h_copy(li + 1, b + HR - NB).start()
            return cc
        lax.fori_loop(0, NB, rows, 0)

    def prepare_rows(li, b):
        rows = pl.ds(pl.multiple_of(b * BB, BB), BB)
        h_copy(li, b).wait()
        hf = h_v[lax.rem(b, HR)].astype(F32)
        r = lax.rsqrt(jnp.mean(hf * hf, axis=-1, keepdims=True) + EPS)
        nb = (hf * r).astype(BF)
        n_v[rows, :] = nb
        nt_v[:, rows] = nb.T
        gt_v[:, rows] = g_v[rows, :].T
        dn_v[rows, :] = jnp.zeros((BB, D), F32)
        h_copy(li, lax.rem(b + HR, NB)).start()

    def gather_first(k):
        @pl.when((k >= 0) & (k < NK))
        def _():
            for m in range(3):
                gather_copy(m, 5, k).wait()

    def gather_rest(k):
        def live(lag):
            return (k + lag >= 0) & (k + lag < NK)

        for lag, stage in ((1, 2), (2, 1), (3, 0)):
            @pl.when(live(lag))
            def _():
                for m in range(3):
                    gather_copy(m, stage, k + lag).wait()
                    if stage > 0:
                        gather_copy(m, stage + 2, k + lag).wait()
                for m in range(3):
                    gather_copy(m, stage + 3, k + lag).start()
                    if stage < 2:
                        gather_copy(m, stage + 1, k + lag).start()

        @pl.when(live(4))
        def _():
            for m in range(2):
                half_copy(m, k + 4).wait()
            merge_rows(k + 4)
            own_copy(k + 4).wait()
            for m in range(3):
                gather_copy(m, 0, k + 4).start()

        @pl.when((k <= 0) & (k > -LEAD))
        def _():
            pick_columns(k + 5)

        @pl.when(k + 5 < NK)
        def _():
            own_copy(k + 5).start()
            for m in range(2):
                half_copy(m, k + 5).start()

        @pl.when((k + 6 == NC) | (k + 6 == 2 * NC))
        def _():
            for m in range(2):
                cols_copy(m, (k + 6) // NC).start()

    def reduce_step(k):
        def live(lag):
            return (k - lag >= 0) & (k - lag < NK)

        def finish():
            kf = k - 4
            for m in range(3):
                reduce_copy(m, 3, kf).wait()
            for m in range(3):
                done = rcs[m][lax.rem(kf, 3)] + pbs[m][lax.rem(kf, 2), (z, x, y)[m]]
                if m == 2:
                    o2_v[LAYERS - 1 - kf // NC, pl.ds(pl.multiple_of(lax.rem(kf, NC) * CPD, CPD), CPD), :] = done
                else:
                    dones[m][...] = done

        def third():
            kf = k - 3
            par = lax.rem(kf, 2)
            for m in range(3):
                reduce_copy(m, 2, kf).wait()
                for a in range(2):
                    kept = (lambda: pa1[par, a, y], lambda: pa3[par, z, a], lambda: pa2[par, a, x])[m]()
                    pbs[m][par, a] = rbs[m][lax.rem(kf, 3), a] + kept
                reduce_copy(m, 3, kf).start()

        def second():
            kf = k - 2
            par = lax.rem(kf, 2)
            for m in range(3):
                reduce_copy(m, 1, kf).wait()
                for a in range(2):
                    for b in range(2):
                        kept = (lambda: g1_v[par, a, b, x, c], lambda: g3_v[par, a, y, b, c], lambda: g2_v[par, z, a, b, c])[m]()
                        pas[m][par, a, b] = ras[m][lax.rem(kf, 3), a, b] + kept
                reduce_copy(m, 2, kf).start()

        def first():
            kf = k - 1
            par = lax.rem(kf, 2)
            for m in range(3):
                reduce_copy(m, 0, kf).wait()
                for a in range(2):
                    for b in range(2):
                        for d in range(2):
                            grads[m][par, a, b, d, c] = grads[m][par, a, b, d, c] + rds[m][par, a, b, d]
                reduce_copy(m, 1, kf).start()

        @pl.when((k + 6 == NC) | (k + 6 == 2 * NC))
        def _():
            for m in range(2):
                cols_copy(m, (k + 6) // NC).wait()

        @pl.when(k <= NK)
        def _():
            pl.when(live(4))(finish)

        @pl.when(k < NK)
        def _():
            pl.when(live(3))(third)
            pl.when(live(2))(second)
            pl.when(live(1))(first)

        @pl.when(k >= NK)
        def _():
            pl.when(live(1))(first)
            pl.when(k == NK)(lambda: finalize_layer(LAYERS - 1))
            pl.when(live(2))(second)
            pl.when(live(3))(third)

        @pl.when(k > NK)
        def _():
            finish()

    def row_phase(k):
        s = lax.rem(k, WS)

        def body(b, carry):
            @pl.when((k == 0) & (b == 1))
            def _():
                gather_rest(k)

            rows = pl.ds(pl.multiple_of(b * RB, RB), RB)
            w1 = jnp.concatenate([w1_v[s, 0].reshape(D, HALF), w1_v[s, 1].reshape(D, HALF)], axis=1)
            w3 = jnp.concatenate([w3_v[s, 0].reshape(D, HALF), w3_v[s, 1].reshape(D, HALF)], axis=1)
            w2 = w2_v[s].reshape(CH, D)
            nb = n_v[rows, :]
            u = dot(nb, w1, 1, 0)
            v = dot(nb, w3, 1, 0)
            da = jnp.concatenate([dot(g_v[pl.ds(pl.multiple_of(b * RB + q * (RB // 2), RB // 2), RB // 2), :], w2, 1, 1) for q in range(2)], axis=0)
            sig = 1.0 / (1.0 + jnp.exp(-u))
            act = u * sig
            a_v[rows, :] = (act * v).astype(BF)
            du = (da * v * sig * (1.0 + u * (1.0 - sig))).astype(BF)
            dv = (da * act).astype(BF)
            d_v[rows, pl.ds(0, CH)] = du
            d_v[rows, pl.ds(CH, CH)] = dv
            for q in range(2):
                rq = slice(q * (RB // 2), (q + 1) * (RB // 2))
                rr = pl.ds(pl.multiple_of(b * RB + q * (RB // 2), RB // 2), RB // 2)
                dn_v[rr, :] += dot(du[rq], w1, 1, 1) + dot(dv[rq], w3, 1, 1)
            return carry

        lax.fori_loop(0, ROWS // RB, body, 0)

    def grad_phase(k):
        par = lax.rem(k, 2)
        pick_columns(k + 6)
        put_columns(k - 4)
        nt = nt_v[...]
        g1_v[par] = dot(nt, d_v[:, pl.ds(0, CH)], 1, 0).reshape(2, 2, 2, 2, DS, CH)
        g3_v[par] = dot(nt, d_v[:, pl.ds(CH, CH)], 1, 0).reshape(2, 2, 2, 2, DS, CH)
        g2_v[par] = dot(gt_v[...], a_v[...], 1, 0).T.reshape(2, 2, 2, 2, CPD, D)

    for m in range(2):
        cols_copy(m, 0).start()
    barrier = pltpu.get_barrier_semaphore()
    for peer in (core, nx, ny, nz):
        pl.semaphore_signal(barrier, inc=1, device_id=(peer,), device_id_type=MESH)
    for b in range(HR):
        h_copy(0, b).start()
    g_copy().start()
    for m in range(2):
        cols_copy(m, 0).wait()
    pick_columns(0)
    pl.semaphore_wait(barrier, 4)

    def step(t, carry):
        k = t - LEAD
        inside = (k >= 0) & (k < NK)
        last = inside & (lax.rem(k + NC, NC) == NC - 1)
        gather_first(k)

        @pl.when(k != 0)
        def _():
            gather_rest(k)

        @pl.when((t >= 1) & (t < LEAD))
        def _():
            @pl.when(t == 1)
            def _():
                g_copy().wait()

            def rows(b, cc):
                prepare_rows(0, b)
                return cc
            lax.fori_loop(3 * (t - 1), 3 * t - t // 3 - t // 4 * 3, rows, 0)

        @pl.when(inside)
        def _():
            row_phase(k)

        @pl.when(last & (k < NK - 1))
        def _():
            finalize_layer(k // NC)

        reduce_step(k)

        @pl.when(inside)
        def _():
            grad_phase(k)
            for m in range(3):
                reduce_copy(m, 0, k).start()

        @pl.when(k >= NK)
        def _():
            put_columns(k - 4)

        @pl.when(last & (k < NK - 1))
        def _():
            li = k // NC

            def rows(b, cc):
                prepare_rows(li + 1, b)
                return cc
            lax.fori_loop(0, NB, rows, 0)
        return carry

    lax.fori_loop(0, LEAD + NK + TAIL, step, 0)


def hand_out(*refs):
    srcs, dsts, sem = refs[:4], refs[4:8], refs[8]
    pieces = [(j, layer) for j in range(3) for layer in range(LAYERS)]
    pieces += [(3, pl.ds(q * (ROWS // 4), ROWS // 4)) for q in range(4)]
    copies = [pltpu.make_async_copy(srcs[j].at[w], dsts[j].at[w], sem.at[n]) for n, (j, w) in enumerate(pieces)]
    for copy in copies:
        copy.start()
    for copy in copies:
        copy.wait()


def fused(h, g, w1, w3, w2):
    any_spec = pl.BlockSpec(memory_space=pl.ANY)
    V = pltpu.VMEM
    wide, low = (DS, CH), (CPD, D)
    three = lambda *lead: [V(lead + wide, F32), V(lead + wide, F32), V(lead + low, F32)]
    scratch = [
        V((ROWS, D), BF), V((D, ROWS), BF), V((D, ROWS), BF),
        V((ROWS, D), F32), V((HR, BB, D), BF), V((ROWS, CH), BF), V((ROWS, 2 * CH), BF),
        V((DS, FF), BF), V((DS, FF), BF), V((2, 2, DS, LANES), F32), V((2, 2, DS, LANES), F32),
        V((2, DS, LANES), F32), V((2, DS, LANES), F32),
        V((WS, 2, 2, 2, 2, 2 * DS, HALF), BF), V((WS, 2, 2, 2, 2, 2 * DS, HALF), BF), V((WS, 2, 2, 2, 2, CPD, D), BF),
        *three(2, 2, 2, 2, 2),
        *three(2, 2, 2, 2), *three(3, 2, 2), *three(3, 2), *three(3),
        *three(2, 2, 2), *three(2, 2), V(wide, F32), V(wide, F32),
        pltpu.SemaphoreType.DMA((3, 6, 2)), pltpu.SemaphoreType.DMA((3, 6, 2)),
        pltpu.SemaphoreType.DMA((3, 4, 3)), pltpu.SemaphoreType.DMA((3, 4, 3)),
        pltpu.SemaphoreType.DMA((2, 2)), pltpu.SemaphoreType.DMA((2, 2)),
        pltpu.SemaphoreType.DMA(()), pltpu.SemaphoreType.DMA((2,)),
        pltpu.SemaphoreType.DMA((HR,)), pltpu.SemaphoreType.DMA(()),
    ]
    results = (
        jax.ShapeDtypeStruct((LAYERS, DS, FF), F32),
        jax.ShapeDtypeStruct((LAYERS, DS, FF), F32),
        jax.ShapeDtypeStruct((LAYERS, FS, D), F32),
        jax.ShapeDtypeStruct((ROWS, D), BF),
    )
    vmem_spec = pl.BlockSpec(memory_space=pltpu.VMEM)
    parts = pl.pallas_call(
        kernel,
        name='mlp_backward',
        out_shape=tuple(V(r.shape, r.dtype) for r in results),
        in_specs=[any_spec] * 5,
        out_specs=(vmem_spec,) * 4,
        scratch_shapes=scratch,
        compiler_params=pltpu.CompilerParams(collective_id=0, has_side_effects=True, vmem_limit_bytes=51 * 1024 * 1024),
    )(h, g, w1, w3, w2)
    return pl.pallas_call(
        hand_out,
        name='hand_out',
        out_shape=results,
        in_specs=[vmem_spec] * 4,
        out_specs=(any_spec,) * 4,
        scratch_shapes=[pltpu.SemaphoreType.DMA((13,))],
        compiler_params=pltpu.CompilerParams(vmem_limit_bytes=1024 * 1024),
    )(*[pltpu.with_memory_space_constraint(part, pltpu.VMEM) for part in parts])


def solution(mesh):
    weight_spec = P(None, 'fsdp', None)
    row_spec = P('fsdp', None)

    return jax.shard_map(fused, mesh=mesh, in_specs=(weight_spec, row_spec, weight_spec, weight_spec, weight_spec), out_specs=(weight_spec, weight_spec, weight_spec, row_spec), check_vma=False)
```

```python
import jax
import jax.numpy as jnp
from jax import lax
from jax.experimental import pallas as pl
from jax.experimental.pallas import tpu as pltpu
from jax.sharding import PartitionSpec as P

EPS = 1e-6
LAYERS = 3
D = 896
FF = 4864
ROWS = 2048
DEV = 16
DS = D // DEV
FS = FF // DEV
CPD = 16
CH = CPD * DEV
NC = FF // CH
NK = NC * LAYERS
LEAD = 5
TAIL = 4
WS = 6
RB = 1024
BB = 256
HALF = CH // 2
LANES = 128
NB = ROWS // BB
HR = 4
MESH = pl.DeviceIdType.MESH
BF = jnp.bfloat16
F32 = jnp.float32


def dot(a, b, ca, cb):
    return lax.dot_general(a, b, (((ca,), (cb,)), ((), ())), preferred_element_type=F32)


def kernel(h_hbm, g_hbm, w1_hbm, w3_hbm, w2_hbm,
           o1_v, o3_v, o2_v, g_v,
           n_v, nt_v, gt_v, dn_v, h_v, a_v, d_v,
           c1_v, c3_v, e1_v, e3_v, f1_v, f3_v,
           w1_v, w3_v, w2_v,
           g1_v, g3_v, g2_v,
           rd1, rd3, rd2, ra1, ra3, ra2, rb1, rb3, rb2, rc1, rc3, rc2,
           pa1, pa3, pa2, pb1, pb3, pb2, s1, s3,
           ag_send, ag_recv, rs_send, rs_recv, ex_send, ex_recv, own_sem, cols_sem, h_sem, g_sem):
    me = lax.axis_index('fsdp')
    c = me % 2
    x = (me // 2) % 2
    y = (me // 4) % 2
    z = (me // 8) % 2
    core = me + 1 - 2 * c
    nx = me + 2 - 4 * x
    ny = me + 4 - 8 * y
    nz = me + 8 - 16 * z

    weights = (w1_v, w3_v, w2_v)
    grads = (g1_v, g3_v, g2_v)
    rds, ras, rbs, rcs = (rd1, rd3, rd2), (ra1, ra3, ra2), (rb1, rb3, rb2), (rc1, rc3, rc2)
    pas, pbs, outs, dones = (pa1, pa3, pa2), (pb1, pb3, pb2), (o1_v, o3_v), (s1, s3)
    cols, halves, theirs = (c1_v, c3_v), (e1_v, e3_v), (f1_v, f3_v)
    order = ((nx, ny, nz), (ny, nz, nx), (nz, nx, ny))

    def gather_slice(m, stage, k):
        s = lax.rem(k, WS)
        w = weights[m]
        if m == 0:
            return (lambda: w.at[s, c, z, y, x], lambda: w.at[s, c, z, y], lambda: w.at[s, c, z],
                    lambda: w.at[s, c, z, y], lambda: w.at[s, c, z, 1 - y], lambda: w.at[s, c, 1 - z])[stage]()
        if m == 1:
            return (lambda: w.at[s, c, z, y, x], lambda: w.at[s, c, z, :, x], lambda: w.at[s, c, :, :, x],
                    lambda: w.at[s, c, z, :, x], lambda: w.at[s, c, 1 - z, :, x], lambda: w.at[s, c, :, :, 1 - x])[stage]()
        return (lambda: w.at[s, z, y, x, c], lambda: w.at[s, :, y, x, c], lambda: w.at[s, :, y, :, c],
                lambda: w.at[s, :, y, x, c], lambda: w.at[s, :, y, 1 - x, c], lambda: w.at[s, :, 1 - y, :, c])[stage]()

    def own_rows(k):
        return w2_hbm.at[LAYERS - 1 - k // NC, pl.ds(pl.multiple_of(lax.rem(k, NC) * CPD, CPD), CPD)]

    def gather_copy(m, stage, k):
        par = lax.rem(k, 2)
        dst = gather_slice(m, stage, k)
        src = own_rows(k) if (stage == 0 and m == 2) else dst
        peer = core if stage >= 3 else order[m][stage]
        return pltpu.make_async_remote_copy(
            src_ref=src, dst_ref=dst, send_sem=ag_send.at[stage, par], recv_sem=ag_recv.at[stage, par],
            device_id=(peer,), device_id_type=MESH)

    def wait_bytes(ref, *sems):
        for sem in sems:
            pltpu.make_async_copy(ref, ref, sem).wait()

    def gather_wait(stage, k):
        par = lax.rem(k, 2)
        three = w1_v.at[pl.ds(0, 3)]
        blocks = (three.at[:, 0, 0, 0, 0], three.at[:, 0, 0, 0], three.at[:, 0, 0])[(0, 1, 2, 1, 1, 2)[stage]]
        wait_bytes(blocks, ag_send.at[stage, par], ag_recv.at[stage, par])

    def reduce_wait(stage, k):
        slot = lax.rem(k, 2 if stage == 0 else 3)
        blocks = (w1_v.at[pl.ds(0, 3)], ra1, ra1.at[:, 0], ra1.at[:, 0, 0])[stage]
        wait_bytes(blocks, rs_send.at[stage, slot], rs_recv.at[stage, slot])

    def half_wait(k):
        par = lax.rem(k, 2)
        wait_bytes(f1_v, ex_send.at[par], ex_recv.at[par])

    def own_copy(k):
        return pltpu.make_async_copy(own_rows(k), gather_slice(2, 0, k), own_sem)

    def cols_copy(m, li):
        return pltpu.make_async_copy((w1_hbm, w3_hbm)[m].at[LAYERS - 1 - li], cols[m], cols_sem.at[m])

    def half_copy(m, k):
        par = lax.rem(k, 2)
        return pltpu.make_async_remote_copy(
            src_ref=halves[m].at[par, 1 - c], dst_ref=theirs[m].at[par], send_sem=ex_send.at[par], recv_sem=ex_recv.at[par],
            device_id=(core,), device_id_type=MESH)

    lane = lax.broadcasted_iota(jnp.int32, (DS, LANES), 1)

    def place(p, i):
        col = FS * p + CPD * i
        tile = col // LANES
        return pl.ds(pl.multiple_of(tile * LANES, LANES), LANES), col - tile * LANES

    def pick_columns(k):
        i = lax.rem(k, NC)
        for m in range(2):
            for half in range(2):
                acc = jnp.zeros((DS, LANES), F32)
                for q in range(DEV // 2):
                    tile, off = place(half * (DEV // 2) + q, i)
                    part = pltpu.roll(cols[m][:, tile].astype(F32), lax.rem(CPD * q + LANES - off, LANES), 1)
                    acc = jnp.where((lane >= CPD * q) & (lane < CPD * (q + 1)), part, acc)
                halves[m][lax.rem(k, 2), half] = acc

    def merge_rows(k):
        par = lax.rem(k, 2)
        for m in range(2):
            mine, other = halves[m][par, c], theirs[m][par]
            low = jnp.where(c == 0, mine, other)
            high = jnp.where(c == 0, other, mine)
            weights[m][lax.rem(k, WS), c, z, y, x] = jnp.concatenate([low, high], axis=0).astype(BF)

    def put_columns(k):
        layer = lax.rem(LAYERS - (k + NC) // NC, LAYERS)
        i = lax.rem(k + NC, NC)
        for m in range(2):
            for half in range(2):
                src = dones[m][:, half * LANES:(half + 1) * LANES]
                for q in range(DEV // 2):
                    tile, off = place(half * (DEV // 2) + q, i)
                    part = pltpu.roll(src, lax.rem(off + LANES - CPD * q, LANES), 1)
                    outs[m][layer, :, tile] = jnp.where((lane >= off) & (lane < off + CPD), part, outs[m][layer, :, tile])

    def reduce_copy(m, stage, k):
        par = lax.rem(k, 2)
        slot = par if stage == 0 else lax.rem(k, 3)
        g, pa, pb = grads[m], pas[m].at[par], pbs[m].at[par]
        if stage == 0:
            src, dst, peer = g.at[par, :, :, :, 1 - c], rds[m].at[par], core
        elif stage == 1:
            src = (g.at[par, :, :, 1 - x, c], g.at[par, :, 1 - y, :, c], g.at[par, 1 - z, :, :, c])[m]
            dst, peer = ras[m].at[slot], order[m][0]
        elif stage == 2:
            src = (pa.at[:, 1 - y], pa.at[1 - z], pa.at[:, 1 - x])[m]
            dst, peer = rbs[m].at[slot], order[m][1]
        else:
            src = (pb.at[1 - z], pb.at[1 - x], pb.at[1 - y])[m]
            dst, peer = rcs[m].at[slot], order[m][2]
        return pltpu.make_async_remote_copy(
            src_ref=src, dst_ref=dst, send_sem=rs_send.at[stage, slot], recv_sem=rs_recv.at[stage, slot],
            device_id=(peer,), device_id_type=MESH)

    def h_copy(li, b):
        rows = pl.ds(pl.multiple_of(b * BB, BB), BB)
        slot = lax.rem(b, HR)
        return pltpu.make_async_copy(h_hbm.at[LAYERS - 1 - li, rows], h_v.at[slot], h_sem.at[slot])

    def g_copy():
        return pltpu.make_async_copy(g_hbm, g_v, g_sem)

    def finalize_rows(b):
        rows = pl.ds(pl.multiple_of(b * BB, BB), BB)
        hf = h_v[lax.rem(b, HR)].astype(F32)
        r = lax.rsqrt(jnp.mean(hf * hf, axis=-1, keepdims=True) + EPS)
        m = hf * r
        dn = dn_v[rows, :]
        dr = r * (dn - m * jnp.mean(dn * m, axis=-1, keepdims=True))
        g_v[rows, :] = (g_v[rows, :].astype(F32) + dr).astype(BF)

    def finalize_layer(li):
        def rows(b, cc):
            h_copy(li, b).wait()
            finalize_rows(b)

            @pl.when(b < NB - HR)
            def _():
                h_copy(li, b + HR).start()

            @pl.when((b >= NB - HR) & (li < LAYERS - 1))
            def _():
                h_copy(li + 1, b + HR - NB).start()
            return cc
        lax.fori_loop(0, NB, rows, 0)

    def prepare_rows(li, b):
        rows = pl.ds(pl.multiple_of(b * BB, BB), BB)
        h_copy(li, b).wait()
        hf = h_v[lax.rem(b, HR)].astype(F32)
        r = lax.rsqrt(jnp.mean(hf * hf, axis=-1, keepdims=True) + EPS)
        nb = (hf * r).astype(BF)
        n_v[rows, :] = nb
        nt_v[:, rows] = nb.T
        gt_v[:, rows] = g_v[rows, :].T
        dn_v[rows, :] = jnp.zeros((BB, D), F32)
        h_copy(li, lax.rem(b + HR, NB)).start()

    def gather_first(k):
        @pl.when((k >= 0) & (k < NK))
        def _():
            gather_wait(5, k)

    def gather_rest(k):
        def live(lag):
            return (k + lag >= 0) & (k + lag < NK)

        for lag, stage in ((1, 2), (2, 1), (3, 0)):
            @pl.when(live(lag))
            def _():
                gather_wait(stage, k + lag)
                if stage > 0:
                    gather_wait(stage + 2, k + lag)
                if stage == 0:
                    own_copy(k + lag).wait()
                for m in range(3):
                    gather_copy(m, stage + 3, k + lag).start()
                    if stage < 2:
                        gather_copy(m, stage + 1, k + lag).start()

        @pl.when(live(4))
        def _():
            half_wait(k + 4)
            merge_rows(k + 4)
            for m in range(3):
                gather_copy(m, 0, k + 4).start()
            own_copy(k + 4).start()

        @pl.when((k <= 0) & (k > -LEAD))
        def _():
            pick_columns(k + 5)

        @pl.when(k + 5 < NK)
        def _():
            for m in range(2):
                half_copy(m, k + 5).start()

        @pl.when((k + 6 == NC) | (k + 6 == 2 * NC))
        def _():
            for m in range(2):
                cols_copy(m, (k + 6) // NC).start()

    def reduce_step(k):
        def live(lag):
            return (k - lag >= 0) & (k - lag < NK)

        def finish():
            kf = k - 4
            reduce_wait(3, kf)
            for m in range(3):
                done = rcs[m][lax.rem(kf, 3)] + pbs[m][lax.rem(kf, 2), (z, x, y)[m]]
                if m == 2:
                    o2_v[LAYERS - 1 - kf // NC, pl.ds(pl.multiple_of(lax.rem(kf, NC) * CPD, CPD), CPD), :] = done
                else:
                    dones[m][...] = done

        def third():
            kf = k - 3
            par = lax.rem(kf, 2)
            reduce_wait(2, kf)
            for m in range(3):
                for a in range(2):
                    kept = (lambda: pa1[par, a, y], lambda: pa3[par, z, a], lambda: pa2[par, a, x])[m]()
                    pbs[m][par, a] = rbs[m][lax.rem(kf, 3), a] + kept
                reduce_copy(m, 3, kf).start()

        def second():
            kf = k - 2
            par = lax.rem(kf, 2)
            reduce_wait(1, kf)
            for m in range(3):
                for a in range(2):
                    for b in range(2):
                        kept = (lambda: g1_v[par, a, b, x, c], lambda: g3_v[par, a, y, b, c], lambda: g2_v[par, z, a, b, c])[m]()
                        pas[m][par, a, b] = ras[m][lax.rem(kf, 3), a, b] + kept
                reduce_copy(m, 2, kf).start()

        def first():
            kf = k - 1
            par = lax.rem(kf, 2)
            reduce_wait(0, kf)
            for m in range(3):
                for a in range(2):
                    for b in range(2):
                        for d in range(2):
                            grads[m][par, a, b, d, c] = grads[m][par, a, b, d, c] + rds[m][par, a, b, d]
                reduce_copy(m, 1, kf).start()

        @pl.when((k + 6 == NC) | (k + 6 == 2 * NC))
        def _():
            for m in range(2):
                cols_copy(m, (k + 6) // NC).wait()

        @pl.when(k <= NK)
        def _():
            pl.when(live(4))(finish)

        @pl.when(k < NK)
        def _():
            pl.when(live(3))(third)
            pl.when(live(2))(second)
            pl.when(live(1))(first)

        @pl.when(k >= NK)
        def _():
            pl.when(live(1))(first)
            pl.when(k == NK)(lambda: finalize_layer(LAYERS - 1))
            pl.when(live(2))(second)
            pl.when(live(3))(third)

        @pl.when(k > NK)
        def _():
            finish()

    def row_phase(k):
        s = lax.rem(k, WS)

        def body(b, carry):
            @pl.when((k == 0) & (b == 1))
            def _():
                gather_rest(k)

            rows = pl.ds(pl.multiple_of(b * RB, RB), RB)
            w1 = jnp.concatenate([w1_v[s, 0].reshape(D, HALF), w1_v[s, 1].reshape(D, HALF)], axis=1)
            w3 = jnp.concatenate([w3_v[s, 0].reshape(D, HALF), w3_v[s, 1].reshape(D, HALF)], axis=1)
            w2 = w2_v[s].reshape(CH, D)
            nb = n_v[rows, :]
            u = dot(nb, w1, 1, 0)
            v = dot(nb, w3, 1, 0)
            da = jnp.concatenate([dot(g_v[pl.ds(pl.multiple_of(b * RB + q * (RB // 2), RB // 2), RB // 2), :], w2, 1, 1) for q in range(2)], axis=0)
            sig = 1.0 / (1.0 + jnp.exp(-u))
            act = u * sig
            a_v[rows, :] = (act * v).astype(BF)
            du = (da * v * sig * (1.0 + u * (1.0 - sig))).astype(BF)
            dv = (da * act).astype(BF)
            d_v[rows, pl.ds(0, CH)] = du
            d_v[rows, pl.ds(CH, CH)] = dv
            for q in range(2):
                rq = slice(q * (RB // 2), (q + 1) * (RB // 2))
                rr = pl.ds(pl.multiple_of(b * RB + q * (RB // 2), RB // 2), RB // 2)
                dn_v[rr, :] += dot(du[rq], w1, 1, 1) + dot(dv[rq], w3, 1, 1)
            return carry

        lax.fori_loop(0, ROWS // RB, body, 0)

    def grad_phase(k):
        par = lax.rem(k, 2)
        pick_columns(k + 6)
        put_columns(k - 4)
        nt = nt_v[...]
        g1_v[par] = dot(nt, d_v[:, pl.ds(0, CH)], 1, 0).reshape(2, 2, 2, 2, DS, CH)
        g3_v[par] = dot(nt, d_v[:, pl.ds(CH, CH)], 1, 0).reshape(2, 2, 2, 2, DS, CH)
        g2_v[par] = dot(gt_v[...], a_v[...], 1, 0).T.reshape(2, 2, 2, 2, CPD, D)

    for m in range(2):
        cols_copy(m, 0).start()
    barrier = pltpu.get_barrier_semaphore()
    for peer in (core, nx, ny, nz):
        pl.semaphore_signal(barrier, inc=1, device_id=(peer,), device_id_type=MESH)
    for b in range(HR):
        h_copy(0, b).start()
    g_copy().start()
    for m in range(2):
        cols_copy(m, 0).wait()
    pick_columns(0)
    pl.semaphore_wait(barrier, 4)

    def step(t, carry):
        k = t - LEAD
        inside = (k >= 0) & (k < NK)
        last = inside & (lax.rem(k + NC, NC) == NC - 1)
        gather_first(k)

        @pl.when(k != 0)
        def _():
            gather_rest(k)

        @pl.when((t >= 1) & (t < LEAD))
        def _():
            @pl.when(t == 1)
            def _():
                g_copy().wait()

            def rows(b, cc):
                prepare_rows(0, b)
                return cc
            lax.fori_loop(3 * (t - 1), 3 * t - t // 3 - t // 4 * 3, rows, 0)

        @pl.when(inside)
        def _():
            row_phase(k)

        @pl.when(last & (k < NK - 1))
        def _():
            finalize_layer(k // NC)

        reduce_step(k)

        @pl.when(inside)
        def _():
            grad_phase(k)
            for m in range(3):
                reduce_copy(m, 0, k).start()

        @pl.when(k >= NK)
        def _():
            put_columns(k - 4)

        @pl.when(last & (k < NK - 1))
        def _():
            li = k // NC

            def rows(b, cc):
                prepare_rows(li + 1, b)
                return cc
            lax.fori_loop(0, NB, rows, 0)
        return carry

    lax.fori_loop(0, LEAD + NK + TAIL, step, 0)


def hand_out(*refs):
    srcs, dsts, sem = refs[:4], refs[4:8], refs[8]
    pieces = [(j, layer) for j in range(3) for layer in range(LAYERS)]
    pieces += [(3, pl.ds(q * (ROWS // 4), ROWS // 4)) for q in range(4)]
    copies = [pltpu.make_async_copy(srcs[j].at[w], dsts[j].at[w], sem.at[n]) for n, (j, w) in enumerate(pieces)]
    for copy in copies:
        copy.start()
    for copy in copies:
        copy.wait()


def fused(h, g, w1, w3, w2):
    any_spec = pl.BlockSpec(memory_space=pl.ANY)
    V = pltpu.VMEM
    wide, low = (DS, CH), (CPD, D)
    three = lambda *lead: [V(lead + wide, F32), V(lead + wide, F32), V(lead + low, F32)]
    scratch = [
        V((ROWS, D), BF), V((D, ROWS), BF), V((D, ROWS), BF),
        V((ROWS, D), F32), V((HR, BB, D), BF), V((ROWS, CH), BF), V((ROWS, 2 * CH), BF),
        V((DS, FF), BF), V((DS, FF), BF), V((2, 2, DS, LANES), F32), V((2, 2, DS, LANES), F32),
        V((2, DS, LANES), F32), V((2, DS, LANES), F32),
        V((WS, 2, 2, 2, 2, 2 * DS, HALF), BF), V((WS, 2, 2, 2, 2, 2 * DS, HALF), BF), V((WS, 2, 2, 2, 2, CPD, D), BF),
        *three(2, 2, 2, 2, 2),
        *three(2, 2, 2, 2), *three(3, 2, 2), *three(3, 2), *three(3),
        *three(2, 2, 2), *three(2, 2), V(wide, F32), V(wide, F32),
        pltpu.SemaphoreType.DMA((6, 2)), pltpu.SemaphoreType.DMA((6, 2)),
        pltpu.SemaphoreType.DMA((4, 3)), pltpu.SemaphoreType.DMA((4, 3)),
        pltpu.SemaphoreType.DMA((2,)), pltpu.SemaphoreType.DMA((2,)),
        pltpu.SemaphoreType.DMA(()), pltpu.SemaphoreType.DMA((2,)),
        pltpu.SemaphoreType.DMA((HR,)), pltpu.SemaphoreType.DMA(()),
    ]
    results = (
        jax.ShapeDtypeStruct((LAYERS, DS, FF), F32),
        jax.ShapeDtypeStruct((LAYERS, DS, FF), F32),
        jax.ShapeDtypeStruct((LAYERS, FS, D), F32),
        jax.ShapeDtypeStruct((ROWS, D), BF),
    )
    vmem_spec = pl.BlockSpec(memory_space=pltpu.VMEM)
    parts = pl.pallas_call(
        kernel,
        name='mlp_backward',
        out_shape=tuple(V(r.shape, r.dtype) for r in results),
        in_specs=[any_spec] * 5,
        out_specs=(vmem_spec,) * 4,
        scratch_shapes=scratch,
        compiler_params=pltpu.CompilerParams(collective_id=0, has_side_effects=True, vmem_limit_bytes=51 * 1024 * 1024),
    )(h, g, w1, w3, w2)
    return pl.pallas_call(
        hand_out,
        name='hand_out',
        out_shape=results,
        in_specs=[vmem_spec] * 4,
        out_specs=(any_spec,) * 4,
        scratch_shapes=[pltpu.SemaphoreType.DMA((13,))],
        compiler_params=pltpu.CompilerParams(vmem_limit_bytes=1024 * 1024),
    )(*[pltpu.with_memory_space_constraint(part, pltpu.VMEM) for part in parts])


def solution(mesh):
    weight_spec = P(None, 'fsdp', None)
    row_spec = P('fsdp', None)

    return jax.shard_map(fused, mesh=mesh, in_specs=(weight_spec, row_spec, weight_spec, weight_spec, weight_spec), out_specs=(weight_spec, weight_spec, weight_spec, row_spec), check_vma=False)
```

```python
import jax
import jax.numpy as jnp
from jax import lax
from jax.experimental import pallas as pl
from jax.experimental.pallas import tpu as pltpu
from jax.sharding import PartitionSpec as P

EPS = 1e-6
LAYERS = 3
D = 896
FF = 4864
ROWS = 2048
DEV = 16
DS = D // DEV
FS = FF // DEV
CPD = 16
CH = CPD * DEV
NC = FF // CH
NK = NC * LAYERS
LEAD = 5
TAIL = 4
WS = 6
RB = 1024
BB = 256
HALF = CH // 2
LANES = 128
NB = ROWS // BB
HR = 4
MESH = pl.DeviceIdType.MESH
BF = jnp.bfloat16
F32 = jnp.float32


def dot(a, b, ca, cb):
    return lax.dot_general(a, b, (((ca,), (cb,)), ((), ())), preferred_element_type=F32)


def kernel(h_hbm, g_hbm, w1_hbm, w3_hbm, w2_hbm,
           o1_v, o3_v, o2_v, g_v,
           n_v, nt_v, gt_v, dn_v, h_v, a_v, d_v,
           c1_v, c3_v, e1_v, e3_v, f1_v, f3_v,
           w1_v, w3_v, w2_v,
           g1_v, g3_v, g2_v,
           rd1, rd3, rd2, ra1, ra3, ra2, rb1, rb3, rb2, rc1, rc3, rc2,
           pa1, pa3, pa2, pb1, pb3, pb2, s1, s3,
           ag_send, ag_recv, rs_send, rs_recv, ex_send, ex_recv, own_sem, cols_sem, h_sem, g_sem):
    me = lax.axis_index('fsdp')
    c = me % 2
    x = (me // 2) % 2
    y = (me // 4) % 2
    z = (me // 8) % 2
    core = me + 1 - 2 * c
    nx = me + 2 - 4 * x
    ny = me + 4 - 8 * y
    nz = me + 8 - 16 * z

    weights = (w1_v, w3_v, w2_v)
    grads = (g1_v, g3_v, g2_v)
    rds, ras, rbs, rcs = (rd1, rd3, rd2), (ra1, ra3, ra2), (rb1, rb3, rb2), (rc1, rc3, rc2)
    pas, pbs, outs, dones = (pa1, pa3, pa2), (pb1, pb3, pb2), (o1_v, o3_v), (s1, s3)
    cols, halves, theirs = (c1_v, c3_v), (e1_v, e3_v), (f1_v, f3_v)
    order = ((nx, ny, nz), (ny, nz, nx), (nz, nx, ny))

    def gather_slice(m, stage, k):
        s = lax.rem(k, WS)
        w = weights[m]
        if m == 0:
            return (lambda: w.at[s, c, z, y, x], lambda: w.at[s, c, z, y], lambda: w.at[s, c, z],
                    lambda: w.at[s, c, z, y], lambda: w.at[s, c, z, 1 - y], lambda: w.at[s, c, 1 - z])[stage]()
        if m == 1:
            return (lambda: w.at[s, c, z, y, x], lambda: w.at[s, c, z, :, x], lambda: w.at[s, c, :, :, x],
                    lambda: w.at[s, c, z, :, x], lambda: w.at[s, c, 1 - z, :, x], lambda: w.at[s, c, :, :, 1 - x])[stage]()
        return (lambda: w.at[s, z, y, x, c], lambda: w.at[s, :, y, x, c], lambda: w.at[s, :, y, :, c],
                lambda: w.at[s, :, y, x, c], lambda: w.at[s, :, y, 1 - x, c], lambda: w.at[s, :, 1 - y, :, c])[stage]()

    def own_rows(k):
        return w2_hbm.at[LAYERS - 1 - k // NC, pl.ds(pl.multiple_of(lax.rem(k, NC) * CPD, CPD), CPD)]

    def gather_copy(m, stage, k):
        par = lax.rem(k, 2)
        dst = gather_slice(m, stage, k)
        src = own_rows(k) if (stage == 0 and m == 2) else dst
        peer = core if stage >= 3 else order[m][stage]
        return pltpu.make_async_remote_copy(
            src_ref=src, dst_ref=dst, send_sem=ag_send.at[stage, par], recv_sem=ag_recv.at[stage, par],
            device_id=(peer,), device_id_type=MESH)

    def wait_bytes(ref, *sems):
        for sem in sems:
            pltpu.make_async_copy(ref, ref, sem).wait()

    def gather_wait(stage, k):
        par = lax.rem(k, 2)
        three = w1_v.at[pl.ds(0, 3)]
        blocks = (three.at[:, 0, 0, 0, 0], three.at[:, 0, 0, 0], three.at[:, 0, 0])[(0, 1, 2, 1, 1, 2)[stage]]
        wait_bytes(blocks, ag_send.at[stage, par], ag_recv.at[stage, par])

    def reduce_wait(stage, k):
        sem = lax.rem(k, 2 if stage == 0 else 3) + (0, 2, 5, 8)[stage]
        blocks = (w1_v.at[pl.ds(0, 3)], ra1, ra1.at[:, 0], ra1.at[:, 0, 0])[stage]
        wait_bytes(blocks, rs_send.at[sem], rs_recv.at[sem])

    def half_wait(k):
        par = lax.rem(k, 2)
        wait_bytes(f1_v, ex_send.at[par], ex_recv.at[par])

    def own_copy(k):
        return pltpu.make_async_copy(own_rows(k), gather_slice(2, 0, k), own_sem)

    def cols_copy(m, li):
        return pltpu.make_async_copy((w1_hbm, w3_hbm)[m].at[LAYERS - 1 - li], cols[m], cols_sem.at[m])

    def half_copy(m, k):
        par = lax.rem(k, 2)
        return pltpu.make_async_remote_copy(
            src_ref=halves[m].at[lax.rem(k, 3), 1 - c], dst_ref=theirs[m].at[par], send_sem=ex_send.at[par], recv_sem=ex_recv.at[par],
            device_id=(core,), device_id_type=MESH)

    lane = lax.broadcasted_iota(jnp.int32, (DS, LANES), 1)

    def place(p, i):
        col = FS * p + CPD * i
        tile = col // LANES
        return pl.ds(pl.multiple_of(tile * LANES, LANES), LANES), col - tile * LANES

    def pick_columns(k):
        i = lax.rem(k, NC)
        for m in range(2):
            for half in range(2):
                acc = jnp.zeros((DS, LANES), F32)
                for q in range(DEV // 2):
                    tile, off = place(half * (DEV // 2) + q, i)
                    part = pltpu.roll(cols[m][:, tile].astype(F32), lax.rem(CPD * q + LANES - off, LANES), 1)
                    acc = jnp.where((lane >= CPD * q) & (lane < CPD * (q + 1)), part, acc)
                halves[m][lax.rem(k, 3), half] = acc

    def merge_rows(k):
        par = lax.rem(k, 2)
        for m in range(2):
            mine, other = halves[m][lax.rem(k, 3), c], theirs[m][par]
            low = jnp.where(c == 0, mine, other)
            high = jnp.where(c == 0, other, mine)
            weights[m][lax.rem(k, WS), c, z, y, x] = jnp.concatenate([low, high], axis=0).astype(BF)

    def put_columns(k):
        layer = lax.rem(LAYERS - (k + NC) // NC, LAYERS)
        i = lax.rem(k + NC, NC)
        for m in range(2):
            for half in range(2):
                src = dones[m][:, half * LANES:(half + 1) * LANES]
                for q in range(DEV // 2):
                    tile, off = place(half * (DEV // 2) + q, i)
                    part = pltpu.roll(src, lax.rem(off + LANES - CPD * q, LANES), 1)
                    outs[m][layer, :, tile] = jnp.where((lane >= off) & (lane < off + CPD), part, outs[m][layer, :, tile])

    def reduce_copy(m, stage, k):
        par = lax.rem(k, 2)
        slot = par if stage == 0 else lax.rem(k, 3)
        sem = slot + (0, 2, 5, 8)[stage]
        g, pa, pb = grads[m], pas[m].at[par], pbs[m].at[par]
        if stage == 0:
            src, dst, peer = g.at[par, :, :, :, 1 - c], rds[m].at[par], core
        elif stage == 1:
            src = (g.at[par, :, :, 1 - x, c], g.at[par, :, 1 - y, :, c], g.at[par, 1 - z, :, :, c])[m]
            dst, peer = ras[m].at[slot], order[m][0]
        elif stage == 2:
            src = (pa.at[:, 1 - y], pa.at[1 - z], pa.at[:, 1 - x])[m]
            dst, peer = rbs[m].at[slot], order[m][1]
        else:
            src = (pb.at[1 - z], pb.at[1 - x], pb.at[1 - y])[m]
            dst, peer = rcs[m].at[slot], order[m][2]
        return pltpu.make_async_remote_copy(
            src_ref=src, dst_ref=dst, send_sem=rs_send.at[sem], recv_sem=rs_recv.at[sem],
            device_id=(peer,), device_id_type=MESH)

    def h_copy(li, b):
        rows = pl.ds(pl.multiple_of(b * BB, BB), BB)
        slot = lax.rem(b, HR)
        return pltpu.make_async_copy(h_hbm.at[LAYERS - 1 - li, rows], h_v.at[slot], h_sem.at[slot])

    def g_copy():
        return pltpu.make_async_copy(g_hbm, g_v, g_sem)

    def finalize_rows(b):
        rows = pl.ds(pl.multiple_of(b * BB, BB), BB)
        hf = h_v[lax.rem(b, HR)].astype(F32)
        r = lax.rsqrt(jnp.mean(hf * hf, axis=-1, keepdims=True) + EPS)
        m = hf * r
        dn = dn_v[rows, :]
        dr = r * (dn - m * jnp.mean(dn * m, axis=-1, keepdims=True))
        g_v[rows, :] = (g_v[rows, :].astype(F32) + dr).astype(BF)

    def finalize_layer(li):
        def rows(b, cc):
            h_copy(li, b).wait()
            finalize_rows(b)

            @pl.when(b < NB - HR)
            def _():
                h_copy(li, b + HR).start()

            @pl.when((b >= NB - HR) & (li < LAYERS - 1))
            def _():
                h_copy(li + 1, b + HR - NB).start()
            return cc
        lax.fori_loop(0, NB, rows, 0)

    def prepare_rows(li, b):
        rows = pl.ds(pl.multiple_of(b * BB, BB), BB)
        h_copy(li, b).wait()
        hf = h_v[lax.rem(b, HR)].astype(F32)
        r = lax.rsqrt(jnp.mean(hf * hf, axis=-1, keepdims=True) + EPS)
        nb = (hf * r).astype(BF)
        n_v[rows, :] = nb
        nt_v[:, rows] = nb.T
        gt_v[:, rows] = g_v[rows, :].T
        dn_v[rows, :] = jnp.zeros((BB, D), F32)
        h_copy(li, lax.rem(b + HR, NB)).start()

    def gather_first(k):
        @pl.when((k >= 0) & (k < NK))
        def _():
            gather_wait(5, k)

    def gather_rest(k):
        def live(lag):
            return (k + lag >= 0) & (k + lag < NK)

        for lag, stage in ((1, 2), (2, 1), (3, 0)):
            @pl.when(live(lag))
            def _():
                gather_wait(stage, k + lag)
                if stage > 0:
                    gather_wait(stage + 2, k + lag)
                if stage == 0:
                    own_copy(k + lag).wait()
                for m in range(3):
                    gather_copy(m, stage + 3, k + lag).start()
                    if stage < 2:
                        gather_copy(m, stage + 1, k + lag).start()

        @pl.when(live(4))
        def _():
            half_wait(k + 4)
            merge_rows(k + 4)
            for m in range(3):
                gather_copy(m, 0, k + 4).start()
            own_copy(k + 4).start()

        @pl.when(k + 5 < NK)
        def _():
            for m in range(2):
                half_copy(m, k + 5).start()

        @pl.when(k < -3)
        def _():
            pick_columns(k + 6)

        @pl.when((k >= -4) & (k < -1))
        def _():
            pick_columns(k + 7)

        @pl.when((k + 6 == NC) | (k + 6 == 2 * NC))
        def _():
            for m in range(2):
                cols_copy(m, (k + 6) // NC).start()

    def reduce_step(k):
        def live(lag):
            return (k - lag >= 0) & (k - lag < NK)

        def finish():
            kf = k - 4
            reduce_wait(3, kf)
            for m in range(3):
                done = rcs[m][lax.rem(kf, 3)] + pbs[m][lax.rem(kf, 2), (z, x, y)[m]]
                if m == 2:
                    o2_v[LAYERS - 1 - kf // NC, pl.ds(pl.multiple_of(lax.rem(kf, NC) * CPD, CPD), CPD), :] = done
                else:
                    dones[m][...] = done

        def third():
            kf = k - 3
            par = lax.rem(kf, 2)
            reduce_wait(2, kf)
            for m in range(3):
                for a in range(2):
                    kept = (lambda: pa1[par, a, y], lambda: pa3[par, z, a], lambda: pa2[par, a, x])[m]()
                    pbs[m][par, a] = rbs[m][lax.rem(kf, 3), a] + kept
                reduce_copy(m, 3, kf).start()

        def second():
            kf = k - 2
            par = lax.rem(kf, 2)
            reduce_wait(1, kf)
            for m in range(3):
                for a in range(2):
                    for b in range(2):
                        kept = (lambda: g1_v[par, a, b, x, c], lambda: g3_v[par, a, y, b, c], lambda: g2_v[par, z, a, b, c])[m]()
                        pas[m][par, a, b] = ras[m][lax.rem(kf, 3), a, b] + kept
                reduce_copy(m, 2, kf).start()

        def first():
            kf = k - 1
            par = lax.rem(kf, 2)
            reduce_wait(0, kf)
            for m in range(3):
                for a in range(2):
                    for b in range(2):
                        for d in range(2):
                            grads[m][par, a, b, d, c] = grads[m][par, a, b, d, c] + rds[m][par, a, b, d]
                reduce_copy(m, 1, kf).start()

        @pl.when((k + 6 == NC) | (k + 6 == 2 * NC))
        def _():
            for m in range(2):
                cols_copy(m, (k + 6) // NC).wait()

        @pl.when(k <= NK)
        def _():
            pl.when(live(4))(finish)

        @pl.when(k < NK)
        def _():
            pl.when(live(3))(third)
            pl.when(live(2))(second)
            pl.when(live(1))(first)

        @pl.when(k >= NK)
        def _():
            pl.when(live(1))(first)
            pl.when(k == NK)(lambda: finalize_layer(LAYERS - 1))
            pl.when(live(2))(second)
            pl.when(live(3))(third)

        @pl.when(k > NK)
        def _():
            finish()

    def row_phase(k):
        s = lax.rem(k, WS)

        def body(b, carry):
            @pl.when((k == 0) & (b == 1))
            def _():
                gather_rest(k)

            rows = pl.ds(pl.multiple_of(b * RB, RB), RB)
            w1 = jnp.concatenate([w1_v[s, 0].reshape(D, HALF), w1_v[s, 1].reshape(D, HALF)], axis=1)
            w3 = jnp.concatenate([w3_v[s, 0].reshape(D, HALF), w3_v[s, 1].reshape(D, HALF)], axis=1)
            w2 = w2_v[s].reshape(CH, D)
            nb = n_v[rows, :]
            u = dot(nb, w1, 1, 0)
            v = dot(nb, w3, 1, 0)
            da = jnp.concatenate([dot(g_v[pl.ds(pl.multiple_of(b * RB + q * (RB // 2), RB // 2), RB // 2), :], w2, 1, 1) for q in range(2)], axis=0)
            sig = 1.0 / (1.0 + jnp.exp(-u))
            act = u * sig
            a_v[rows, :] = (act * v).astype(BF)
            du = (da * v * sig * (1.0 + u * (1.0 - sig))).astype(BF)
            dv = (da * act).astype(BF)
            d_v[rows, pl.ds(0, CH)] = du
            d_v[rows, pl.ds(CH, CH)] = dv
            for q in range(2):
                rq = slice(q * (RB // 2), (q + 1) * (RB // 2))
                rr = pl.ds(pl.multiple_of(b * RB + q * (RB // 2), RB // 2), RB // 2)
                dn_v[rr, :] += dot(du[rq], w1, 1, 1) + dot(dv[rq], w3, 1, 1)
            return carry

        lax.fori_loop(0, ROWS // RB, body, 0)

    def grad_phase(k):
        par = lax.rem(k, 2)
        pick_columns(k + 6)
        put_columns(k - 4)
        nt = nt_v[...]
        g1_v[par] = dot(nt, d_v[:, pl.ds(0, CH)], 1, 0).reshape(2, 2, 2, 2, DS, CH)
        g3_v[par] = dot(nt, d_v[:, pl.ds(CH, CH)], 1, 0).reshape(2, 2, 2, 2, DS, CH)
        g2_v[par] = dot(gt_v[...], a_v[...], 1, 0).T.reshape(2, 2, 2, 2, CPD, D)

    for m in range(2):
        cols_copy(m, 0).start()
    barrier = pltpu.get_barrier_semaphore()
    for peer in (core, nx, ny, nz):
        pl.semaphore_signal(barrier, inc=1, device_id=(peer,), device_id_type=MESH)
    for b in range(HR):
        h_copy(0, b).start()
    g_copy().start()
    for m in range(2):
        cols_copy(m, 0).wait()
    pick_columns(0)
    pl.semaphore_wait(barrier, 4)

    def step(t, carry):
        k = t - LEAD
        inside = (k >= 0) & (k < NK)
        last = inside & (lax.rem(k + NC, NC) == NC - 1)
        gather_first(k)

        @pl.when(k != 0)
        def _():
            gather_rest(k)

        @pl.when((t >= 1) & (t < LEAD))
        def _():
            @pl.when(t == 1)
            def _():
                g_copy().wait()

            def rows(b, cc):
                prepare_rows(0, b)
                return cc
            lax.fori_loop(3 * (t - 1), 3 * t - t // 3 - t // 4 * 3, rows, 0)

        @pl.when(inside)
        def _():
            row_phase(k)

        @pl.when(last & (k < NK - 1))
        def _():
            finalize_layer(k // NC)

        reduce_step(k)

        @pl.when(inside)
        def _():
            grad_phase(k)
            for m in range(3):
                reduce_copy(m, 0, k).start()

        @pl.when(k >= NK)
        def _():
            put_columns(k - 4)

        @pl.when(last & (k < NK - 1))
        def _():
            li = k // NC

            def rows(b, cc):
                prepare_rows(li + 1, b)
                return cc
            lax.fori_loop(0, NB, rows, 0)
        return carry

    lax.fori_loop(0, LEAD + NK + TAIL, step, 0)


def hand_out(*refs):
    srcs, dsts, sem = refs[:4], refs[4:8], refs[8]
    pieces = []
    for j, cut in enumerate((DS * 3 // 7, DS * 3 // 7, FS // 2)):
        for layer in range(LAYERS):
            pieces += [(j, (layer, pl.ds(0, cut))), (j, (layer, pl.ds(cut, srcs[j].shape[1] - cut)))]
    pieces += [(3, pl.ds(q * (ROWS // 8), ROWS // 8)) for q in range(8)]
    copies = [pltpu.make_async_copy(srcs[j].at[w], dsts[j].at[w], sem.at[n]) for n, (j, w) in enumerate(pieces)]
    for copy in copies:
        copy.start()
    for copy in copies:
        copy.wait()


def fused(h, g, w1, w3, w2):
    any_spec = pl.BlockSpec(memory_space=pl.ANY)
    V = pltpu.VMEM
    wide, low = (DS, CH), (CPD, D)
    three = lambda *lead: [V(lead + wide, F32), V(lead + wide, F32), V(lead + low, F32)]
    scratch = [
        V((ROWS, D), BF), V((D, ROWS), BF), V((D, ROWS), BF),
        V((ROWS, D), F32), V((HR, BB, D), BF), V((ROWS, CH), BF), V((ROWS, 2 * CH), BF),
        V((DS, FF), BF), V((DS, FF), BF), V((3, 2, DS, LANES), F32), V((3, 2, DS, LANES), F32),
        V((2, DS, LANES), F32), V((2, DS, LANES), F32),
        V((WS, 2, 2, 2, 2, 2 * DS, HALF), BF), V((WS, 2, 2, 2, 2, 2 * DS, HALF), BF), V((WS, 2, 2, 2, 2, CPD, D), BF),
        *three(2, 2, 2, 2, 2),
        *three(2, 2, 2, 2), *three(3, 2, 2), *three(3, 2), *three(3),
        *three(2, 2, 2), *three(2, 2), V(wide, F32), V(wide, F32),
        pltpu.SemaphoreType.DMA((6, 2)), pltpu.SemaphoreType.DMA((6, 2)),
        pltpu.SemaphoreType.DMA((11,)), pltpu.SemaphoreType.DMA((11,)),
        pltpu.SemaphoreType.DMA((2,)), pltpu.SemaphoreType.DMA((2,)),
        pltpu.SemaphoreType.DMA(()), pltpu.SemaphoreType.DMA((2,)),
        pltpu.SemaphoreType.DMA((HR,)), pltpu.SemaphoreType.DMA(()),
    ]
    results = (
        jax.ShapeDtypeStruct((LAYERS, DS, FF), F32),
        jax.ShapeDtypeStruct((LAYERS, DS, FF), F32),
        jax.ShapeDtypeStruct((LAYERS, FS, D), F32),
        jax.ShapeDtypeStruct((ROWS, D), BF),
    )
    vmem_spec = pl.BlockSpec(memory_space=pltpu.VMEM)
    parts = pl.pallas_call(
        kernel,
        name='mlp_backward',
        out_shape=tuple(V(r.shape, r.dtype) for r in results),
        in_specs=[any_spec] * 5,
        out_specs=(vmem_spec,) * 4,
        scratch_shapes=scratch,
        compiler_params=pltpu.CompilerParams(collective_id=0, has_side_effects=True, vmem_limit_bytes=51 * 1024 * 1024),
    )(h, g, w1, w3, w2)
    return pl.pallas_call(
        hand_out,
        name='hand_out',
        out_shape=results,
        in_specs=[vmem_spec] * 4,
        out_specs=(any_spec,) * 4,
        scratch_shapes=[pltpu.SemaphoreType.DMA((26,))],
        compiler_params=pltpu.CompilerParams(vmem_limit_bytes=1024 * 1024),
    )(*[pltpu.with_memory_space_constraint(part, pltpu.VMEM) for part in parts])


def solution(mesh):
    weight_spec = P(None, 'fsdp', None)
    row_spec = P('fsdp', None)

    return jax.shard_map(fused, mesh=mesh, in_specs=(weight_spec, row_spec, weight_spec, weight_spec, weight_spec), out_specs=(weight_spec, weight_spec, weight_spec, row_spec), check_vma=False)
```

```python
import jax
import jax.numpy as jnp
from jax import lax
from jax.experimental import pallas as pl
from jax.experimental.pallas import tpu as pltpu
from jax.sharding import PartitionSpec as P

EPS = 1e-6
LAYERS = 3
D = 896
FF = 4864
ROWS = 2048
DEV = 16
DS = D // DEV
FS = FF // DEV
CPD = 16
CH = CPD * DEV
NC = FF // CH
NK = NC * LAYERS
LEAD = 5
TAIL = 4
WS = 6
RB = 1024
BB = 256
HALF = CH // 2
LANES = 128
NB = ROWS // BB
HR = 4
MESH = pl.DeviceIdType.MESH
BF = jnp.bfloat16
F32 = jnp.float32


def dot(a, b, ca, cb):
    return lax.dot_general(a, b, (((ca,), (cb,)), ((), ())), preferred_element_type=F32)


def kernel(h_hbm, g_hbm, w1_hbm, w3_hbm, w2_hbm,
           o1_v, o3_v, o2_v, g_v,
           n_v, nt_v, gt_v, dn_v, h_v, a_v, d_v,
           c1_v, c3_v, e1_v, e3_v, f1_v, f3_v,
           w1_v, w3_v, w2_v,
           g1_v, g3_v, g2_v,
           rd1, rd3, rd2, ra1, ra3, ra2, rb1, rb3, rb2, rc1, rc3, rc2,
           pa1, pa3, pa2, pb1, pb3, pb2, s1, s3,
           ag_send, ag_recv, rs_send, rs_recv, ex_send, ex_recv, own_sem, cols_sem, h_sem, g_sem):
    me = lax.axis_index('fsdp')
    c = me % 2
    x = (me // 2) % 2
    y = (me // 4) % 2
    z = (me // 8) % 2
    core = me + 1 - 2 * c
    nx = me + 2 - 4 * x
    ny = me + 4 - 8 * y
    nz = me + 8 - 16 * z

    weights = (w1_v, w3_v, w2_v)
    grads = (g1_v, g3_v, g2_v)
    rds, ras, rbs, rcs = (rd1, rd3, rd2), (ra1, ra3, ra2), (rb1, rb3, rb2), (rc1, rc3, rc2)
    pas, pbs, outs, dones = (pa1, pa3, pa2), (pb1, pb3, pb2), (o1_v, o3_v), (s1, s3)
    cols, halves, theirs = (c1_v, c3_v), (e1_v, e3_v), (f1_v, f3_v)
    order = ((nx, ny, nz), (ny, nz, nx), (nz, nx, ny))

    def gather_slice(m, stage, k):
        s = lax.rem(k, WS)
        w = weights[m]
        if m == 0:
            return (lambda: w.at[s, c, z, y, x], lambda: w.at[s, c, z, y], lambda: w.at[s, c, z],
                    lambda: w.at[s, c, z, y], lambda: w.at[s, c, z, 1 - y], lambda: w.at[s, c, 1 - z])[stage]()
        if m == 1:
            return (lambda: w.at[s, c, z, y, x], lambda: w.at[s, c, z, :, x], lambda: w.at[s, c, :, :, x],
                    lambda: w.at[s, c, z, :, x], lambda: w.at[s, c, 1 - z, :, x], lambda: w.at[s, c, :, :, 1 - x])[stage]()
        return (lambda: w.at[s, z, y, x, c], lambda: w.at[s, :, y, x, c], lambda: w.at[s, :, y, :, c],
                lambda: w.at[s, :, y, x, c], lambda: w.at[s, :, y, 1 - x, c], lambda: w.at[s, :, 1 - y, :, c])[stage]()

    def own_rows(k):
        return w2_hbm.at[LAYERS - 1 - k // NC, pl.ds(pl.multiple_of(lax.rem(k, NC) * CPD, CPD), CPD)]

    def gather_copy(m, stage, k):
        par = lax.rem(k, 2)
        dst = gather_slice(m, stage, k)
        src = own_rows(k) if (stage == 0 and m == 2) else dst
        peer = core if stage >= 3 else order[m][stage]
        return pltpu.make_async_remote_copy(
            src_ref=src, dst_ref=dst, send_sem=ag_send.at[stage, par], recv_sem=ag_recv.at[stage, par],
            device_id=(peer,), device_id_type=MESH)

    def wait_bytes(ref, *sems):
        for sem in sems:
            pltpu.make_async_copy(ref, ref, sem).wait()

    def gather_wait(stage, k):
        par = lax.rem(k, 2)
        three = w1_v.at[pl.ds(0, 3)]
        blocks = (three.at[:, 0, 0, 0, 0], three.at[:, 0, 0, 0], three.at[:, 0, 0])[(0, 1, 2, 1, 1, 2)[stage]]
        wait_bytes(blocks, ag_send.at[stage, par], ag_recv.at[stage, par])

    def reduce_wait(stage, k):
        slot = lax.rem(k, 2 if stage == 0 else 3)
        blocks = (w1_v.at[pl.ds(0, 3)], ra1, ra1.at[:, 0], ra1.at[:, 0, 0])[stage]
        wait_bytes(blocks, rs_send.at[stage, slot], rs_recv.at[stage, slot])

    def half_wait(k):
        par = lax.rem(k, 2)
        wait_bytes(f1_v, ex_send.at[par], ex_recv.at[par])

    def own_copy(k):
        return pltpu.make_async_copy(own_rows(k), gather_slice(2, 0, k), own_sem)

    def cols_copy(m, li):
        return pltpu.make_async_copy((w1_hbm, w3_hbm)[m].at[LAYERS - 1 - li], cols[m], cols_sem.at[m])

    def half_copy(m, k):
        par = lax.rem(k, 2)
        return pltpu.make_async_remote_copy(
            src_ref=halves[m].at[par, 1 - c], dst_ref=theirs[m].at[par], send_sem=ex_send.at[par], recv_sem=ex_recv.at[par],
            device_id=(core,), device_id_type=MESH)

    lane = lax.broadcasted_iota(jnp.int32, (DS, LANES), 1)

    def place(p, i):
        col = FS * p + CPD * i
        tile = col // LANES
        return pl.ds(pl.multiple_of(tile * LANES, LANES), LANES), col - tile * LANES

    def pick_columns(k):
        i = lax.rem(k, NC)
        for m in range(2):
            for half in range(2):
                acc = jnp.zeros((DS, LANES), F32)
                for q in range(DEV // 2):
                    tile, off = place(half * (DEV // 2) + q, i)
                    part = pltpu.roll(cols[m][:, tile].astype(F32), lax.rem(CPD * q + LANES - off, LANES), 1)
                    acc = jnp.where((lane >= CPD * q) & (lane < CPD * (q + 1)), part, acc)
                halves[m][lax.rem(k, 2), half] = acc

    def merge_rows(k):
        par = lax.rem(k, 2)
        for m in range(2):
            mine, other = halves[m][par, c], theirs[m][par]
            low = jnp.where(c == 0, mine, other)
            high = jnp.where(c == 0, other, mine)
            weights[m][lax.rem(k, WS), c, z, y, x] = jnp.concatenate([low, high], axis=0).astype(BF)

    def put_columns(k):
        layer = lax.rem(LAYERS - (k + NC) // NC, LAYERS)
        i = lax.rem(k + NC, NC)
        for m in range(2):
            for half in range(2):
                src = dones[m][:, half * LANES:(half + 1) * LANES]
                for q in range(DEV // 2):
                    tile, off = place(half * (DEV // 2) + q, i)
                    part = pltpu.roll(src, lax.rem(off + LANES - CPD * q, LANES), 1)
                    outs[m][layer, :, tile] = jnp.where((lane >= off) & (lane < off + CPD), part, outs[m][layer, :, tile])

    def reduce_copy(m, stage, k):
        par = lax.rem(k, 2)
        slot = par if stage == 0 else lax.rem(k, 3)
        g, pa, pb = grads[m], pas[m].at[par], pbs[m].at[lax.rem(k, 3)]
        if stage == 0:
            src, dst, peer = g.at[par, :, :, :, 1 - c], rds[m].at[par], core
        elif stage == 1:
            src = (g.at[par, :, :, 1 - x, c], g.at[par, :, 1 - y, :, c], g.at[par, 1 - z, :, :, c])[m]
            dst, peer = ras[m].at[slot], order[m][0]
        elif stage == 2:
            src = (pa.at[:, 1 - y], pa.at[1 - z], pa.at[:, 1 - x])[m]
            dst, peer = rbs[m].at[slot], order[m][1]
        else:
            src = (pb.at[1 - z], pb.at[1 - x], pb.at[1 - y])[m]
            dst, peer = rcs[m].at[slot], order[m][2]
        return pltpu.make_async_remote_copy(
            src_ref=src, dst_ref=dst, send_sem=rs_send.at[stage, slot], recv_sem=rs_recv.at[stage, slot],
            device_id=(peer,), device_id_type=MESH)

    def h_copy(li, b):
        rows = pl.ds(pl.multiple_of(b * BB, BB), BB)
        slot = lax.rem(b, HR)
        return pltpu.make_async_copy(h_hbm.at[LAYERS - 1 - li, rows], h_v.at[slot], h_sem.at[slot])

    def g_copy():
        return pltpu.make_async_copy(g_hbm, g_v, g_sem)

    def finalize_rows(b):
        rows = pl.ds(pl.multiple_of(b * BB, BB), BB)
        hf = h_v[lax.rem(b, HR)].astype(F32)
        r = lax.rsqrt(jnp.mean(hf * hf, axis=-1, keepdims=True) + EPS)
        m = hf * r
        dn = dn_v[rows, :]
        dr = r * (dn - m * jnp.mean(dn * m, axis=-1, keepdims=True))
        g_v[rows, :] = (g_v[rows, :].astype(F32) + dr).astype(BF)

    def finalize_layer(li):
        def rows(b, cc):
            h_copy(li, b).wait()
            finalize_rows(b)

            @pl.when(b < NB - HR)
            def _():
                h_copy(li, b + HR).start()

            @pl.when((b >= NB - HR) & (li < LAYERS - 1))
            def _():
                h_copy(li + 1, b + HR - NB).start()
            return cc
        lax.fori_loop(0, NB, rows, 0)

    def prepare_rows(li, b):
        rows = pl.ds(pl.multiple_of(b * BB, BB), BB)
        h_copy(li, b).wait()
        hf = h_v[lax.rem(b, HR)].astype(F32)
        r = lax.rsqrt(jnp.mean(hf * hf, axis=-1, keepdims=True) + EPS)
        nb = (hf * r).astype(BF)
        n_v[rows, :] = nb
        nt_v[:, rows] = nb.T
        gt_v[:, rows] = g_v[rows, :].T
        dn_v[rows, :] = jnp.zeros((BB, D), F32)
        h_copy(li, lax.rem(b + HR, NB)).start()

    def gather_first(k):
        @pl.when((k >= 0) & (k < NK))
        def _():
            gather_wait(5, k)

    def gather_rest(k):
        def live(lag):
            return (k + lag >= 0) & (k + lag < NK)

        for lag, stage in ((1, 2), (2, 1), (3, 0)):
            @pl.when(live(lag))
            def _():
                gather_wait(stage, k + lag)
                if stage > 0:
                    gather_wait(stage + 2, k + lag)
                if stage == 0:
                    own_copy(k + lag).wait()
                for m in range(3):
                    gather_copy(m, stage + 3, k + lag).start()
                    if stage < 2:
                        gather_copy(m, stage + 1, k + lag).start()

        @pl.when(live(4))
        def _():
            half_wait(k + 4)
            merge_rows(k + 4)
            for m in range(3):
                gather_copy(m, 0, k + 4).start()
            own_copy(k + 4).start()

        @pl.when((k <= 0) & (k > -LEAD))
        def _():
            pick_columns(k + 5)

        @pl.when(k + 5 < NK)
        def _():
            for m in range(2):
                half_copy(m, k + 5).start()

        @pl.when((k + 6 == NC) | (k + 6 == 2 * NC))
        def _():
            for m in range(2):
                cols_copy(m, (k + 6) // NC).start()

    def reduce_step(k):
        def live(lag):
            return (k - lag >= 0) & (k - lag < NK)

        def finish(kf):
            reduce_wait(3, kf)
            for m in range(3):
                done = rcs[m][lax.rem(kf, 3)] + pbs[m][lax.rem(kf, 3), (z, x, y)[m]]
                if m == 2:
                    o2_v[LAYERS - 1 - kf // NC, pl.ds(pl.multiple_of(lax.rem(kf, NC) * CPD, CPD), CPD), :] = done
                else:
                    dones[m][...] = done

        def third(kf, send=True):
            par = lax.rem(kf, 2)
            reduce_wait(2, kf)
            for m in range(3):
                for a in range(2):
                    kept = (lambda: pa1[par, a, y], lambda: pa3[par, z, a], lambda: pa2[par, a, x])[m]()
                    pbs[m][lax.rem(kf, 3), a] = rbs[m][lax.rem(kf, 3), a] + kept
                if send:
                    reduce_copy(m, 3, kf).start()

        def second(kf):
            par = lax.rem(kf, 2)
            reduce_wait(1, kf)
            for m in range(3):
                for a in range(2):
                    for b in range(2):
                        kept = (lambda: g1_v[par, a, b, x, c], lambda: g3_v[par, a, y, b, c], lambda: g2_v[par, z, a, b, c])[m]()
                        pas[m][par, a, b] = ras[m][lax.rem(kf, 3), a, b] + kept
                reduce_copy(m, 2, kf).start()

        def first(kf):
            par = lax.rem(kf, 2)
            reduce_wait(0, kf)
            for m in range(3):
                for a in range(2):
                    for b in range(2):
                        for d in range(2):
                            grads[m][par, a, b, d, c] = grads[m][par, a, b, d, c] + rds[m][par, a, b, d]
                reduce_copy(m, 1, kf).start()

        @pl.when((k + 6 == NC) | (k + 6 == 2 * NC))
        def _():
            for m in range(2):
                cols_copy(m, (k + 6) // NC).wait()

        @pl.when(k <= NK)
        def _():
            pl.when(live(4))(lambda: finish(k - 4))

        @pl.when(k < NK)
        def _():
            pl.when(live(3))(lambda: third(k - 3))
            pl.when(live(2))(lambda: second(k - 2))
            pl.when(live(1))(lambda: first(k - 1))

        @pl.when(k == NK)
        def _():
            first(k - 1)
            finalize_layer(LAYERS - 1)
            second(k - 2)
            third(k - 3, send=False)

        @pl.when(k == NK + 1)
        def _():
            second(k - 2)
            for m in range(3):
                reduce_copy(m, 3, k - 4).start()
            third(k - 3)

        @pl.when(k == NK + 2)
        def _():
            third(k - 3)
            finish(k - 5)
            put_columns(k - 5)
            finish(k - 4)
            put_columns(k - 4)

        @pl.when(k == NK + 3)
        def _():
            finish(k - 4)
            put_columns(k - 4)

    def row_phase(k):
        s = lax.rem(k, WS)

        def body(b, carry):
            @pl.when((k == 0) & (b == 1))
            def _():
                gather_rest(k)

            rows = pl.ds(pl.multiple_of(b * RB, RB), RB)
            w1 = jnp.concatenate([w1_v[s, 0].reshape(D, HALF), w1_v[s, 1].reshape(D, HALF)], axis=1)
            w3 = jnp.concatenate([w3_v[s, 0].reshape(D, HALF), w3_v[s, 1].reshape(D, HALF)], axis=1)
            w2 = w2_v[s].reshape(CH, D)
            nb = n_v[rows, :]
            u = dot(nb, w1, 1, 0)
            v = dot(nb, w3, 1, 0)
            da = jnp.concatenate([dot(g_v[pl.ds(pl.multiple_of(b * RB + q * (RB // 2), RB // 2), RB // 2), :], w2, 1, 1) for q in range(2)], axis=0)
            sig = 1.0 / (1.0 + jnp.exp(-u))
            act = u * sig
            a_v[rows, :] = (act * v).astype(BF)
            du = (da * v * sig * (1.0 + u * (1.0 - sig))).astype(BF)
            dv = (da * act).astype(BF)
            d_v[rows, pl.ds(0, CH)] = du
            d_v[rows, pl.ds(CH, CH)] = dv
            for q in range(2):
                rq = slice(q * (RB // 2), (q + 1) * (RB // 2))
                rr = pl.ds(pl.multiple_of(b * RB + q * (RB // 2), RB // 2), RB // 2)
                dn_v[rr, :] += dot(du[rq], w1, 1, 1) + dot(dv[rq], w3, 1, 1)
            return carry

        lax.fori_loop(0, ROWS // RB, body, 0)

    def grad_phase(k):
        par = lax.rem(k, 2)
        pick_columns(k + 6)
        put_columns(k - 4)
        nt = nt_v[...]
        g1_v[par] = dot(nt, d_v[:, pl.ds(0, CH)], 1, 0).reshape(2, 2, 2, 2, DS, CH)
        g3_v[par] = dot(nt, d_v[:, pl.ds(CH, CH)], 1, 0).reshape(2, 2, 2, 2, DS, CH)
        g2_v[par] = dot(gt_v[...], a_v[...], 1, 0).T.reshape(2, 2, 2, 2, CPD, D)

    for m in range(2):
        cols_copy(m, 0).start()
    barrier = pltpu.get_barrier_semaphore()
    for peer in (core, nx, ny, nz):
        pl.semaphore_signal(barrier, inc=1, device_id=(peer,), device_id_type=MESH)
    for b in range(HR):
        h_copy(0, b).start()
    g_copy().start()
    for m in range(2):
        cols_copy(m, 0).wait()
    pick_columns(0)
    pl.semaphore_wait(barrier, 4)

    def step(t, carry):
        k = t - LEAD
        inside = (k >= 0) & (k < NK)
        last = inside & (lax.rem(k + NC, NC) == NC - 1)
        gather_first(k)

        @pl.when(k != 0)
        def _():
            gather_rest(k)

        @pl.when((t >= 1) & (t < LEAD))
        def _():
            @pl.when(t == 1)
            def _():
                g_copy().wait()

            def rows(b, cc):
                prepare_rows(0, b)
                return cc
            lax.fori_loop(3 * (t - 1), 3 * t - t // 3 - t // 4 * 3, rows, 0)

        @pl.when(inside)
        def _():
            row_phase(k)

        @pl.when(last & (k < NK - 1))
        def _():
            finalize_layer(k // NC)

        reduce_step(k)

        @pl.when(inside)
        def _():
            grad_phase(k)
            for m in range(3):
                reduce_copy(m, 0, k).start()

        @pl.when(k == NK)
        def _():
            put_columns(k - 4)

        @pl.when(last & (k < NK - 1))
        def _():
            li = k // NC

            def rows(b, cc):
                prepare_rows(li + 1, b)
                return cc
            lax.fori_loop(0, NB, rows, 0)
        return carry

    lax.fori_loop(0, LEAD + NK + TAIL, step, 0)


def hand_out(*refs):
    srcs, dsts, sem = refs[:4], refs[4:8], refs[8]
    pieces = [(j, layer) for j in range(3) for layer in range(LAYERS)]
    pieces += [(3, pl.ds(q * (ROWS // 4), ROWS // 4)) for q in range(4)]
    copies = [pltpu.make_async_copy(srcs[j].at[w], dsts[j].at[w], sem.at[n]) for n, (j, w) in enumerate(pieces)]
    for copy in copies:
        copy.start()
    for copy in copies:
        copy.wait()


def fused(h, g, w1, w3, w2):
    any_spec = pl.BlockSpec(memory_space=pl.ANY)
    V = pltpu.VMEM
    wide, low = (DS, CH), (CPD, D)
    three = lambda *lead: [V(lead + wide, F32), V(lead + wide, F32), V(lead + low, F32)]
    scratch = [
        V((ROWS, D), BF), V((D, ROWS), BF), V((D, ROWS), BF),
        V((ROWS, D), F32), V((HR, BB, D), BF), V((ROWS, CH), BF), V((ROWS, 2 * CH), BF),
        V((DS, FF), BF), V((DS, FF), BF), V((2, 2, DS, LANES), F32), V((2, 2, DS, LANES), F32),
        V((2, DS, LANES), F32), V((2, DS, LANES), F32),
        V((WS, 2, 2, 2, 2, 2 * DS, HALF), BF), V((WS, 2, 2, 2, 2, 2 * DS, HALF), BF), V((WS, 2, 2, 2, 2, CPD, D), BF),
        *three(2, 2, 2, 2, 2),
        *three(2, 2, 2, 2), *three(3, 2, 2), *three(3, 2), *three(3),
        *three(2, 2, 2), *three(3, 2), V(wide, F32), V(wide, F32),
        pltpu.SemaphoreType.DMA((6, 2)), pltpu.SemaphoreType.DMA((6, 2)),
        pltpu.SemaphoreType.DMA((4, 3)), pltpu.SemaphoreType.DMA((4, 3)),
        pltpu.SemaphoreType.DMA((2,)), pltpu.SemaphoreType.DMA((2,)),
        pltpu.SemaphoreType.DMA(()), pltpu.SemaphoreType.DMA((2,)),
        pltpu.SemaphoreType.DMA((HR,)), pltpu.SemaphoreType.DMA(()),
    ]
    results = (
        jax.ShapeDtypeStruct((LAYERS, DS, FF), F32),
        jax.ShapeDtypeStruct((LAYERS, DS, FF), F32),
        jax.ShapeDtypeStruct((LAYERS, FS, D), F32),
        jax.ShapeDtypeStruct((ROWS, D), BF),
    )
    vmem_spec = pl.BlockSpec(memory_space=pltpu.VMEM)
    parts = pl.pallas_call(
        kernel,
        name='mlp_backward',
        out_shape=tuple(V(r.shape, r.dtype) for r in results),
        in_specs=[any_spec] * 5,
        out_specs=(vmem_spec,) * 4,
        scratch_shapes=scratch,
        compiler_params=pltpu.CompilerParams(collective_id=0, has_side_effects=True, vmem_limit_bytes=51 * 1024 * 1024),
    )(h, g, w1, w3, w2)
    return pl.pallas_call(
        hand_out,
        name='hand_out',
        out_shape=results,
        in_specs=[vmem_spec] * 4,
        out_specs=(any_spec,) * 4,
        scratch_shapes=[pltpu.SemaphoreType.DMA((13,))],
        compiler_params=pltpu.CompilerParams(vmem_limit_bytes=1024 * 1024),
    )(*[pltpu.with_memory_space_constraint(part, pltpu.VMEM) for part in parts])


def solution(mesh):
    weight_spec = P(None, 'fsdp', None)
    row_spec = P('fsdp', None)

    return jax.shard_map(fused, mesh=mesh, in_specs=(weight_spec, row_spec, weight_spec, weight_spec, weight_spec), out_specs=(weight_spec, weight_spec, weight_spec, row_spec), check_vma=False)
```

```python
import jax
import jax.numpy as jnp
from jax import lax
from jax.experimental import pallas as pl
from jax.experimental.pallas import tpu as pltpu
from jax.sharding import PartitionSpec as P

EPS = 1e-6
LAYERS = 3
D = 896
FF = 4864
ROWS = 2048
DEV = 16
DS = D // DEV
FS = FF // DEV
CPD = 16
CH = CPD * DEV
NC = FF // CH
NK = NC * LAYERS
LEAD = 5
TAIL = 4
WS = 6
RB = 1024
BB = 256
HALF = CH // 2
LANES = 128
NB = ROWS // BB
HR = 4
MESH = pl.DeviceIdType.MESH
BF = jnp.bfloat16
F32 = jnp.float32


def dot(a, b, ca, cb):
    return lax.dot_general(a, b, (((ca,), (cb,)), ((), ())), preferred_element_type=F32)


def kernel(h_hbm, g_hbm, w1_hbm, w3_hbm, w2_hbm,
           o1_v, o3_v, o2_v, g_v,
           n_v, nt_v, gt_v, dn_v, h_v, a_v, d_v,
           c1_v, c3_v, e1_v, e3_v, f1_v, f3_v,
           w1_v, w3_v, w2_v,
           g1_v, g3_v, g2_v,
           rd1, rd3, rd2, ra1, ra3, ra2, rb1, rb3, rb2, rc1, rc3, rc2,
           pa1, pa3, pa2, pb1, pb3, pb2, s1, s3,
           ag_send, ag_recv, rs_send, rs_recv, ex_send, ex_recv, own_sem, cols_sem, h_sem, g_sem):
    me = lax.axis_index('fsdp')
    c = me % 2
    x = (me // 2) % 2
    y = (me // 4) % 2
    z = (me // 8) % 2
    core = me + 1 - 2 * c
    nx = me + 2 - 4 * x
    ny = me + 4 - 8 * y
    nz = me + 8 - 16 * z

    weights = (w1_v, w3_v, w2_v)
    grads = (g1_v, g3_v, g2_v)
    rds, ras, rbs, rcs = (rd1, rd3, rd2), (ra1, ra3, ra2), (rb1, rb3, rb2), (rc1, rc3, rc2)
    pas, pbs, outs, dones = (pa1, pa3, pa2), (pb1, pb3, pb2), (o1_v, o3_v), (s1, s3)
    cols, halves, theirs = (c1_v, c3_v), (e1_v, e3_v), (f1_v, f3_v)
    order = ((nx, ny, nz), (ny, nz, nx), (nz, nx, ny))

    def gather_slice(m, stage, k):
        s = lax.rem(k, WS)
        w = weights[m]
        if m == 0:
            return (lambda: w.at[s, c, z, y, x], lambda: w.at[s, c, z, y], lambda: w.at[s, c, z],
                    lambda: w.at[s, c, z, y], lambda: w.at[s, c, z, 1 - y], lambda: w.at[s, c, 1 - z])[stage]()
        if m == 1:
            return (lambda: w.at[s, c, z, y, x], lambda: w.at[s, c, z, :, x], lambda: w.at[s, c, :, :, x],
                    lambda: w.at[s, c, z, :, x], lambda: w.at[s, c, 1 - z, :, x], lambda: w.at[s, c, :, :, 1 - x])[stage]()
        return (lambda: w.at[s, z, y, x, c], lambda: w.at[s, :, y, x, c], lambda: w.at[s, :, y, :, c],
                lambda: w.at[s, :, y, x, c], lambda: w.at[s, :, y, 1 - x, c], lambda: w.at[s, :, 1 - y, :, c])[stage]()

    def own_rows(k):
        return w2_hbm.at[LAYERS - 1 - k // NC, pl.ds(pl.multiple_of(lax.rem(k, NC) * CPD, CPD), CPD)]

    def gather_copy(m, stage, k):
        par = lax.rem(k, 2)
        dst = gather_slice(m, stage, k)
        src = own_rows(k) if (stage == 0 and m == 2) else dst
        peer = core if stage >= 3 else order[m][stage]
        return pltpu.make_async_remote_copy(
            src_ref=src, dst_ref=dst, send_sem=ag_send.at[stage, par], recv_sem=ag_recv.at[stage, par],
            device_id=(peer,), device_id_type=MESH)

    def wait_bytes(ref, *sems):
        for sem in sems:
            pltpu.make_async_copy(ref, ref, sem).wait()

    def gather_wait(stage, k):
        par = lax.rem(k, 2)
        three = w1_v.at[pl.ds(0, 3)]
        blocks = (three.at[:, 0, 0, 0, 0], three.at[:, 0, 0, 0], three.at[:, 0, 0])[(0, 1, 2, 1, 1, 2)[stage]]
        wait_bytes(blocks, ag_send.at[stage, par], ag_recv.at[stage, par])

    def reduce_wait(stage, k):
        slot = lax.rem(k, 2 if stage == 0 else 3)
        blocks = (w1_v.at[pl.ds(0, 3)], ra1, ra1.at[:, 0], ra1.at[:, 0, 0])[stage]
        wait_bytes(blocks, rs_send.at[stage, slot], rs_recv.at[stage, slot])

    def half_wait(k):
        par = lax.rem(k, 2)
        wait_bytes(f1_v, ex_send.at[par], ex_recv.at[par])

    def own_copy(k):
        return pltpu.make_async_copy(own_rows(k), gather_slice(2, 0, k), own_sem)

    def cols_copy(m, li):
        return pltpu.make_async_copy((w1_hbm, w3_hbm)[m].at[LAYERS - 1 - li], cols[m], cols_sem.at[m])

    def half_copy(m, k):
        par = lax.rem(k, 2)
        return pltpu.make_async_remote_copy(
            src_ref=halves[m].at[lax.rem(k, 3), 1 - c], dst_ref=theirs[m].at[par], send_sem=ex_send.at[par], recv_sem=ex_recv.at[par],
            device_id=(core,), device_id_type=MESH)

    lane = lax.broadcasted_iota(jnp.int32, (DS, LANES), 1)

    def place(p, i):
        col = FS * p + CPD * i
        tile = col // LANES
        return pl.ds(pl.multiple_of(tile * LANES, LANES), LANES), col - tile * LANES

    def pick_columns(k):
        i = lax.rem(k, NC)
        for m in range(2):
            for half in range(2):
                acc = jnp.zeros((DS, LANES), F32)
                for q in range(DEV // 2):
                    tile, off = place(half * (DEV // 2) + q, i)
                    part = pltpu.roll(cols[m][:, tile].astype(F32), lax.rem(CPD * q + LANES - off, LANES), 1)
                    acc = jnp.where((lane >= CPD * q) & (lane < CPD * (q + 1)), part, acc)
                halves[m][lax.rem(k, 3), half] = acc

    def merge_rows(k):
        par = lax.rem(k, 2)
        for m in range(2):
            mine, other = halves[m][lax.rem(k, 3), c], theirs[m][par]
            low = jnp.where(c == 0, mine, other)
            high = jnp.where(c == 0, other, mine)
            weights[m][lax.rem(k, WS), c, z, y, x] = jnp.concatenate([low, high], axis=0).astype(BF)

    def put_columns(k):
        layer = lax.rem(LAYERS - (k + NC) // NC, LAYERS)
        i = lax.rem(k + NC, NC)
        for m in range(2):
            for half in range(2):
                src = dones[m][:, half * LANES:(half + 1) * LANES]
                for q in range(DEV // 2):
                    tile, off = place(half * (DEV // 2) + q, i)
                    part = pltpu.roll(src, lax.rem(off + LANES - CPD * q, LANES), 1)
                    outs[m][layer, :, tile] = jnp.where((lane >= off) & (lane < off + CPD), part, outs[m][layer, :, tile])

    def reduce_copy(m, stage, k):
        par = lax.rem(k, 2)
        slot = par if stage == 0 else lax.rem(k, 3)
        g, pa, pb = grads[m], pas[m].at[par], pbs[m].at[lax.rem(k, 3)]
        if stage == 0:
            src, dst, peer = g.at[par, :, :, :, 1 - c], rds[m].at[par], core
        elif stage == 1:
            src = (g.at[par, :, :, 1 - x, c], g.at[par, :, 1 - y, :, c], g.at[par, 1 - z, :, :, c])[m]
            dst, peer = ras[m].at[slot], order[m][0]
        elif stage == 2:
            src = (pa.at[:, 1 - y], pa.at[1 - z], pa.at[:, 1 - x])[m]
            dst, peer = rbs[m].at[slot], order[m][1]
        else:
            src = (pb.at[1 - z], pb.at[1 - x], pb.at[1 - y])[m]
            dst, peer = rcs[m].at[slot], order[m][2]
        return pltpu.make_async_remote_copy(
            src_ref=src, dst_ref=dst, send_sem=rs_send.at[stage, slot], recv_sem=rs_recv.at[stage, slot],
            device_id=(peer,), device_id_type=MESH)

    def h_copy(li, b):
        rows = pl.ds(pl.multiple_of(b * BB, BB), BB)
        slot = lax.rem(b, HR)
        return pltpu.make_async_copy(h_hbm.at[LAYERS - 1 - li, rows], h_v.at[slot], h_sem.at[slot])

    def g_copy():
        return pltpu.make_async_copy(g_hbm, g_v, g_sem)

    def finalize_rows(b):
        rows = pl.ds(pl.multiple_of(b * BB, BB), BB)
        hf = h_v[lax.rem(b, HR)].astype(F32)
        r = lax.rsqrt(jnp.mean(hf * hf, axis=-1, keepdims=True) + EPS)
        m = hf * r
        dn = dn_v[rows, :]
        dr = r * (dn - m * jnp.mean(dn * m, axis=-1, keepdims=True))
        g_v[rows, :] = (g_v[rows, :].astype(F32) + dr).astype(BF)

    def finalize_layer(li):
        def rows(b, cc):
            h_copy(li, b).wait()
            finalize_rows(b)

            @pl.when(b < NB - HR)
            def _():
                h_copy(li, b + HR).start()

            @pl.when((b >= NB - HR) & (li < LAYERS - 1))
            def _():
                h_copy(li + 1, b + HR - NB).start()
            return cc
        lax.fori_loop(0, NB, rows, 0)

    def prepare_rows(li, b):
        rows = pl.ds(pl.multiple_of(b * BB, BB), BB)
        h_copy(li, b).wait()
        hf = h_v[lax.rem(b, HR)].astype(F32)
        r = lax.rsqrt(jnp.mean(hf * hf, axis=-1, keepdims=True) + EPS)
        nb = (hf * r).astype(BF)
        n_v[rows, :] = nb
        nt_v[:, rows] = nb.T
        gt_v[:, rows] = g_v[rows, :].T
        dn_v[rows, :] = jnp.zeros((BB, D), F32)
        h_copy(li, lax.rem(b + HR, NB)).start()

    def gather_first(k):
        @pl.when((k >= 0) & (k < NK))
        def _():
            gather_wait(5, k)

    def gather_rest(k):
        def live(lag):
            return (k + lag >= 0) & (k + lag < NK)

        for lag, stage in ((1, 2), (2, 1), (3, 0)):
            @pl.when(live(lag))
            def _():
                gather_wait(stage, k + lag)
                if stage > 0:
                    gather_wait(stage + 2, k + lag)
                if stage == 0:
                    own_copy(k + lag).wait()
                for m in range(3):
                    gather_copy(m, stage + 3, k + lag).start()
                    if stage < 2:
                        gather_copy(m, stage + 1, k + lag).start()

        @pl.when(live(4))
        def _():
            half_wait(k + 4)
            merge_rows(k + 4)
            for m in range(3):
                gather_copy(m, 0, k + 4).start()
            own_copy(k + 4).start()

        @pl.when(k + 5 < NK)
        def _():
            for m in range(2):
                half_copy(m, k + 5).start()

        @pl.when(k < -3)
        def _():
            pick_columns(k + 6)

        @pl.when((k >= -4) & (k < -1))
        def _():
            pick_columns(k + 7)

        @pl.when((k + 6 == NC) | (k + 6 == 2 * NC))
        def _():
            for m in range(2):
                cols_copy(m, (k + 6) // NC).start()

    def reduce_step(k):
        def live(lag):
            return (k - lag >= 0) & (k - lag < NK)

        def finish(kf):
            reduce_wait(3, kf)
            for m in range(3):
                done = rcs[m][lax.rem(kf, 3)] + pbs[m][lax.rem(kf, 3), (z, x, y)[m]]
                if m == 2:
                    o2_v[LAYERS - 1 - kf // NC, pl.ds(pl.multiple_of(lax.rem(kf, NC) * CPD, CPD), CPD), :] = done
                else:
                    dones[m][...] = done

        def third(kf, send=True):
            par = lax.rem(kf, 2)
            reduce_wait(2, kf)
            for m in range(3):
                for a in range(2):
                    kept = (lambda: pa1[par, a, y], lambda: pa3[par, z, a], lambda: pa2[par, a, x])[m]()
                    pbs[m][lax.rem(kf, 3), a] = rbs[m][lax.rem(kf, 3), a] + kept
                if send:
                    reduce_copy(m, 3, kf).start()

        def second(kf):
            par = lax.rem(kf, 2)
            reduce_wait(1, kf)
            for m in range(3):
                for a in range(2):
                    for b in range(2):
                        kept = (lambda: g1_v[par, a, b, x, c], lambda: g3_v[par, a, y, b, c], lambda: g2_v[par, z, a, b, c])[m]()
                        pas[m][par, a, b] = ras[m][lax.rem(kf, 3), a, b] + kept
                reduce_copy(m, 2, kf).start()

        def first(kf):
            par = lax.rem(kf, 2)
            reduce_wait(0, kf)
            for m in range(3):
                for a in range(2):
                    for b in range(2):
                        for d in range(2):
                            grads[m][par, a, b, d, c] = grads[m][par, a, b, d, c] + rds[m][par, a, b, d]
                reduce_copy(m, 1, kf).start()

        @pl.when((k + 6 == NC) | (k + 6 == 2 * NC))
        def _():
            for m in range(2):
                cols_copy(m, (k + 6) // NC).wait()

        @pl.when(k <= NK)
        def _():
            pl.when(live(4))(lambda: finish(k - 4))

        @pl.when(k < NK)
        def _():
            pl.when(live(3))(lambda: third(k - 3))
            pl.when(live(2))(lambda: second(k - 2))
            pl.when(live(1))(lambda: first(k - 1))

        @pl.when(k == NK)
        def _():
            first(k - 1)
            finalize_layer(LAYERS - 1)
            second(k - 2)
            third(k - 3, send=False)

        @pl.when(k == NK + 1)
        def _():
            second(k - 2)
            for m in range(3):
                reduce_copy(m, 3, k - 4).start()
            third(k - 3)

        @pl.when(k == NK + 2)
        def _():
            third(k - 3)
            finish(k - 5)
            put_columns(k - 5)
            finish(k - 4)
            put_columns(k - 4)

        @pl.when(k == NK + 3)
        def _():
            finish(k - 4)
            put_columns(k - 4)

    def row_phase(k):
        s = lax.rem(k, WS)

        def body(b, carry):
            @pl.when((k == 0) & (b == 1))
            def _():
                gather_rest(k)

            rows = pl.ds(pl.multiple_of(b * RB, RB), RB)
            w1 = jnp.concatenate([w1_v[s, 0].reshape(D, HALF), w1_v[s, 1].reshape(D, HALF)], axis=1)
            w3 = jnp.concatenate([w3_v[s, 0].reshape(D, HALF), w3_v[s, 1].reshape(D, HALF)], axis=1)
            w2 = w2_v[s].reshape(CH, D)
            nb = n_v[rows, :]
            u = dot(nb, w1, 1, 0)
            v = dot(nb, w3, 1, 0)
            da = jnp.concatenate([dot(g_v[pl.ds(pl.multiple_of(b * RB + q * (RB // 2), RB // 2), RB // 2), :], w2, 1, 1) for q in range(2)], axis=0)
            sig = 1.0 / (1.0 + jnp.exp(-u))
            act = u * sig
            a_v[rows, :] = (act * v).astype(BF)
            du = (da * v * sig * (1.0 + u * (1.0 - sig))).astype(BF)
            dv = (da * act).astype(BF)
            d_v[rows, pl.ds(0, CH)] = du
            d_v[rows, pl.ds(CH, CH)] = dv
            for q in range(2):
                rq = slice(q * (RB // 2), (q + 1) * (RB // 2))
                rr = pl.ds(pl.multiple_of(b * RB + q * (RB // 2), RB // 2), RB // 2)
                dn_v[rr, :] += dot(du[rq], w1, 1, 1) + dot(dv[rq], w3, 1, 1)
            return carry

        lax.fori_loop(0, ROWS // RB, body, 0)

    def grad_phase(k):
        par = lax.rem(k, 2)
        pick_columns(k + 6)
        put_columns(k - 4)
        nt = nt_v[...]
        g1_v[par] = dot(nt, d_v[:, pl.ds(0, CH)], 1, 0).reshape(2, 2, 2, 2, DS, CH)
        g3_v[par] = dot(nt, d_v[:, pl.ds(CH, CH)], 1, 0).reshape(2, 2, 2, 2, DS, CH)
        g2_v[par] = dot(gt_v[...], a_v[...], 1, 0).T.reshape(2, 2, 2, 2, CPD, D)

    for m in range(2):
        cols_copy(m, 0).start()
    barrier = pltpu.get_barrier_semaphore()
    for peer in (core, nx, ny, nz):
        pl.semaphore_signal(barrier, inc=1, device_id=(peer,), device_id_type=MESH)
    for b in range(HR):
        h_copy(0, b).start()
    g_copy().start()
    for m in range(2):
        cols_copy(m, 0).wait()
    pick_columns(0)
    pl.semaphore_wait(barrier, 4)

    def step(t, carry):
        k = t - LEAD
        inside = (k >= 0) & (k < NK)
        last = inside & (lax.rem(k + NC, NC) == NC - 1)
        gather_first(k)

        @pl.when(k != 0)
        def _():
            gather_rest(k)

        @pl.when((t >= 1) & (t < LEAD))
        def _():
            @pl.when(t == 1)
            def _():
                g_copy().wait()

            def rows(b, cc):
                prepare_rows(0, b)
                return cc
            lax.fori_loop(3 * (t - 1), 3 * t - t // 3 - t // 4 * 3, rows, 0)

        @pl.when(inside)
        def _():
            row_phase(k)

        @pl.when(last & (k < NK - 1))
        def _():
            finalize_layer(k // NC)

        reduce_step(k)

        @pl.when(inside)
        def _():
            grad_phase(k)
            for m in range(3):
                reduce_copy(m, 0, k).start()

        @pl.when(k == NK)
        def _():
            put_columns(k - 4)

        @pl.when(last & (k < NK - 1))
        def _():
            li = k // NC

            def rows(b, cc):
                prepare_rows(li + 1, b)
                return cc
            lax.fori_loop(0, NB, rows, 0)
        return carry

    lax.fori_loop(0, LEAD + NK + TAIL, step, 0)


def hand_out(*refs):
    srcs, dsts, sem = refs[:4], refs[4:8], refs[8]
    pieces = [(j, layer) for j in range(3) for layer in range(LAYERS)]
    pieces += [(3, pl.ds(q * (ROWS // 4), ROWS // 4)) for q in range(4)]
    copies = [pltpu.make_async_copy(srcs[j].at[w], dsts[j].at[w], sem.at[n]) for n, (j, w) in enumerate(pieces)]
    for copy in copies:
        copy.start()
    for copy in copies:
        copy.wait()


def fused(h, g, w1, w3, w2):
    any_spec = pl.BlockSpec(memory_space=pl.ANY)
    V = pltpu.VMEM
    wide, low = (DS, CH), (CPD, D)
    three = lambda *lead: [V(lead + wide, F32), V(lead + wide, F32), V(lead + low, F32)]
    scratch = [
        V((ROWS, D), BF), V((D, ROWS), BF), V((D, ROWS), BF),
        V((ROWS, D), F32), V((HR, BB, D), BF), V((ROWS, CH), BF), V((ROWS, 2 * CH), BF),
        V((DS, FF), BF), V((DS, FF), BF), V((3, 2, DS, LANES), F32), V((3, 2, DS, LANES), F32),
        V((2, DS, LANES), F32), V((2, DS, LANES), F32),
        V((WS, 2, 2, 2, 2, 2 * DS, HALF), BF), V((WS, 2, 2, 2, 2, 2 * DS, HALF), BF), V((WS, 2, 2, 2, 2, CPD, D), BF),
        *three(2, 2, 2, 2, 2),
        *three(2, 2, 2, 2), *three(3, 2, 2), *three(3, 2), *three(3),
        *three(2, 2, 2), *three(3, 2), V(wide, F32), V(wide, F32),
        pltpu.SemaphoreType.DMA((6, 2)), pltpu.SemaphoreType.DMA((6, 2)),
        pltpu.SemaphoreType.DMA((4, 3)), pltpu.SemaphoreType.DMA((4, 3)),
        pltpu.SemaphoreType.DMA((2,)), pltpu.SemaphoreType.DMA((2,)),
        pltpu.SemaphoreType.DMA(()), pltpu.SemaphoreType.DMA((2,)),
        pltpu.SemaphoreType.DMA((HR,)), pltpu.SemaphoreType.DMA(()),
    ]
    results = (
        jax.ShapeDtypeStruct((LAYERS, DS, FF), F32),
        jax.ShapeDtypeStruct((LAYERS, DS, FF), F32),
        jax.ShapeDtypeStruct((LAYERS, FS, D), F32),
        jax.ShapeDtypeStruct((ROWS, D), BF),
    )
    vmem_spec = pl.BlockSpec(memory_space=pltpu.VMEM)
    parts = pl.pallas_call(
        kernel,
        name='mlp_backward',
        out_shape=tuple(V(r.shape, r.dtype) for r in results),
        in_specs=[any_spec] * 5,
        out_specs=(vmem_spec,) * 4,
        scratch_shapes=scratch,
        compiler_params=pltpu.CompilerParams(collective_id=0, has_side_effects=True, vmem_limit_bytes=51 * 1024 * 1024),
    )(h, g, w1, w3, w2)
    return pl.pallas_call(
        hand_out,
        name='hand_out',
        out_shape=results,
        in_specs=[vmem_spec] * 4,
        out_specs=(any_spec,) * 4,
        scratch_shapes=[pltpu.SemaphoreType.DMA((13,))],
        compiler_params=pltpu.CompilerParams(vmem_limit_bytes=1024 * 1024),
    )(*[pltpu.with_memory_space_constraint(part, pltpu.VMEM) for part in parts])


def solution(mesh):
    weight_spec = P(None, 'fsdp', None)
    row_spec = P('fsdp', None)

    return jax.shard_map(fused, mesh=mesh, in_specs=(weight_spec, row_spec, weight_spec, weight_spec, weight_spec), out_specs=(weight_spec, weight_spec, weight_spec, row_spec), check_vma=False)
```
